32 devices in a mesh: xy: 16 (over z, y, core), gz: 2 (over x).
Axes of the slice: x: 2, y: 2, z: 4, core: 2. Of those that a mesh axis runs over, the one named last changes fastest.
Arguments:
- e_check: float32 [3, 128, 4, 1024], P(None, 'xy', 'gz'), may hold values from -6 to 6
- h_check: float32 [3, 128, 4, 1024], P(None, 'xy', 'gz'), may hold values from -6 to 6
- adj_e: float32 [3, 128, 4, 1024], P(None, 'xy', 'gz'), may hold values from -6 to 6
- adj_h: float32 [3, 128, 4, 1024], P(None, 'xy', 'gz'), may hold values from -6 to 6
- material: int32 [128, 4, 1024], P('xy', 'gz'), may hold values from 0 to 3
- owner: int32 [128, 4, 1024], P('xy', 'gz'), may hold values from 0 to 7
- permittivity: float32 [4], replicated, may hold values from 1 to 4
Outputs:
- adj_e_out: float32 [3, 128, 4, 1024], P(None, 'xy', 'gz')
- adj_h_out: float32 [3, 128, 4, 1024], P(None, 'xy', 'gz')
- height_grad: float32 [8], replicated
The draws below stay inside these ranges and needn't reach their ends.
All inputs are finite; a program needn't handle non-finite values.
Results may differ from the reference program's by a relative error of at most 0.0003.
Values sent between devices are 32-bit elements; how exact they have to be, the bound alone decides.
A program may use at most 64 MiB of HBM per device.

```python
import math
import jax
import jax.numpy as jnp
from jax import lax

NY = 1024
NI = 8
NX = 128
NZ = 4


def plant(entries, own_key, least, top_value):
    spot = [jax.random.randint(jax.random.fold_in(own_key, axis), (), 0, length) for axis, length in enumerate(entries.shape)]
    longest = entries.shape.index(max(entries.shape))
    neighbour = spot[:longest] + [(spot[longest] + 1) % entries.shape[longest]] + spot[longest + 1:]
    return entries.at[tuple(spot)].set(least).at[tuple(neighbour)].set(top_value)


def block_scale(rng, extent, split, least, largest):
    factor_of, own = 1.0, jax.random.fold_in(rng, 6)
    for dim, blocks in split:
        steps = jnp.exp(jax.random.uniform(jax.random.fold_in(own, dim), (blocks,), jnp.float32, least / len(split), largest / len(split)))
        factor_of = factor_of * jnp.repeat(steps, extent[dim] // blocks).reshape([-1 if axis == dim else 1 for axis in range(len(extent))])
    return factor_of


def centred(key, shape, scale, limit, shards=(), dtype=jnp.bfloat16):
    gain = block_scale(key, shape, shards, -0.22, 0.18) if shards else 1.0
    drawn = jax.random.normal(key, shape, jnp.float32) * scale * gain
    return jnp.minimum(jnp.maximum(drawn, -limit), limit).astype(dtype)


def setup_inputs(seed: int = 0) -> dict:
    splits = jax.random.split(jax.random.key(seed), 8)
    return {
        "e_check": centred(splits[0], (3, NX, NZ, NY), 1.0, 6.0, ((1, 16), (2, 2)), jnp.float32),
        "h_check": centred(splits[1], (3, NX, NZ, NY), 1.0, 6.0, ((1, 16), (2, 2)), jnp.float32),
        "adj_e": centred(splits[2], (3, NX, NZ, NY), 1.0, 6.0, ((1, 16), (2, 2)), jnp.float32),
        "adj_h": centred(splits[3], (3, NX, NZ, NY), 1.0, 6.0, ((1, 16), (2, 2)), jnp.float32),
        "material": plant(jax.random.randint(splits[4], (NX, NZ, NY), 0, 4), jax.random.fold_in(splits[4], 1), 0, 3).astype(jnp.int32),
        "owner": plant(jax.random.randint(splits[5], (NX, NZ, NY), 0, NI), jax.random.fold_in(splits[5], 1), 0, NI - 1).astype(jnp.int32),
        "permittivity": jnp.clip(jnp.exp(jax.random.uniform(splits[6], (4,), jnp.float32, math.log(1.0), math.log(4.0))), 1.0, 4.0),
    }


COURANT = 0.5

def diff_ahead(values, dim_axis):
    count = values.shape[dim_axis]
    zero_plane = jnp.zeros_like(lax.slice_in_dim(values, 0, 1, axis=dim_axis))
    later = jnp.concatenate([lax.slice_in_dim(values, 1, count, axis=dim_axis), zero_plane], axis=dim_axis)
    return later - values

def diff_behind(values, dim_axis):
    count = values.shape[dim_axis]
    zero_plane = jnp.zeros_like(lax.slice_in_dim(values, 0, 1, axis=dim_axis))
    earlier = jnp.concatenate([zero_plane, lax.slice_in_dim(values, 0, count - 1, axis=dim_axis)], axis=dim_axis)
    return values - earlier

def curl_with(fields, differ):
    comp_x, comp_y, comp_z = (fields[0], fields[1], fields[2])
    curl_x = differ(comp_z, 2) - differ(comp_y, 1)
    curl_y = differ(comp_x, 1) - differ(comp_z, 0)
    curl_z = differ(comp_y, 0) - differ(comp_x, 2)
    return jnp.stack([curl_x, curl_y, curl_z], axis=0)

def reference(e_check, h_check, adj_e, adj_h, material, owner, permittivity):
    e_coef = COURANT / permittivity[material]
    electric = [e_check]
    magnetic = h_check
    for index_step in range(2):
        magnetic = magnetic - COURANT * curl_with(electric[-1], diff_ahead)
        electric.append(electric[-1] + e_coef * curl_with(magnetic, diff_behind))
    adjoint_e, adjoint_h = (adj_e, adj_h)
    gradient = jnp.zeros((NI,), jnp.float32)
    for later_step in (2, 1):
        weight = e_coef * lax.optimization_barrier(jnp.sum(adjoint_e * (electric[later_step] - electric[later_step - 1]), axis=0))
        gradient = gradient + jax.ops.segment_sum(weight.reshape(-1), owner.reshape(-1).astype(jnp.int32), num_segments=NI)
        adjoint_h = adjoint_h + curl_with(e_coef * adjoint_e, diff_ahead)
        adjoint_e = adjoint_e - COURANT * curl_with(adjoint_h, diff_behind)
    total_cells = NX * NZ * NY
    gradient = gradient / jnp.sqrt(jnp.float32(total_cells / NI))
    return (adjoint_e, adjoint_h, gradient)
```

```python
import functools

import jax
import jax.numpy as jnp
import numpy as np
from jax import lax
from jax.experimental import pallas as pl
from jax.experimental.pallas import tpu as pltpu
from jax.sharding import PartitionSpec as P

NI = 8
COURANT = 0.5
MESH = pl.DeviceIdType.MESH
SCALES = (-COURANT, 1.0)


def kernel(
    dims, e_hbm, h_hbm, g_hbm, k_hbm, mat_hbm, own_hbm, perm,
    go_ref, ko_ref, grad_ref,
    field, inner, partial, curl_in, outer, mat, own, coef, weight,
    send_xf, send_xl, send_d5, send_d6,
    got_xf, got_zf, got_xl, got_zl, got_d5, got_d6,
    mine, gathered,
    load_sem, send_sem, recv_sem, sum_send, sum_recv, line_sem,
):
    n_x, n_z, nx, nz, ny, kinds, group, norm = dims
    total = n_x * n_z
    i = lax.axis_index("xy")
    k = lax.axis_index("gz")
    me = i * n_z + k

    def load(src, dst, slot):
        copies = []
        for z in range(nz):
            src_z = src.at[:, :, z, :] if len(src.shape) == 4 else src.at[:, z, :]
            dst_z = dst.at[:, z] if len(src.shape) == 4 else dst.at[z]
            copies.append(pltpu.make_async_copy(src_z, dst_z, load_sem.at[slot, z]))
        return copies

    loads = [
        load(e_hbm, field.at[0], 0),
        load(h_hbm, inner.at[0], 1),
        load(mat_hbm, mat, 2),
        load(g_hbm, outer, 3),
        load(k_hbm, inner.at[1], 4),
        load(own_hbm, own, 5),
    ]
    for copies in loads:
        for copy in copies:
            copy.start()

    barrier = pltpu.get_barrier_semaphore()
    line, spot = i // group, lax.rem(i, group)
    lines, plane = n_x // group, group * n_z

    def signal(sem, x, z):
        pl.semaphore_signal(sem, inc=1, device_id=(x, z), device_id_type=MESH)

    def greet_plane(step, carry):
        other = lax.rem(spot * n_z + k + step, plane)
        signal(barrier, line * group + other // n_z, lax.rem(other, n_z))
        return carry

    def greet_line(sem):
        def greet(step, carry):
            signal(sem, lax.rem(line + step, lines) * group + spot, k)
            return carry

        lax.fori_loop(1, lines, greet, 0)

    lax.fori_loop(1, plane, greet_plane, 0)
    greet_line(barrier)
    greeted = plane - 1 + lines - 1
    down, up = (spot == 0) & (line > 0), (spot == group - 1) & (line < lines - 1)
    outside = (
        (down, -1, 0), (down & (k < n_z - 1), -1, 1), (up, 1, 0), (up & (k > 0), 1, -1),
    )
    for cond, step_x, step_z in outside:
        pl.when(cond)(functools.partial(signal, barrier, i + step_x, k + step_z))
        greeted = greeted + cond.astype(jnp.int32)

    rows = lax.broadcasted_iota(jnp.int32, (nx, ny), 0)
    lanes = lax.broadcasted_iota(jnp.int32, (nx, ny), 1)
    first_row, last_row = rows == 0, rows == nx - 1
    first_lane, last_lane = lanes == 0, lanes == ny - 1

    def dy(v):
        return jnp.where(last_lane, 0.0, pltpu.roll(v, ny - 1, 1)) - v

    def dx(v):
        return jnp.where(last_row, 0.0, pltpu.roll(v, nx - 1, 0)) - v

    def by(v):
        return v - jnp.where(first_lane, 0.0, pltpu.roll(v, 1, 1))

    def bx(v, row):
        return v - jnp.where(first_row, row, pltpu.roll(v, 1, 0))

    def local_part(q, mag):
        scale = SCALES[q % 2]
        f = field.at[q]
        for z in range(nz):
            fx, fy, fz = f[0, z], f[1, z], f[2, z]
            if z < nz - 1:
                up_x, up_y = f[0, z + 1] - fx, f[1, z + 1] - fy
            else:
                up_x, up_y = -fx, -fy
            lx = mag[0, z] + scale * (dy(fz) - up_y)
            ly = mag[1, z] + scale * (up_x - dx(fz))
            lz = mag[2, z] + scale * (dx(fy) - dy(fx))
            partial[q, 0, z], partial[q, 1, z], partial[q, 2, z] = lx, ly, lz
            send_xf[q, z : z + 1] = fy[0:1]
            send_xf[q, nz + z : nz + z + 1] = fz[0:1]
            send_xl[q, z : z + 1] = ly[nx - 1 : nx]
            send_xl[q, nz + z : nz + z + 1] = lz[nx - 1 : nx]
            if z == 0:
                send_d5[q] = fx[nx - 1 : nx]
            if z == nz - 1:
                send_d6[q] = fz[0:1]

    def messages(q):
        below_x, above_x = i > 0, i < n_x - 1
        below_z, above_z = k > 0, k < n_z - 1
        table = (
            (send_d5.at[q], got_d5.at[q], (i + 1, k - 1), above_x & below_z, below_x & above_z),
            (send_d6.at[q], got_d6.at[q], (i - 1, k + 1), below_x & above_z, above_x & below_z),
            (send_xf.at[q], got_xf.at[q], (i - 1, k), below_x, above_x),
            (send_xl.at[q], got_xl.at[q], (i + 1, k), above_x, below_x),
            (field.at[q, 0:2, 0], got_zf.at[q], (i, k - 1), below_z, above_z),
            (partial.at[q, 0:2, nz - 1], got_zl.at[q], (i, k + 1), above_z, below_z),
        )
        return [
            (
                pltpu.make_async_remote_copy(
                    src_ref=src, dst_ref=dst, send_sem=send_sem.at[q, m],
                    recv_sem=recv_sem.at[q, m], device_id=target, device_id_type=MESH,
                ),
                sends,
                receives,
            )
            for m, (src, dst, target, sends, receives) in enumerate(table)
        ]

    def send(q):
        for copy, sends, _ in messages(q):
            pl.when(sends)(copy.start)

    def receive(q):
        for copy, _, receives in messages(q):
            pl.when(receives)(copy.wait_recv)

    def finish(q, put):
        scale = SCALES[q % 2]
        f, part = field.at[q], partial.at[q]
        not_first_x, not_last_x = i > 0, i < n_x - 1
        not_first_z, not_last_z = k > 0, k < n_z - 1

        def only(cond, v):
            return jnp.where(cond, v, 0.0)

        below_x = only(not_first_z, got_zl[q, 0] - scale * f[1, 0])
        below_y = got_zl[q, 1] + scale * f[0, 0]
        diagonal = only(not_last_x, scale * got_d6[q])
        below_y = only(not_first_z, below_y - jnp.where(last_row, diagonal, 0.0))
        result = []
        for z in range(nz):
            mx, my, mz = part[0, z], part[1, z], part[2, z]
            edge_y = got_xl[q, z : z + 1] - scale * f[2, z, 0:1]
            edge_z = got_xl[q, nz + z : nz + z + 1] + scale * f[1, z, 0:1]
            if z == nz - 1:
                mx = mx - only(not_last_z, scale * got_zf[q, 1])
                my = my + only(not_last_z, scale * got_zf[q, 0])
                edge_y = edge_y + only(not_last_z, scale * got_d5[q])
            edge_y, edge_z = only(not_first_x, edge_y), only(not_first_x, edge_z)
            next_y = only(not_last_x, scale * got_xf[q, z : z + 1])
            next_z = only(not_last_x, scale * got_xf[q, nz + z : nz + z + 1])
            my = my - jnp.where(last_row, next_z, 0.0)
            mz = mz + jnp.where(last_row, next_y, 0.0)
            if put is not None:
                put[0, z], put[1, z], put[2, z] = mx, my, mz
            result.append(
                (
                    by(mz) - (my - below_y),
                    (mx - below_x) - bx(mz, edge_z),
                    bx(my, edge_y) - by(mx),
                )
            )
            below_x, below_y = mx, my
        return result

    for slot in (0, 1):
        for copy in loads[slot]:
            copy.wait()
    local_part(0, inner.at[0])
    pl.semaphore_wait(barrier, greeted)
    send(0)
    greet_line(line_sem)
    for slot in (2, 3, 4):
        for copy in loads[slot]:
            copy.wait()
    for z in range(nz):
        kind = mat[z]
        eps = jnp.full((nx, ny), perm[0], jnp.float32)
        for number in range(1, kinds):
            eps = jnp.where(kind == number, perm[number], eps)
        coef[z] = COURANT / eps
        for c in range(3):
            field[1, c, z] = coef[z] * outer[c, z]
    local_part(1, inner.at[1])
    send(1)

    receive(0)
    change = finish(0, curl_in.at[0])
    for z in range(nz):
        for c in range(3):
            moved = coef[z] * change[z][c]
            curl_in[2, c, z] = moved
            field[2, c, z] = field[0, c, z] + moved
    local_part(2, curl_in.at[0])
    send(2)

    receive(1)
    change = finish(1, curl_in.at[1])
    for z in range(nz):
        dot = None
        for c in range(3):
            now = outer[c, z] - COURANT * change[z][c]
            inner[1, c, z] = now
            field[3, c, z] = coef[z] * now
            term = now * curl_in[2, c, z]
            dot = term if dot is None else dot + term
        weight[z] = coef[z] * dot
    local_part(3, curl_in.at[1])
    send(3)
    for copy in loads[5]:
        copy.wait()

    receive(2)
    change = finish(2, None)
    sums = [jnp.zeros((nx, 128), jnp.float32)] * NI
    for z in range(nz):
        dot = None
        for c in range(3):
            term = outer[c, z] * (coef[z] * change[z][c])
            dot = term if dot is None else dot + term
        both = weight[z] + coef[z] * dot
        which = own[z]
        for t in range(0, ny, 128):
            part, index = both[:, t : t + 128], which[:, t : t + 128]
            for j in range(NI):
                sums[j] = sums[j] + jnp.where(index == j, part, 0.0)
    lane = lax.broadcasted_iota(jnp.int32, (1, 128), 1)
    row = jnp.zeros((1, 128), jnp.float32)
    for j in range(NI):
        column = jnp.sum(sums[j], axis=0, keepdims=True)
        row = jnp.where(lane == j, jnp.sum(column, axis=1, keepdims=True), row)
    mine[0] = row
    gathered[me] = row

    pl.semaphore_wait(line_sem, lines - 1)

    def share_sum(step, carry):
        other = jnp.where(step < me, step, step + 1)
        pltpu.make_async_remote_copy(
            src_ref=mine.at[0], dst_ref=gathered.at[me], send_sem=sum_send, recv_sem=sum_recv,
            device_id=(other // n_z, lax.rem(other, n_z)), device_id_type=MESH,
        ).start()
        return carry

    lax.fori_loop(0, total - 1, share_sum, 0)

    receive(3)
    change = finish(3, ko_ref)
    for z in range(nz):
        for c in range(3):
            go_ref[c, z] = inner[1, c, z] - COURANT * change[z][c]
    everyone = gathered.at[0 : total - 1]
    pltpu.make_async_copy(everyone, everyone, sum_recv).wait()
    pltpu.make_async_copy(everyone, everyone, sum_send).wait()
    grad_ref[...] = jnp.sum(gathered[...], axis=0)[:, :NI] / norm
    for q in range(4):
        for copy, sends, _ in messages(q):
            pl.when(sends)(copy.wait_send)

def store(g_ref, h_ref, grad_ref, g_hbm, h_hbm, grad_hbm, sem):
    copies = [pltpu.make_async_copy(grad_ref, grad_hbm, sem.at[2, 0])]
    for z in range(g_ref.shape[1]):
        copies.append(pltpu.make_async_copy(g_ref.at[:, z], g_hbm.at[:, :, z, :], sem.at[0, z]))
        copies.append(pltpu.make_async_copy(h_ref.at[:, z], h_hbm.at[:, :, z, :], sem.at[1, z]))
    for copy in copies:
        copy.start()
    for copy in copies:
        copy.wait()


def solution(mesh):
    n_x, n_z = mesh.shape["xy"], mesh.shape["gz"]

    def body(e_check, h_check, adj_e, adj_h, material, owner, permittivity):
        _, nx, nz, ny = e_check.shape
        cells = nx * n_x * nz * n_z * ny
        norm = np.sqrt(np.float32(cells / NI))
        group = max(g for g in range(1, n_x + 1) if n_x % g == 0 and g * g <= n_x)
        dims = (n_x, n_z, nx, nz, ny, permittivity.shape[0], group, norm)
        f32 = jnp.float32
        hbm_spec = pl.BlockSpec(memory_space=pltpu.HBM)
        vmem_spec = pl.BlockSpec(memory_space=pltpu.VMEM)
        block = (3, nz, nx, ny)
        g, h, grad = pl.pallas_call(
            functools.partial(kernel, dims),
            out_shape=(
                pltpu.VMEM(block, f32), pltpu.VMEM(block, f32), pltpu.VMEM((1, NI), f32),
            ),
            in_specs=[hbm_spec] * 6 + [pl.BlockSpec(memory_space=pltpu.SMEM)],
            out_specs=(vmem_spec,) * 3,
            scratch_shapes=[
                pltpu.VMEM((4,) + block, f32),
                pltpu.VMEM((2,) + block, f32),
                pltpu.VMEM((4,) + block, f32),
                pltpu.VMEM((3,) + block, f32),
                pltpu.VMEM(block, f32),
                pltpu.VMEM((nz, nx, ny), jnp.int32),
                pltpu.VMEM((nz, nx, ny), jnp.int32),
                pltpu.VMEM((nz, nx, ny), f32),
                pltpu.VMEM((nz, nx, ny), f32),
                pltpu.VMEM((4, 2 * nz, ny), f32),
                pltpu.VMEM((4, 2 * nz, ny), f32),
                pltpu.VMEM((4, 1, ny), f32),
                pltpu.VMEM((4, 1, ny), f32),
                pltpu.VMEM((4, 2 * nz, ny), f32),
                pltpu.VMEM((4, 2, nx, ny), f32),
                pltpu.VMEM((4, 2 * nz, ny), f32),
                pltpu.VMEM((4, 2, nx, ny), f32),
                pltpu.VMEM((4, 1, ny), f32),
                pltpu.VMEM((4, 1, ny), f32),
                pltpu.VMEM((1, 1, 128), f32),
                pltpu.VMEM((n_x * n_z, 1, 128), f32),
                pltpu.SemaphoreType.DMA((6, nz)),
                pltpu.SemaphoreType.DMA((4, 6)),
                pltpu.SemaphoreType.DMA((4, 6)),
                pltpu.SemaphoreType.DMA,
                pltpu.SemaphoreType.DMA,
                pltpu.SemaphoreType.REGULAR,
            ],
            compiler_params=pltpu.CompilerParams(
                collective_id=0, has_side_effects=True
            ),
            name="yee_adjoint",
        )(e_check, h_check, adj_e, adj_h, material, owner, permittivity)
        g, h, grad = pl.pallas_call(
            store,
            out_shape=(
                jax.ShapeDtypeStruct(e_check.shape, f32),
                jax.ShapeDtypeStruct(e_check.shape, f32),
                jax.ShapeDtypeStruct((1, NI), f32),
            ),
            in_specs=[vmem_spec] * 3,
            out_specs=(hbm_spec,) * 3,
            scratch_shapes=[pltpu.SemaphoreType.DMA((3, nz))],
            compiler_params=pltpu.CompilerParams(vmem_limit_bytes=2**20),
            name="store_outputs",
        )(g, h, grad)
        return g, h, grad.reshape(NI)

    split = P(None, "xy", "gz", None)
    return jax.shard_map(
        body,
        mesh=mesh,
        in_specs=(split,) * 4 + (P("xy", "gz", None),) * 2 + (P(),),
        out_specs=(split, split, P()),
        check_vma=False,
    )
```

```python
import functools
import itertools

import jax
import jax.numpy as jnp
import numpy as np
from jax import lax
from jax.experimental import pallas as pl
from jax.experimental.pallas import tpu as pltpu
from jax.sharding import PartitionSpec as P

NI = 8
COURANT = 0.5
MESH = pl.DeviceIdType.MESH
SCALES = (-COURANT, 1.0)


def kernel(
    dims, e_hbm, h_hbm, g_hbm, k_hbm, mat_hbm, own_hbm, perm_hbm,
    go_ref, ko_ref, grad_ref,
    perm, field, inner, partial, curl_in, outer, mat, own, coef, weight,
    send_xf, send_xl, send_d5, send_d6,
    got_xf, got_zf, got_xl, got_zl, got_d5, got_d6,
    mine, gathered, tally,
    load_sem, send_sem, recv_sem, sum_send, sum_recv, plane_sem, line_sem,
):
    n_x, n_z, nx, nz, ny, kinds, group, norm = dims
    total = n_x * n_z
    i = lax.axis_index("xy")
    k = lax.axis_index("gz")
    me = i * n_z + k

    def load(src, dst, slot):
        for z in range(nz):
            src_z = src.at[:, :, z, :] if len(src.shape) == 4 else src.at[:, z, :]
            dst_z = dst.at[:, z] if len(src.shape) == 4 else dst.at[z]
            pltpu.make_async_copy(src_z, dst_z, load_sem.at[slot]).start()
        return pltpu.make_async_copy(dst, dst, load_sem.at[slot])

    barrier = pltpu.get_barrier_semaphore()
    line, spot = i // group, lax.rem(i, group)
    lines = n_x // group

    def signal(sem, x, z):
        pl.semaphore_signal(sem, inc=1, device_id=(x, z), device_id_type=MESH)

    def greet(sem, partners):
        count = 0
        for cond, x, z in partners:
            pl.when(cond)(functools.partial(signal, sem, x, z))
            count = count + cond.astype(jnp.int32)
        return count

    def greet_group(sem):
        for step in range(1, group):
            signal(sem, line * group + lax.rem(spot + step, group), k)
        return group - 1

    def greet_line(sem, hop):
        return greet(
            sem, ((line >= hop, i - hop * group, k), (line < lines - hop, i + hop * group, k))
        )

    first, last = (spot == 0) & (line > 0), (spot == group - 1) & (line < lines - 1)
    greeted = greet(
        barrier,
        (
            (first, i - 1, k), (first & (k < n_z - 1), i - 1, k + 1),
            (last, i + 1, k), (last & (k > 0), i + 1, k - 1),
            (~first & (i > 0) & (k < n_z - 1), i - 1, k + 1),
            (~last & (i < n_x - 1) & (k > 0), i + 1, k - 1),
        ),
    )
    for step in range(1, n_z):
        signal(barrier, i, lax.rem(k + step, n_z))
    greeted = greeted + n_z - 1 + greet_group(barrier) + greet_line(barrier, 1)

    loads = [load(e_hbm, field.at[0], 0), load(h_hbm, inner.at[0], 1)]
    perm_load = pltpu.make_async_copy(perm_hbm, perm, load_sem.at[6])
    perm_load.start()
    loads.append(load(mat_hbm, mat, 2))
    loads.append(load(g_hbm, outer, 3))
    loads.append(load(k_hbm, inner.at[1], 4))
    loads.append(load(own_hbm, own, 5))

    rows = lax.broadcasted_iota(jnp.int32, (nx, ny), 0)
    lanes = lax.broadcasted_iota(jnp.int32, (nx, ny), 1)
    first_row, last_row = rows == 0, rows == nx - 1
    first_lane, last_lane = lanes == 0, lanes == ny - 1

    def dy(v):
        return jnp.where(last_lane, 0.0, pltpu.roll(v, ny - 1, 1)) - v

    def dx(v):
        return jnp.where(last_row, 0.0, pltpu.roll(v, nx - 1, 0)) - v

    def by(v):
        return v - jnp.where(first_lane, 0.0, pltpu.roll(v, 1, 1))

    def bx(v, row):
        return v - jnp.where(first_row, row, pltpu.roll(v, 1, 0))

    def local_part(q, mag):
        scale = SCALES[q % 2]
        f = field.at[q]
        for z in range(nz):
            fx, fy, fz = f[0, z], f[1, z], f[2, z]
            if z < nz - 1:
                up_x, up_y = f[0, z + 1] - fx, f[1, z + 1] - fy
            else:
                up_x, up_y = -fx, -fy
            lx = mag[0, z] + scale * (dy(fz) - up_y)
            ly = mag[1, z] + scale * (up_x - dx(fz))
            lz = mag[2, z] + scale * (dx(fy) - dy(fx))
            partial[q, 0, z], partial[q, 1, z], partial[q, 2, z] = lx, ly, lz
            send_xf[q, z : z + 1] = fy[0:1]
            send_xf[q, nz + z : nz + z + 1] = fz[0:1]
            send_xl[q, z : z + 1] = ly[nx - 1 : nx]
            send_xl[q, nz + z : nz + z + 1] = lz[nx - 1 : nx]
            if z == 0:
                send_d5[q] = fx[nx - 1 : nx]
            if z == nz - 1:
                send_d6[q] = fz[0:1]

    def messages(q):
        below_x, above_x = i > 0, i < n_x - 1
        below_z, above_z = k > 0, k < n_z - 1
        return (
            (send_d5.at[q], got_d5.at[q], (i + 1, k - 1), above_x & below_z, below_x & above_z),
            (send_d6.at[q], got_d6.at[q], (i - 1, k + 1), below_x & above_z, above_x & below_z),
            (send_xf.at[q], got_xf.at[q], (i - 1, k), below_x, above_x),
            (send_xl.at[q], got_xl.at[q], (i + 1, k), above_x, below_x),
            (field.at[q, 0:2, 0], got_zf.at[q], (i, k - 1), below_z, above_z),
            (partial.at[q, 0:2, nz - 1], got_zl.at[q], (i, k + 1), above_z, below_z),
        )

    def send(q):
        for src, dst, target, sends, _ in messages(q):
            copy = pltpu.make_async_remote_copy(
                src_ref=src, dst_ref=dst, send_sem=send_sem, recv_sem=recv_sem.at[q],
                device_id=target, device_id_type=MESH,
            )
            pl.when(sends)(copy.start)

    sides = []
    for below_x, above_x, below_z, above_z in itertools.product((False, True), repeat=4):
        if below_x + above_x > n_x - 1 or below_z + above_z > n_z - 1:
            continue
        if (n_x > 1 and not below_x + above_x) or (n_z > 1 and not below_z + above_z):
            continue
        here = ((i > 0) == below_x) & ((i < n_x - 1) == above_x)
        here = here & ((k > 0) == below_z) & ((k < n_z - 1) == above_z)
        length = (above_x & below_z) + (below_x & above_z)
        length += 2 * nz * (below_x + above_x) + 2 * nx * (below_z + above_z)
        sides.append((here, length))

    def wait_exchange(sem, times):
        for here, length in sides:
            span = tally.at[0 : times * length]
            pl.when(here)(pltpu.make_async_copy(span, span, sem).wait)

    def receive(q):
        wait_exchange(recv_sem.at[q], 1)

    def finish(q, put):
        scale = SCALES[q % 2]
        f, part = field.at[q], partial.at[q]
        not_first_x, not_last_x = i > 0, i < n_x - 1
        not_first_z, not_last_z = k > 0, k < n_z - 1

        def only(cond, v):
            return jnp.where(cond, v, 0.0)

        below_x = only(not_first_z, got_zl[q, 0] - scale * f[1, 0])
        below_y = got_zl[q, 1] + scale * f[0, 0]
        diagonal = only(not_last_x, scale * got_d6[q])
        below_y = only(not_first_z, below_y - jnp.where(last_row, diagonal, 0.0))
        result = []
        for z in range(nz):
            mx, my, mz = part[0, z], part[1, z], part[2, z]
            edge_y = got_xl[q, z : z + 1] - scale * f[2, z, 0:1]
            edge_z = got_xl[q, nz + z : nz + z + 1] + scale * f[1, z, 0:1]
            if z == nz - 1:
                mx = mx - only(not_last_z, scale * got_zf[q, 1])
                my = my + only(not_last_z, scale * got_zf[q, 0])
                edge_y = edge_y + only(not_last_z, scale * got_d5[q])
            edge_y, edge_z = only(not_first_x, edge_y), only(not_first_x, edge_z)
            next_y = only(not_last_x, scale * got_xf[q, z : z + 1])
            next_z = only(not_last_x, scale * got_xf[q, nz + z : nz + z + 1])
            my = my - jnp.where(last_row, next_z, 0.0)
            mz = mz + jnp.where(last_row, next_y, 0.0)
            if put is not None:
                put[0, z], put[1, z], put[2, z] = mx, my, mz
            result.append(
                (
                    by(mz) - (my - below_y),
                    (mx - below_x) - bx(mz, edge_z),
                    bx(my, edge_y) - by(mx),
                )
            )
            below_x, below_y = mx, my
        return result

    for slot in (0, 1):
        loads[slot].wait()
    local_part(0, inner.at[0])
    pl.semaphore_wait(barrier, greeted)
    send(0)
    greeted = greet_group(plane_sem)
    perm_load.wait()
    for slot in (2, 3, 4):
        loads[slot].wait()
    for z in range(nz):
        kind = mat[z]
        eps = jnp.full((nx, ny), perm[0], jnp.float32)
        for number in range(1, kinds):
            eps = jnp.where(kind == number, perm[number], eps)
        coef[z] = COURANT / eps
        for c in range(3):
            field[1, c, z] = coef[z] * outer[c, z]
    local_part(1, inner.at[1])
    send(1)
    pl.semaphore_wait(plane_sem, greeted)
    hops = [1 << turn for turn in range((lines - 1).bit_length())]
    greeted = greet_line(line_sem.at[0], hops[0])

    receive(0)
    change = finish(0, curl_in.at[0])
    for z in range(nz):
        for c in range(3):
            moved = coef[z] * change[z][c]
            curl_in[2, c, z] = moved
            field[2, c, z] = field[0, c, z] + moved
    local_part(2, curl_in.at[0])
    send(2)
    for turn, hop in enumerate(hops[1:], 1):
        pl.semaphore_wait(line_sem.at[turn - 1], greeted)
        greeted = greet_line(line_sem.at[turn], hop)

    receive(1)
    change = finish(1, curl_in.at[1])
    for z in range(nz):
        dot = None
        for c in range(3):
            now = outer[c, z] - COURANT * change[z][c]
            inner[1, c, z] = now
            field[3, c, z] = coef[z] * now
            term = now * curl_in[2, c, z]
            dot = term if dot is None else dot + term
        weight[z] = coef[z] * dot
    local_part(3, curl_in.at[1])
    send(3)
    loads[5].wait()

    receive(2)
    change = finish(2, None)
    sums = [jnp.zeros((nx, 128), jnp.float32)] * NI
    for z in range(nz):
        dot = None
        for c in range(3):
            term = outer[c, z] * (coef[z] * change[z][c])
            dot = term if dot is None else dot + term
        both = weight[z] + coef[z] * dot
        which = own[z]
        for t in range(0, ny, 128):
            part, index = both[:, t : t + 128], which[:, t : t + 128]
            for j in range(NI):
                sums[j] = sums[j] + jnp.where(index == j, part, 0.0)
    lane = lax.broadcasted_iota(jnp.int32, (1, 128), 1)
    row = jnp.zeros((1, 128), jnp.float32)
    for j in range(NI):
        column = jnp.sum(sums[j], axis=0, keepdims=True)
        row = jnp.where(lane == j, jnp.sum(column, axis=1, keepdims=True), row)
    mine[0] = row
    gathered[me] = row

    pl.semaphore_wait(line_sem.at[len(hops) - 1], greeted)

    def share_sum(step, carry):
        other = jnp.where(step < me, step, step + 1)
        pltpu.make_async_remote_copy(
            src_ref=mine.at[0], dst_ref=gathered.at[me], send_sem=sum_send, recv_sem=sum_recv,
            device_id=(other // n_z, lax.rem(other, n_z)), device_id_type=MESH,
        ).start()
        return carry

    lax.fori_loop(0, total - 1, share_sum, 0)

    receive(3)
    change = finish(3, ko_ref)
    for z in range(nz):
        for c in range(3):
            go_ref[c, z] = inner[1, c, z] - COURANT * change[z][c]
    everyone = gathered.at[0 : total - 1]
    pltpu.make_async_copy(everyone, everyone, sum_recv).wait()
    pltpu.make_async_copy(everyone, everyone, sum_send).wait()
    grad_ref[...] = jnp.sum(gathered[...], axis=0)[:, :NI] / norm
    wait_exchange(send_sem, 4)

def store(g_ref, h_ref, grad_ref, g_hbm, h_hbm, grad_hbm, sem):
    pltpu.make_async_copy(grad_ref, grad_hbm, sem.at[2]).start()
    for z in range(g_ref.shape[1]):
        pltpu.make_async_copy(g_ref.at[:, z], g_hbm.at[:, :, z, :], sem.at[0]).start()
        pltpu.make_async_copy(h_ref.at[:, z], h_hbm.at[:, :, z, :], sem.at[1]).start()
    for n, ref in enumerate((g_ref, h_ref, grad_ref)):
        pltpu.make_async_copy(ref, ref, sem.at[n]).wait()


def solution(mesh):
    n_x, n_z = mesh.shape["xy"], mesh.shape["gz"]

    def body(e_check, h_check, adj_e, adj_h, material, owner, permittivity):
        _, nx, nz, ny = e_check.shape
        cells = nx * n_x * nz * n_z * ny
        norm = np.sqrt(np.float32(cells / NI))
        group = max(g for g in range(1, n_x + 1) if n_x % g == 0 and g * g <= n_x)
        dims = (n_x, n_z, nx, nz, ny, permittivity.shape[0], group, norm)
        f32 = jnp.float32
        hbm_spec = pl.BlockSpec(memory_space=pltpu.HBM)
        vmem_spec = pl.BlockSpec(memory_space=pltpu.VMEM)
        block = (3, nz, nx, ny)
        g, h, grad = pl.pallas_call(
            functools.partial(kernel, dims),
            out_shape=(
                pltpu.VMEM(block, f32), pltpu.VMEM(block, f32), pltpu.VMEM((1, NI), f32),
            ),
            in_specs=[hbm_spec] * 7,
            out_specs=(vmem_spec,) * 3,
            scratch_shapes=[
                pltpu.SMEM(permittivity.shape, f32),
                pltpu.VMEM((4,) + block, f32),
                pltpu.VMEM((2,) + block, f32),
                pltpu.VMEM((4,) + block, f32),
                pltpu.VMEM((3,) + block, f32),
                pltpu.VMEM(block, f32),
                pltpu.VMEM((nz, nx, ny), jnp.int32),
                pltpu.VMEM((nz, nx, ny), jnp.int32),
                pltpu.VMEM((nz, nx, ny), f32),
                pltpu.VMEM((nz, nx, ny), f32),
                pltpu.VMEM((4, 2 * nz, ny), f32),
                pltpu.VMEM((4, 2 * nz, ny), f32),
                pltpu.VMEM((4, 1, ny), f32),
                pltpu.VMEM((4, 1, ny), f32),
                pltpu.VMEM((4, 2 * nz, ny), f32),
                pltpu.VMEM((4, 2, nx, ny), f32),
                pltpu.VMEM((4, 2 * nz, ny), f32),
                pltpu.VMEM((4, 2, nx, ny), f32),
                pltpu.VMEM((4, 1, ny), f32),
                pltpu.VMEM((4, 1, ny), f32),
                pltpu.VMEM((1, 1, 128), f32),
                pltpu.VMEM((n_x * n_z, 1, 128), f32),
                pltpu.VMEM((8 * (1 + 2 * nz + 2 * nx), 1, ny), f32),
                pltpu.SemaphoreType.DMA((7,)),
                pltpu.SemaphoreType.DMA,
                pltpu.SemaphoreType.DMA((4,)),
                pltpu.SemaphoreType.DMA,
                pltpu.SemaphoreType.DMA,
                pltpu.SemaphoreType.REGULAR,
                pltpu.SemaphoreType.REGULAR((max(1, (n_x // group - 1).bit_length()),)),
            ],
            compiler_params=pltpu.CompilerParams(
                collective_id=0, has_side_effects=True
            ),
            name="yee_adjoint",
        )(e_check, h_check, adj_e, adj_h, material, owner, permittivity)
        g, h, grad = pl.pallas_call(
            store,
            out_shape=(
                jax.ShapeDtypeStruct(e_check.shape, f32),
                jax.ShapeDtypeStruct(e_check.shape, f32),
                jax.ShapeDtypeStruct((1, NI), f32),
            ),
            in_specs=[vmem_spec] * 3,
            out_specs=(hbm_spec,) * 3,
            scratch_shapes=[pltpu.SemaphoreType.DMA((3,))],
            compiler_params=pltpu.CompilerParams(vmem_limit_bytes=2**20),
            name="store_outputs",
        )(g, h, grad)
        return g, h, grad.reshape(NI)

    split = P(None, "xy", "gz", None)
    return jax.shard_map(
        body,
        mesh=mesh,
        in_specs=(split,) * 4 + (P("xy", "gz", None),) * 2 + (P(),),
        out_specs=(split, split, P()),
        check_vma=False,
    )
```

```python
import functools
import itertools

import jax
import jax.numpy as jnp
import numpy as np
from jax import lax
from jax.experimental import pallas as pl
from jax.experimental.pallas import tpu as pltpu
from jax.sharding import PartitionSpec as P

NI = 8
COURANT = 0.5
MESH = pl.DeviceIdType.MESH
LINES, PLANES = slice(0, 4), slice(4, 6)
SCALES = (-COURANT, 1.0)


def kernel(
    dims, e_hbm, h_hbm, g_hbm, k_hbm, mat_hbm, own_hbm, perm_hbm,
    go_ref, ko_ref, grad_ref,
    perm, field, inner, partial, curl_in, outer, mat, own, coef, weight,
    send_xf, send_xl, send_d5, send_d6,
    got_xf, got_zf, got_xl, got_zl, got_d5, got_d6,
    mine, gathered, tally,
    load_sem, send_sem, plane_sent, recv_sem, sum_send, sum_recv,
    plane_sem, line_sem, pair_sem,
):
    n_x, n_z, nx, nz, ny, kinds, group, norm = dims
    total = n_x * n_z
    i = lax.axis_index("xy")
    k = lax.axis_index("gz")
    me = i * n_z + k

    def load(src, dst, slot):
        for z in range(nz):
            src_z = src.at[:, :, z, :] if len(src.shape) == 4 else src.at[:, z, :]
            dst_z = dst.at[:, z] if len(src.shape) == 4 else dst.at[z]
            pltpu.make_async_copy(src_z, dst_z, load_sem.at[slot]).start()
        return pltpu.make_async_copy(dst, dst, load_sem.at[slot])

    barrier = pltpu.get_barrier_semaphore()
    line, spot = i // group, lax.rem(i, group)
    lines = n_x // group

    def signal(sem, x, z):
        pl.semaphore_signal(sem, inc=1, device_id=(x, z), device_id_type=MESH)

    def greet(sem, partners):
        count = 0
        for cond, x, z in partners:
            pl.when(cond)(functools.partial(signal, sem, x, z))
            count = count + cond.astype(jnp.int32)
        return count

    def greet_group(sem):
        for step in range(1, group):
            signal(sem, line * group + lax.rem(spot + step, group), k)
        return group - 1

    def greet_line(sem, hop):
        return greet(
            sem, ((line >= hop, i - hop * group, k), (line < lines - hop, i + hop * group, k))
        )

    first, last = (spot == 0) & (line > 0), (spot == group - 1) & (line < lines - 1)
    greeted = greet(
        barrier,
        (
            (first, i - 1, k), (first & (k < n_z - 1), i - 1, k + 1),
            (last, i + 1, k), (last & (k > 0), i + 1, k - 1),
            (~first & (i > 0) & (k < n_z - 1), i - 1, k + 1),
            (~last & (i < n_x - 1) & (k > 0), i + 1, k - 1),
        ),
    )
    for step in range(1, n_z):
        signal(barrier, i, lax.rem(k + step, n_z))
    greeted = greeted + n_z - 1 + greet_group(barrier) + greet_line(barrier, 1)

    loads = [load(e_hbm, field.at[0], 0), load(h_hbm, inner.at[0], 1)]
    perm_load = pltpu.make_async_copy(perm_hbm, perm, load_sem.at[6])
    perm_load.start()
    loads.append(load(mat_hbm, mat, 2))
    loads.append(load(g_hbm, outer, 3))
    loads.append(load(k_hbm, inner.at[1], 4))
    loads.append(load(own_hbm, own, 5))

    rows = lax.broadcasted_iota(jnp.int32, (nx, ny), 0)
    lanes = lax.broadcasted_iota(jnp.int32, (nx, ny), 1)
    first_row, last_row = rows == 0, rows == nx - 1
    first_lane, last_lane = lanes == 0, lanes == ny - 1

    def dy(v):
        return jnp.where(last_lane, 0.0, pltpu.roll(v, ny - 1, 1)) - v

    def dx(v):
        return jnp.where(last_row, 0.0, pltpu.roll(v, nx - 1, 0)) - v

    def by(v):
        return v - jnp.where(first_lane, 0.0, pltpu.roll(v, 1, 1))

    def bx(v, row):
        return v - jnp.where(first_row, row, pltpu.roll(v, 1, 0))

    def local_part(q, mag):
        scale = SCALES[q % 2]
        f = field.at[q]
        for z in range(nz):
            fx, fy, fz = f[0, z], f[1, z], f[2, z]
            if z < nz - 1:
                up_x, up_y = f[0, z + 1] - fx, f[1, z + 1] - fy
            else:
                up_x, up_y = -fx, -fy
            lx = mag[0, z] + scale * (dy(fz) - up_y)
            ly = mag[1, z] + scale * (up_x - dx(fz))
            lz = mag[2, z] + scale * (dx(fy) - dy(fx))
            partial[q, 0, z], partial[q, 1, z], partial[q, 2, z] = lx, ly, lz
            send_xf[q, z : z + 1] = fy[0:1]
            send_xf[q, nz + z : nz + z + 1] = fz[0:1]
            send_xl[q, z : z + 1] = ly[nx - 1 : nx]
            send_xl[q, nz + z : nz + z + 1] = lz[nx - 1 : nx]
            if z == 0:
                send_d5[q] = fx[nx - 1 : nx]
            if z == nz - 1:
                send_d6[q] = fz[0:1]

    def messages(q):
        below_x, above_x = i > 0, i < n_x - 1
        below_z, above_z = k > 0, k < n_z - 1
        return (
            (send_d5.at[q], got_d5.at[q], (i + 1, k - 1), above_x & below_z, below_x & above_z),
            (send_d6.at[q], got_d6.at[q], (i - 1, k + 1), below_x & above_z, above_x & below_z),
            (send_xf.at[q], got_xf.at[q], (i - 1, k), below_x, above_x),
            (send_xl.at[q], got_xl.at[q], (i + 1, k), above_x, below_x),
            (field.at[q, 0:2, 0], got_zf.at[q], (i, k - 1), below_z, above_z),
            (partial.at[q, 0:2, nz - 1], got_zl.at[q], (i, k + 1), above_z, below_z),
        )

    def send(q, part=slice(None)):
        for src, dst, target, sends, _ in messages(q)[part]:
            copy = pltpu.make_async_remote_copy(
                src_ref=src, dst_ref=dst, device_id=target, device_id_type=MESH,
                send_sem=plane_sent.at[q // 2] if part == PLANES and q % 2 == 0 else send_sem,
                recv_sem=recv_sem.at[q],
            )
            pl.when(sends)(copy.start)

    sides = []
    for below_x, above_x, below_z, above_z in itertools.product((False, True), repeat=4):
        if below_x + above_x > n_x - 1 or below_z + above_z > n_z - 1:
            continue
        if (n_x > 1 and not below_x + above_x) or (n_z > 1 and not below_z + above_z):
            continue
        here = ((i > 0) == below_x) & ((i < n_x - 1) == above_x)
        here = here & ((k > 0) == below_z) & ((k < n_z - 1) == above_z)
        length = (above_x & below_z) + (below_x & above_z) + 2 * nz * (below_x + above_x)
        sides.append((here, length, 2 * nx * (below_z + above_z)))

    def wait_exchange(sem, lines, planes):
        for here, length, plane in sides:
            if lines * length + planes * plane:
                span = tally.at[0 : lines * length + planes * plane]
                pl.when(here)(pltpu.make_async_copy(span, span, sem).wait)

    def send_after(q):
        send(q, LINES)
        wait_exchange(plane_sent.at[q // 2], 0, 1)
        if n_x % 2 == 0:
            signal(pair_sem.at[q // 2], i + 1 - 2 * lax.rem(i, 2), k)
            pl.semaphore_wait(pair_sem.at[q // 2], 1)
        send(q, PLANES)

    def receive(q):
        wait_exchange(recv_sem.at[q], 1, 1)

    def finish(q, put):
        scale = SCALES[q % 2]
        f, part = field.at[q], partial.at[q]
        not_first_x, not_last_x = i > 0, i < n_x - 1
        not_first_z, not_last_z = k > 0, k < n_z - 1

        def only(cond, v):
            return jnp.where(cond, v, 0.0)

        below_x = only(not_first_z, got_zl[q, 0] - scale * f[1, 0])
        below_y = got_zl[q, 1] + scale * f[0, 0]
        diagonal = only(not_last_x, scale * got_d6[q])
        below_y = only(not_first_z, below_y - jnp.where(last_row, diagonal, 0.0))
        result = []
        for z in range(nz):
            mx, my, mz = part[0, z], part[1, z], part[2, z]
            edge_y = got_xl[q, z : z + 1] - scale * f[2, z, 0:1]
            edge_z = got_xl[q, nz + z : nz + z + 1] + scale * f[1, z, 0:1]
            if z == nz - 1:
                mx = mx - only(not_last_z, scale * got_zf[q, 1])
                my = my + only(not_last_z, scale * got_zf[q, 0])
                edge_y = edge_y + only(not_last_z, scale * got_d5[q])
            edge_y, edge_z = only(not_first_x, edge_y), only(not_first_x, edge_z)
            next_y = only(not_last_x, scale * got_xf[q, z : z + 1])
            next_z = only(not_last_x, scale * got_xf[q, nz + z : nz + z + 1])
            my = my - jnp.where(last_row, next_z, 0.0)
            mz = mz + jnp.where(last_row, next_y, 0.0)
            if put is not None:
                put[0, z], put[1, z], put[2, z] = mx, my, mz
            result.append(
                (
                    by(mz) - (my - below_y),
                    (mx - below_x) - bx(mz, edge_z),
                    bx(my, edge_y) - by(mx),
                )
            )
            below_x, below_y = mx, my
        return result

    for slot in (0, 1):
        loads[slot].wait()
    local_part(0, inner.at[0])
    pl.semaphore_wait(barrier, greeted)
    send(0, LINES)
    send(0, PLANES)
    greeted = greet_group(plane_sem)
    perm_load.wait()
    for slot in (2, 3, 4):
        loads[slot].wait()
    for z in range(nz):
        kind = mat[z]
        eps = jnp.full((nx, ny), perm[0], jnp.float32)
        for number in range(1, kinds):
            eps = jnp.where(kind == number, perm[number], eps)
        coef[z] = COURANT / eps
        for c in range(3):
            field[1, c, z] = coef[z] * outer[c, z]
    local_part(1, inner.at[1])
    send_after(1)
    pl.semaphore_wait(plane_sem, greeted)
    hops = [1 << turn for turn in range((lines - 1).bit_length())]
    greeted = greet_line(line_sem.at[0], hops[0])

    receive(0)
    change = finish(0, curl_in.at[0])
    for z in range(nz):
        for c in range(3):
            moved = coef[z] * change[z][c]
            curl_in[2, c, z] = moved
            field[2, c, z] = field[0, c, z] + moved
    local_part(2, curl_in.at[0])
    send(2, LINES)
    send(2, PLANES)
    for turn, hop in enumerate(hops[1:], 1):
        pl.semaphore_wait(line_sem.at[turn - 1], greeted)
        greeted = greet_line(line_sem.at[turn], hop)

    receive(1)
    change = finish(1, curl_in.at[1])
    for z in range(nz):
        dot = None
        for c in range(3):
            now = outer[c, z] - COURANT * change[z][c]
            inner[1, c, z] = now
            field[3, c, z] = coef[z] * now
            term = now * curl_in[2, c, z]
            dot = term if dot is None else dot + term
        weight[z] = coef[z] * dot
    local_part(3, curl_in.at[1])
    send_after(3)
    loads[5].wait()

    receive(2)
    change = finish(2, None)
    sums = [jnp.zeros((nx, 128), jnp.float32)] * NI
    for z in range(nz):
        dot = None
        for c in range(3):
            term = outer[c, z] * (coef[z] * change[z][c])
            dot = term if dot is None else dot + term
        both = weight[z] + coef[z] * dot
        which = own[z]
        for t in range(0, ny, 128):
            part, index = both[:, t : t + 128], which[:, t : t + 128]
            for j in range(NI):
                sums[j] = sums[j] + jnp.where(index == j, part, 0.0)
    lane = lax.broadcasted_iota(jnp.int32, (1, 128), 1)
    row = jnp.zeros((1, 128), jnp.float32)
    for j in range(NI):
        column = jnp.sum(sums[j], axis=0, keepdims=True)
        row = jnp.where(lane == j, jnp.sum(column, axis=1, keepdims=True), row)
    mine[0] = row
    gathered[me] = row

    pl.semaphore_wait(line_sem.at[len(hops) - 1], greeted)

    def share_sum(step, carry):
        other = jnp.where(step < me, step, step + 1)
        pltpu.make_async_remote_copy(
            src_ref=mine.at[0], dst_ref=gathered.at[me], send_sem=sum_send, recv_sem=sum_recv,
            device_id=(other // n_z, lax.rem(other, n_z)), device_id_type=MESH,
        ).start()
        return carry

    lax.fori_loop(0, total - 1, share_sum, 0)

    receive(3)
    change = finish(3, ko_ref)
    for z in range(nz):
        for c in range(3):
            go_ref[c, z] = inner[1, c, z] - COURANT * change[z][c]
    everyone = gathered.at[0 : total - 1]
    pltpu.make_async_copy(everyone, everyone, sum_recv).wait()
    pltpu.make_async_copy(everyone, everyone, sum_send).wait()
    grad_ref[...] = jnp.sum(gathered[...], axis=0)[:, :NI] / norm
    wait_exchange(send_sem, 4, 2)

def store(g_ref, h_ref, grad_ref, g_hbm, h_hbm, grad_hbm, sem):
    pltpu.make_async_copy(grad_ref, grad_hbm, sem.at[2]).start()
    for z in range(g_ref.shape[1]):
        pltpu.make_async_copy(g_ref.at[:, z], g_hbm.at[:, :, z, :], sem.at[0]).start()
        pltpu.make_async_copy(h_ref.at[:, z], h_hbm.at[:, :, z, :], sem.at[1]).start()
    for n, ref in enumerate((g_ref, h_ref, grad_ref)):
        pltpu.make_async_copy(ref, ref, sem.at[n]).wait()


def solution(mesh):
    n_x, n_z = mesh.shape["xy"], mesh.shape["gz"]

    def body(e_check, h_check, adj_e, adj_h, material, owner, permittivity):
        _, nx, nz, ny = e_check.shape
        cells = nx * n_x * nz * n_z * ny
        norm = np.sqrt(np.float32(cells / NI))
        group = max(g for g in range(1, n_x + 1) if n_x % g == 0 and g * g <= n_x)
        dims = (n_x, n_z, nx, nz, ny, permittivity.shape[0], group, norm)
        f32 = jnp.float32
        hbm_spec = pl.BlockSpec(memory_space=pltpu.HBM)
        vmem_spec = pl.BlockSpec(memory_space=pltpu.VMEM)
        block = (3, nz, nx, ny)
        g, h, grad = pl.pallas_call(
            functools.partial(kernel, dims),
            out_shape=(
                pltpu.VMEM(block, f32), pltpu.VMEM(block, f32), pltpu.VMEM((1, NI), f32),
            ),
            in_specs=[hbm_spec] * 7,
            out_specs=(vmem_spec,) * 3,
            scratch_shapes=[
                pltpu.SMEM(permittivity.shape, f32),
                pltpu.VMEM((4,) + block, f32),
                pltpu.VMEM((2,) + block, f32),
                pltpu.VMEM((4,) + block, f32),
                pltpu.VMEM((3,) + block, f32),
                pltpu.VMEM(block, f32),
                pltpu.VMEM((nz, nx, ny), jnp.int32),
                pltpu.VMEM((nz, nx, ny), jnp.int32),
                pltpu.VMEM((nz, nx, ny), f32),
                pltpu.VMEM((nz, nx, ny), f32),
                pltpu.VMEM((4, 2 * nz, ny), f32),
                pltpu.VMEM((4, 2 * nz, ny), f32),
                pltpu.VMEM((4, 1, ny), f32),
                pltpu.VMEM((4, 1, ny), f32),
                pltpu.VMEM((4, 2 * nz, ny), f32),
                pltpu.VMEM((4, 2, nx, ny), f32),
                pltpu.VMEM((4, 2 * nz, ny), f32),
                pltpu.VMEM((4, 2, nx, ny), f32),
                pltpu.VMEM((4, 1, ny), f32),
                pltpu.VMEM((4, 1, ny), f32),
                pltpu.VMEM((1, 1, 128), f32),
                pltpu.VMEM((n_x * n_z, 1, 128), f32),
                pltpu.VMEM((8 * (1 + 2 * nz + 2 * nx), 1, ny), f32),
                pltpu.SemaphoreType.DMA((7,)),
                pltpu.SemaphoreType.DMA,
                pltpu.SemaphoreType.DMA((2,)),
                pltpu.SemaphoreType.DMA((4,)),
                pltpu.SemaphoreType.DMA,
                pltpu.SemaphoreType.DMA,
                pltpu.SemaphoreType.REGULAR,
                pltpu.SemaphoreType.REGULAR((max(1, (n_x // group - 1).bit_length()),)),
                pltpu.SemaphoreType.REGULAR((2,)),
            ],
            compiler_params=pltpu.CompilerParams(
                collective_id=0, has_side_effects=True
            ),
            name="yee_adjoint",
        )(e_check, h_check, adj_e, adj_h, material, owner, permittivity)
        g, h, grad = pl.pallas_call(
            store,
            out_shape=(
                jax.ShapeDtypeStruct(e_check.shape, f32),
                jax.ShapeDtypeStruct(e_check.shape, f32),
                jax.ShapeDtypeStruct((1, NI), f32),
            ),
            in_specs=[vmem_spec] * 3,
            out_specs=(hbm_spec,) * 3,
            scratch_shapes=[pltpu.SemaphoreType.DMA((3,))],
            compiler_params=pltpu.CompilerParams(vmem_limit_bytes=2**20),
            name="store_outputs",
        )(g, h, grad)
        return g, h, grad.reshape(NI)

    split = P(None, "xy", "gz", None)
    return jax.shard_map(
        body,
        mesh=mesh,
        in_specs=(split,) * 4 + (P("xy", "gz", None),) * 2 + (P(),),
        out_specs=(split, split, P()),
        check_vma=False,
    )
```

```python
import functools
import itertools

import jax
import jax.numpy as jnp
import numpy as np
from jax import lax
from jax.experimental import pallas as pl
from jax.experimental.pallas import tpu as pltpu
from jax.sharding import PartitionSpec as P

NI = 8
COURANT = 0.5
MESH = pl.DeviceIdType.MESH
LINES, PLANES = (0, 1, 2, 3), (4, 5, 6, 7)
SCALES = (-COURANT, 1.0)


def kernel(
    dims, e_hbm, h_hbm, g_hbm, k_hbm, mat_hbm, own_hbm, perm_hbm,
    go_ref, ko_ref, grad_ref,
    perm, field, inner, partial, curl_in, outer, mat, own, coef, weight,
    send_xf, send_xl, send_d5, send_d6,
    got_xf, got_zf, got_xl, got_zl, got_d5, got_d6,
    mine, gathered, tally,
    load_sem, send_sem, plane_sent, recv_sem, sum_send, sum_recv,
    line_sem, pair_sem,
):
    n_x, n_z, nx, nz, ny, kinds, norm = dims
    total = n_x * n_z
    i = lax.axis_index("xy")
    k = lax.axis_index("gz")
    me = i * n_z + k
    odd = lax.rem(i, 2) == 1

    def load(src, dst, slot):
        for z in range(nz):
            src_z = src.at[:, :, z, :] if len(src.shape) == 4 else src.at[:, z, :]
            dst_z = dst.at[:, z] if len(src.shape) == 4 else dst.at[z]
            pltpu.make_async_copy(src_z, dst_z, load_sem.at[slot]).start()
        return pltpu.make_async_copy(dst, dst, load_sem.at[slot])

    barrier = pltpu.get_barrier_semaphore()

    def signal(sem, x, z):
        pl.semaphore_signal(sem, inc=1, device_id=(x, z), device_id_type=MESH)

    def greet(sem, partners):
        count = 0
        for cond, x, z in partners:
            pl.when(cond)(functools.partial(signal, sem, x, z))
            count = count + cond.astype(jnp.int32)
        return count

    def greet_line(sem, hop):
        return greet(sem, ((i >= hop, i - hop, k), (i < n_x - hop, i + hop, k)))

    loads = [load(e_hbm, field.at[0], 0), load(h_hbm, inner.at[0], 1)]
    greeted = greet_line(barrier, 1) + greet(
        barrier,
        (
            ((i > 0) & (k < n_z - 1), i - 1, k + 1),
            ((i < n_x - 1) & (k > 0), i + 1, k - 1),
        ),
    )
    for step in range(1, n_z):
        signal(barrier, i, lax.rem(k + step, n_z))
    greeted = greeted + n_z - 1

    perm_load = pltpu.make_async_copy(perm_hbm, perm, load_sem.at[6])
    perm_load.start()
    loads.append(load(mat_hbm, mat, 2))
    loads.append(load(g_hbm, outer, 3))
    loads.append(load(k_hbm, inner.at[1], 4))
    loads.append(load(own_hbm, own, 5))

    rows = lax.broadcasted_iota(jnp.int32, (nx, ny), 0)
    lanes = lax.broadcasted_iota(jnp.int32, (nx, ny), 1)
    first_row, last_row = rows == 0, rows == nx - 1
    first_lane, last_lane = lanes == 0, lanes == ny - 1

    def dy(v):
        return jnp.where(last_lane, 0.0, pltpu.roll(v, ny - 1, 1)) - v

    def dx(v):
        return jnp.where(last_row, 0.0, pltpu.roll(v, nx - 1, 0)) - v

    def by(v):
        return v - jnp.where(first_lane, 0.0, pltpu.roll(v, 1, 1))

    def bx(v, row):
        return v - jnp.where(first_row, row, pltpu.roll(v, 1, 0))

    def local_part(q, mag):
        scale = SCALES[q % 2]
        f = field.at[q]
        for z in range(nz):
            fx, fy, fz = f[0, z], f[1, z], f[2, z]
            if z < nz - 1:
                up_x, up_y = f[0, z + 1] - fx, f[1, z + 1] - fy
            else:
                up_x, up_y = -fx, -fy
            lx = mag[0, z] + scale * (dy(fz) - up_y)
            ly = mag[1, z] + scale * (up_x - dx(fz))
            lz = mag[2, z] + scale * (dx(fy) - dy(fx))
            partial[q, 0, z], partial[q, 1, z], partial[q, 2, z] = lx, ly, lz
            if q:
                send_xf[q, 0, z : z + 1] = fy[0:1]
                send_xf[q, 1, z : z + 1] = fz[0:1]
            send_xl[q, z : z + 1] = ly[nx - 1 : nx]
            send_xl[q, nz + z : nz + z + 1] = lz[nx - 1 : nx]
            if q and z == 0:
                send_d5[q] = fx[nx - 1 : nx]
            if q and z == nz - 1:
                send_d6[q] = fz[0:1]

    def messages(q):
        below_x, above_x = i > 0, i < n_x - 1
        below_z, above_z = k > 0, k < n_z - 1
        sources = (
            (
                e_hbm.at[0, nx - 1 : nx, 0], e_hbm.at[2, 0:1, nz - 1],
                e_hbm.at[1:3, 0], e_hbm.at[0:2, :, 0],
            )
            if q == 0
            else (send_d5.at[q], send_d6.at[q], send_xf.at[q], field.at[q, 0:2, 0])
        )
        top = partial.at[q, 0:2, nz - 1]
        return (
            (sources[0], got_d5.at[q], (i + 1, k - 1), above_x & below_z),
            (sources[1], got_d6.at[q], (i - 1, k + 1), below_x & above_z),
            (sources[2], got_xf.at[q], (i - 1, k), below_x),
            (send_xl.at[q], got_xl.at[q], (i + 1, k), above_x),
            (sources[3].at[0], got_zf.at[q, 0], (i, k - 1), below_z),
            (top.at[0], got_zl.at[q, 0], (i, k + 1), above_z),
            (sources[3].at[1], got_zf.at[q, 1], (i, k - 1), below_z),
            (top.at[1], got_zl.at[q, 1], (i, k + 1), above_z),
        )

    def send(q, *chosen):
        for m, (src, dst, target, sends) in enumerate(messages(q)):
            if m in chosen:
                awaited = m in PLANES and q % 2 == 0
                copy = pltpu.make_async_remote_copy(
                    src_ref=src, dst_ref=dst, device_id=target, device_id_type=MESH,
                    send_sem=plane_sent.at[q // 2] if awaited else send_sem,
                    recv_sem=recv_sem.at[q],
                )
                pl.when(sends)(copy.start)

    sides = []
    for below_x, above_x, below_z, above_z in itertools.product((False, True), repeat=4):
        if below_x + above_x > n_x - 1 or below_z + above_z > n_z - 1:
            continue
        if (n_x > 1 and not below_x + above_x) or (n_z > 1 and not below_z + above_z):
            continue
        here = ((i > 0) == below_x) & ((i < n_x - 1) == above_x)
        here = here & ((k > 0) == below_z) & ((k < n_z - 1) == above_z)
        length = (above_x & below_z) + (below_x & above_z) + 2 * nz * (below_x + above_x)
        sides.append((here, length, nx * (below_z + above_z)))

    def wait_exchange(sem, lines, planes):
        for here, length, plane in sides:
            if lines * length + planes * plane:
                span = tally.at[0 : lines * length + planes * plane]
                pl.when(here)(pltpu.make_async_copy(span, span, sem).wait)

    def receive(q):
        wait_exchange(recv_sem.at[q], 1, 2)

    def finish(q, put):
        scale = SCALES[q % 2]
        f, part = field.at[q], partial.at[q]
        not_first_x, not_last_x = i > 0, i < n_x - 1
        not_first_z, not_last_z = k > 0, k < n_z - 1

        def only(cond, v):
            return jnp.where(cond, v, 0.0)

        below_x = only(not_first_z, got_zl[q, 0] - scale * f[1, 0])
        below_y = got_zl[q, 1] + scale * f[0, 0]
        diagonal = only(not_last_x, scale * got_d6[q])
        below_y = only(not_first_z, below_y - jnp.where(last_row, diagonal, 0.0))
        result = []
        for z in range(nz):
            mx, my, mz = part[0, z], part[1, z], part[2, z]
            edge_y = got_xl[q, z : z + 1] - scale * f[2, z, 0:1]
            edge_z = got_xl[q, nz + z : nz + z + 1] + scale * f[1, z, 0:1]
            if z == nz - 1:
                mx = mx - only(not_last_z, scale * got_zf[q, 1])
                my = my + only(not_last_z, scale * got_zf[q, 0])
                edge_y = edge_y + only(not_last_z, scale * got_d5[q])
            edge_y, edge_z = only(not_first_x, edge_y), only(not_first_x, edge_z)
            next_y = only(not_last_x, scale * got_xf[q, 0, z : z + 1])
            next_z = only(not_last_x, scale * got_xf[q, 1, z : z + 1])
            my = my - jnp.where(last_row, next_z, 0.0)
            mz = mz + jnp.where(last_row, next_y, 0.0)
            if put is not None:
                put[0, z], put[1, z], put[2, z] = mx, my, mz
            result.append(
                (
                    by(mz) - (my - below_y),
                    (mx - below_x) - bx(mz, edge_z),
                    bx(my, edge_y) - by(mx),
                )
            )
            below_x, below_y = mx, my
        return result

    def open_exchange(*chosen):
        pl.semaphore_wait(barrier, greeted)
        send(0, *chosen)

    pl.when(k == n_z - 1)(functools.partial(open_exchange, 4, 6, 0, 1, 2))
    for slot in (0, 1):
        loads[slot].wait()
    local_part(0, inner.at[0])
    pl.when(k < n_z - 1)(functools.partial(open_exchange, 5, 7, 4, 6, 0, 1, 2))
    send(0, 3)
    hops = [1 << turn for turn in range((n_x - 1).bit_length())]
    told = [greet_line(line_sem.at[0], 1)]

    def tell():
        turn = len(told)
        if turn <= len(hops):
            pl.semaphore_wait(line_sem.at[turn - 1], told[-1])
            told.append(greet_line(line_sem.at[turn], hops[turn]) if turn < len(hops) else 0)

    perm_load.wait()
    for slot in (2, 3, 4):
        loads[slot].wait()
    for z in range(nz):
        kind = mat[z]
        eps = jnp.full((nx, ny), perm[0], jnp.float32)
        for number in range(1, kinds):
            eps = jnp.where(kind == number, perm[number], eps)
        coef[z] = COURANT / eps
        for c in range(3):
            field[1, c, z] = coef[z] * outer[c, z]
    local_part(1, inner.at[1])
    send(1, *LINES)
    pl.when(odd)(functools.partial(wait_exchange, plane_sent.at[0], 0, 2))
    send(1, *PLANES)
    tell()
    tell()

    receive(0)
    change = finish(0, curl_in.at[0])
    for z in range(nz):
        for c in range(3):
            moved = coef[z] * change[z][c]
            curl_in[2, c, z] = moved
            field[2, c, z] = field[0, c, z] + moved
    local_part(2, curl_in.at[0])
    send(2, *LINES, *PLANES)
    tell()

    receive(1)
    change = finish(1, curl_in.at[1])
    for z in range(nz):
        dot = None
        for c in range(3):
            now = outer[c, z] - COURANT * change[z][c]
            inner[1, c, z] = now
            field[3, c, z] = coef[z] * now
            term = now * curl_in[2, c, z]
            dot = term if dot is None else dot + term
        weight[z] = coef[z] * dot
    local_part(3, curl_in.at[1])
    send(3, *LINES)
    pl.when(~odd)(functools.partial(send, 3, *PLANES))
    wait_exchange(plane_sent.at[1], 0, 2)
    pl.when(~odd & (i < n_x - 1))(functools.partial(signal, pair_sem, i + 1, k))

    @pl.when(odd)
    def _():
        pl.semaphore_wait(pair_sem, 1)
        send(3, *PLANES)

    loads[5].wait()

    receive(2)
    change = finish(2, None)
    sums = [jnp.zeros((nx, 128), jnp.float32)] * NI
    for z in range(nz):
        dot = None
        for c in range(3):
            term = outer[c, z] * (coef[z] * change[z][c])
            dot = term if dot is None else dot + term
        both = weight[z] + coef[z] * dot
        which = own[z]
        for t in range(0, ny, 128):
            part, index = both[:, t : t + 128], which[:, t : t + 128]
            for j in range(NI):
                sums[j] = sums[j] + jnp.where(index == j, part, 0.0)
    lane = lax.broadcasted_iota(jnp.int32, (1, 128), 1)
    row = jnp.zeros((1, 128), jnp.float32)
    for j in range(NI):
        column = jnp.sum(sums[j], axis=0, keepdims=True)
        row = jnp.where(lane == j, jnp.sum(column, axis=1, keepdims=True), row)
    mine[0] = row
    gathered[me] = row

    while len(told) <= len(hops):
        tell()

    def share_sum(step, carry):
        other = jnp.where(step < me, step, step + 1)
        pltpu.make_async_remote_copy(
            src_ref=mine.at[0], dst_ref=gathered.at[me], send_sem=sum_send, recv_sem=sum_recv,
            device_id=(other // n_z, lax.rem(other, n_z)), device_id_type=MESH,
        ).start()
        return carry

    lax.fori_loop(0, total - 1, share_sum, 0)

    receive(3)
    change = finish(3, ko_ref)
    for z in range(nz):
        for c in range(3):
            go_ref[c, z] = inner[1, c, z] - COURANT * change[z][c]
    everyone = gathered.at[0 : total - 1]
    pltpu.make_async_copy(everyone, everyone, sum_recv).wait()
    pltpu.make_async_copy(everyone, everyone, sum_send).wait()
    grad_ref[...] = jnp.sum(gathered[...], axis=0)[:, :NI] / norm
    wait_exchange(send_sem, 4, 4)
    pl.when(~odd)(functools.partial(wait_exchange, plane_sent.at[0], 0, 2))

def store(g_ref, h_ref, grad_ref, g_hbm, h_hbm, grad_hbm, sem):
    pltpu.make_async_copy(grad_ref, grad_hbm, sem.at[2]).start()
    for z in range(g_ref.shape[1]):
        pltpu.make_async_copy(g_ref.at[:, z], g_hbm.at[:, :, z, :], sem.at[0]).start()
        pltpu.make_async_copy(h_ref.at[:, z], h_hbm.at[:, :, z, :], sem.at[1]).start()
    for n, ref in enumerate((g_ref, h_ref, grad_ref)):
        pltpu.make_async_copy(ref, ref, sem.at[n]).wait()


def solution(mesh):
    n_x, n_z = mesh.shape["xy"], mesh.shape["gz"]

    def body(e_check, h_check, adj_e, adj_h, material, owner, permittivity):
        _, nx, nz, ny = e_check.shape
        cells = nx * n_x * nz * n_z * ny
        norm = np.sqrt(np.float32(cells / NI))
        dims = (n_x, n_z, nx, nz, ny, permittivity.shape[0], norm)
        f32 = jnp.float32
        hbm_spec = pl.BlockSpec(memory_space=pltpu.HBM)
        vmem_spec = pl.BlockSpec(memory_space=pltpu.VMEM)
        block = (3, nz, nx, ny)
        g, h, grad = pl.pallas_call(
            functools.partial(kernel, dims),
            out_shape=(
                pltpu.VMEM(block, f32), pltpu.VMEM(block, f32), pltpu.VMEM((1, NI), f32),
            ),
            in_specs=[hbm_spec] * 7,
            out_specs=(vmem_spec,) * 3,
            scratch_shapes=[
                pltpu.SMEM(permittivity.shape, f32),
                pltpu.VMEM((4,) + block, f32),
                pltpu.VMEM((2,) + block, f32),
                pltpu.VMEM((4,) + block, f32),
                pltpu.VMEM((3,) + block, f32),
                pltpu.VMEM(block, f32),
                pltpu.VMEM((nz, nx, ny), jnp.int32),
                pltpu.VMEM((nz, nx, ny), jnp.int32),
                pltpu.VMEM((nz, nx, ny), f32),
                pltpu.VMEM((nz, nx, ny), f32),
                pltpu.VMEM((4, 2, nz, ny), f32),
                pltpu.VMEM((4, 2 * nz, ny), f32),
                pltpu.VMEM((4, 1, ny), f32),
                pltpu.VMEM((4, 1, ny), f32),
                pltpu.VMEM((4, 2, nz, ny), f32),
                pltpu.VMEM((4, 2, nx, ny), f32),
                pltpu.VMEM((4, 2 * nz, ny), f32),
                pltpu.VMEM((4, 2, nx, ny), f32),
                pltpu.VMEM((4, 1, ny), f32),
                pltpu.VMEM((4, 1, ny), f32),
                pltpu.VMEM((1, 1, 128), f32),
                pltpu.VMEM((n_x * n_z, 1, 128), f32),
                pltpu.VMEM((8 * (1 + 2 * nz + 2 * nx), 1, ny), f32),
                pltpu.SemaphoreType.DMA((7,)),
                pltpu.SemaphoreType.DMA,
                pltpu.SemaphoreType.DMA((2,)),
                pltpu.SemaphoreType.DMA((4,)),
                pltpu.SemaphoreType.DMA,
                pltpu.SemaphoreType.DMA,
                pltpu.SemaphoreType.REGULAR((max(1, (n_x - 1).bit_length()),)),
                pltpu.SemaphoreType.REGULAR,
            ],
            compiler_params=pltpu.CompilerParams(
                collective_id=0, has_side_effects=True
            ),
            name="yee_adjoint",
        )(e_check, h_check, adj_e, adj_h, material, owner, permittivity)
        g, h, grad = pl.pallas_call(
            store,
            out_shape=(
                jax.ShapeDtypeStruct(e_check.shape, f32),
                jax.ShapeDtypeStruct(e_check.shape, f32),
                jax.ShapeDtypeStruct((1, NI), f32),
            ),
            in_specs=[vmem_spec] * 3,
            out_specs=(hbm_spec,) * 3,
            scratch_shapes=[pltpu.SemaphoreType.DMA((3,))],
            compiler_params=pltpu.CompilerParams(vmem_limit_bytes=2**20),
            name="store_outputs",
        )(g, h, grad)
        return g, h, grad.reshape(NI)

    split = P(None, "xy", "gz", None)
    return jax.shard_map(
        body,
        mesh=mesh,
        in_specs=(split,) * 4 + (P("xy", "gz", None),) * 2 + (P(),),
        out_specs=(split, split, P()),
        check_vma=False,
    )
```

```python
import functools
import itertools

import jax
import jax.numpy as jnp
import numpy as np
from jax import lax
from jax.experimental import pallas as pl
from jax.experimental.pallas import tpu as pltpu
from jax.sharding import PartitionSpec as P

NI = 8
COURANT = 0.5
MESH = pl.DeviceIdType.MESH
LINES, PLANES = (0, 1, 2, 3), (4, 5)
SCALES = (-COURANT, 1.0)


def kernel(
    dims, e_hbm, h_hbm, g_hbm, k_hbm, mat_hbm, own_hbm, perm_hbm,
    go_ref, ko_ref, grad_ref,
    perm, field, inner, partial, curl_in, outer, mat, own, coef, weight,
    send_xf, send_xl, send_d5, send_d6,
    got_xf, got_zf, got_xl, got_zl, got_d5, got_d6,
    mine, gathered, tally,
    load_sem, send_sem, plane_sent, recv_sem, sum_send, sum_recv,
    line_sem, pair_sem,
):
    n_x, n_z, nx, nz, ny, kinds, norm = dims
    total = n_x * n_z
    i = lax.axis_index("xy")
    k = lax.axis_index("gz")
    me = i * n_z + k
    odd = lax.rem(i, 2) == 1

    def load(src, dst, slot):
        for z in range(nz):
            src_z = src.at[:, :, z, :] if len(src.shape) == 4 else src.at[:, z, :]
            dst_z = dst.at[:, z] if len(src.shape) == 4 else dst.at[z]
            pltpu.make_async_copy(src_z, dst_z, load_sem.at[slot]).start()
        return pltpu.make_async_copy(dst, dst, load_sem.at[slot])

    barrier = pltpu.get_barrier_semaphore()

    def signal(sem, x, z):
        pl.semaphore_signal(sem, inc=1, device_id=(x, z), device_id_type=MESH)

    def greet(sem, partners):
        count = 0
        for cond, x, z in partners:
            pl.when(cond)(functools.partial(signal, sem, x, z))
            count = count + cond.astype(jnp.int32)
        return count

    def greet_line(sem, hop):
        return greet(sem, ((i >= hop, i - hop, k), (i < n_x - hop, i + hop, k)))

    loads = [load(e_hbm, field.at[0], 0), load(h_hbm, inner.at[0], 1)]
    greeted = greet_line(barrier, 1) + greet(
        barrier,
        (
            ((i > 0) & (k < n_z - 1), i - 1, k + 1),
            ((i < n_x - 1) & (k > 0), i + 1, k - 1),
        ),
    )
    for step in range(1, n_z):
        signal(barrier, i, lax.rem(k + step, n_z))
    greeted = greeted + n_z - 1

    perm_load = pltpu.make_async_copy(perm_hbm, perm, load_sem.at[6])
    perm_load.start()
    loads.append(load(mat_hbm, mat, 2))
    loads.append(load(g_hbm, outer, 3))
    loads.append(load(k_hbm, inner.at[1], 4))
    loads.append(load(own_hbm, own, 5))

    rows = lax.broadcasted_iota(jnp.int32, (nx, ny), 0)
    lanes = lax.broadcasted_iota(jnp.int32, (nx, ny), 1)

    def first_row(v):
        return rows[:, : v.shape[1]] == 0

    def last_row(v):
        return rows[:, : v.shape[1]] == nx - 1

    def dy(v, whole):
        width = v.shape[1]
        later = pltpu.roll(v, width - 1, 1)
        return jnp.where(lanes[:, :width] == width - 1, 0.0, later) - v if whole else later - v

    def dx(v):
        return jnp.where(last_row(v), 0.0, pltpu.roll(v, nx - 1, 0)) - v

    def by(v, whole):
        earlier = pltpu.roll(v, 1, 1)
        return v - (jnp.where(lanes[:, : v.shape[1]] == 0, 0.0, earlier) if whole else earlier)

    def bx(v, row):
        return v - jnp.where(first_row(v), row, pltpu.roll(v, 1, 0))

    def local_part(q, mag, low=0, high=ny):
        scale = SCALES[q % 2]
        end = min(high + 128, ny)
        inside, keep = pl.ds(low, end - low), pl.ds(low, high - low)
        width = high - low

        def put(ref, index, v):
            ref[index + (keep,)] = v[:, :width]

        for z in range(nz):
            fx, fy, fz = (field[q, c, z, :, inside] for c in range(3))
            if z < nz - 1:
                up_x, up_y = (field[q, c, z + 1, :, inside] for c in range(2))
                up_x, up_y = up_x - fx, up_y - fy
            else:
                up_x, up_y = -fx, -fy
            whole = end == high
            lx = mag[0, z, :, inside] + scale * (dy(fz, whole) - up_y)
            ly = mag[1, z, :, inside] + scale * (up_x - dx(fz))
            lz = mag[2, z, :, inside] + scale * (dx(fy) - dy(fx, whole))
            for c, v in enumerate((lx, ly, lz)):
                put(partial, (q, c, z, slice(None)), v)
            if q:
                put(send_xf, (q, 0, slice(z, z + 1)), fy[0:1])
                put(send_xf, (q, 1, slice(z, z + 1)), fz[0:1])
            put(send_xl, (q, slice(z, z + 1)), ly[nx - 1 : nx])
            put(send_xl, (q, slice(nz + z, nz + z + 1)), lz[nx - 1 : nx])
            if q and z == 0:
                put(send_d5, (q, slice(None)), fx[nx - 1 : nx])
            if q and z == nz - 1:
                put(send_d6, (q, slice(None)), fz[0:1])

    cut = ny * 4 // 8 // 128 * 128 if ny >= 512 and ny % 128 == 0 else ny
    spans = [((0, ny),)] * 4
    if cut < ny:
        spans[0], spans[2] = ((0, cut), (cut, ny)), ((0, cut - 128), (cut - 128, ny))
    widths = [high - low for low, high in spans[0]]

    def messages(q):
        below_x, above_x = i > 0, i < n_x - 1
        below_z, above_z = k > 0, k < n_z - 1
        sources = (
            (
                e_hbm.at[0, nx - 1 : nx, 0], e_hbm.at[2, 0:1, nz - 1],
                e_hbm.at[1:3, 0], e_hbm.at[0:2, :, 0],
            )
            if q == 0
            else (send_d5.at[q], send_d6.at[q], send_xf.at[q], field.at[q, 0:2, 0])
        )
        table = [
            (sources[0], got_d5.at[q], (i + 1, k - 1), above_x & below_z),
            (sources[1], got_d6.at[q], (i - 1, k + 1), below_x & above_z),
            (sources[2], got_xf.at[q], (i - 1, k), below_x),
            (send_xl.at[q], got_xl.at[q], (i + 1, k), above_x),
        ]
        top = partial.at[q, 0:2, nz - 1]
        for low, high in spans[q]:
            keep = pl.ds(low, high - low)
            for src, got, target, sends in (
                (sources[3], got_zf, (i, k - 1), below_z), (top, got_zl, (i, k + 1), above_z),
            ):
                table.append((src.at[:, :, keep], got.at[q, :, :, keep], target, sends))
        return table

    def send(q, *chosen):
        table = messages(q)
        for m in chosen:
            src, dst, target, sends = table[m]
            sent, late = send_sem, q == 0 and m >= 6
            if m >= 4 and q % 2 == 0:
                sent = plane_sent.at[q + late]
            copy = pltpu.make_async_remote_copy(
                src_ref=src, dst_ref=dst, device_id=target, device_id_type=MESH,
                send_sem=sent, recv_sem=recv_sem.at[4 if late else q],
            )
            pl.when(sends)(copy.start)

    sides = []
    for below_x, above_x, below_z, above_z in itertools.product((False, True), repeat=4):
        if below_x + above_x > n_x - 1 or below_z + above_z > n_z - 1:
            continue
        if (n_x > 1 and not below_x + above_x) or (n_z > 1 and not below_z + above_z):
            continue
        here = ((i > 0) == below_x) & ((i < n_x - 1) == above_x)
        here = here & ((k > 0) == below_z) & ((k < n_z - 1) == above_z)
        length = (above_x & below_z) + (below_x & above_z) + 2 * nz * (below_x + above_x)
        sides.append((here, length, 2 * nx * (below_z + above_z)))

    def wait_exchange(sem, lines, *widths):
        for here, length, plane in sides:
            count = (lines * length * ny + plane * sum(widths)) // 128
            if count:
                span = tally.at[0:count]
                pl.when(here)(pltpu.make_async_copy(span, span, sem).wait)

    def finish(q, put, low=0, high=ny):
        scale = SCALES[q % 2]
        start = max(low - 128, 0)
        inside = pl.ds(start, high - start)
        not_first_x, not_last_x = i > 0, i < n_x - 1
        not_first_z, not_last_z = k > 0, k < n_z - 1

        def only(cond, v):
            return jnp.where(cond, v, 0.0)

        def f(c, z, part=slice(None)):
            return field[q, c, z, part, inside]

        bottom_x, bottom_y = got_zl[q, 0, :, inside], got_zl[q, 1, :, inside]
        below_x = only(not_first_z, bottom_x - scale * f(1, 0))
        below_y = bottom_y + scale * f(0, 0)
        diagonal = only(not_last_x, scale * got_d6[q, :, inside])
        below_y = only(not_first_z, below_y - jnp.where(last_row(below_y), diagonal, 0.0))
        result = []
        for z in range(nz):
            mx, my, mz = (partial[q, c, z, :, inside] for c in range(3))
            edge_y = got_xl[q, z : z + 1, inside] - scale * f(2, z, slice(0, 1))
            edge_z = got_xl[q, nz + z : nz + z + 1, inside] + scale * f(1, z, slice(0, 1))
            if z == nz - 1:
                mx = mx - only(not_last_z, scale * got_zf[q, 1, :, inside])
                my = my + only(not_last_z, scale * got_zf[q, 0, :, inside])
                edge_y = edge_y + only(not_last_z, scale * got_d5[q, :, inside])
            edge_y, edge_z = only(not_first_x, edge_y), only(not_first_x, edge_z)
            next_y = only(not_last_x, scale * got_xf[q, 0, z : z + 1, inside])
            next_z = only(not_last_x, scale * got_xf[q, 1, z : z + 1, inside])
            my = my - jnp.where(last_row(my), next_z, 0.0)
            mz = mz + jnp.where(last_row(mz), next_y, 0.0)
            curl = (
                by(mz, start == 0) - (my - below_y),
                (mx - below_x) - bx(mz, edge_z),
                bx(my, edge_y) - by(mx, start == 0),
            )
            if put is not None:
                for c, v in enumerate((mx, my, mz)):
                    put[c, z, :, pl.ds(low, high - low)] = v[:, low - start :]
            result.append([v[:, low - start :] for v in curl])
            below_x, below_y = mx, my
        return result

    def open_exchange(*chosen):
        pl.semaphore_wait(barrier, greeted)
        send(0, *chosen)

    downs = [4 + 2 * n for n in range(len(widths))]
    ups = [n + 1 for n in downs]
    both = [n for pair in zip(ups, downs) for n in pair]
    pl.when(k == n_z - 1)(functools.partial(open_exchange, 0, 1, *downs, 2))
    for slot in (0, 1):
        loads[slot].wait()
    local_part(0, inner.at[0])
    pl.when(k < n_z - 1)(functools.partial(open_exchange, 0, 1, *both, 2))
    send(0, 3)
    hops = [1 << turn for turn in range((n_x - 1).bit_length())]
    told = [greet_line(line_sem.at[0], 1)]

    def tell():
        turn = len(told)
        if turn <= len(hops):
            pl.semaphore_wait(line_sem.at[turn - 1], told[-1])
            told.append(greet_line(line_sem.at[turn], hops[turn]) if turn < len(hops) else 0)

    perm_load.wait()
    for slot in (2, 3, 4):
        loads[slot].wait()
    for z in range(nz):
        kind = mat[z]
        eps = jnp.full((nx, ny), perm[0], jnp.float32)
        for number in range(1, kinds):
            eps = jnp.where(kind == number, perm[number], eps)
        coef[z] = COURANT / eps
        for c in range(3):
            field[1, c, z] = coef[z] * outer[c, z]
    local_part(1, inner.at[1])
    send(1, *LINES)
    wait_exchange(plane_sent.at[0], 0, widths[0])
    if len(widths) > 1:
        pl.when(odd)(functools.partial(wait_exchange, plane_sent.at[1], 0, widths[1]))
    send(1, *PLANES)
    tell()
    tell()

    for n, (low, high) in enumerate(spans[0]):
        wait_exchange(recv_sem.at[4 if n else 0], int(n == 0), high - low)
        change = finish(0, curl_in.at[0], low, high)
        keep = pl.ds(low, high - low)
        for z in range(nz):
            for c in range(3):
                moved = coef[z, :, keep] * change[z][c]
                curl_in[2, c, z, :, keep] = moved
                field[2, c, z, :, keep] = field[0, c, z, :, keep] + moved
        local_part(2, curl_in.at[0], *spans[2][n])
        send(2, 4 + 2 * n, 5 + 2 * n)
    send(2, *LINES)
    tell()

    wait_exchange(recv_sem.at[1], 1, ny)
    change = finish(1, curl_in.at[1])
    for z in range(nz):
        dot = None
        for c in range(3):
            now = outer[c, z] - COURANT * change[z][c]
            inner[1, c, z] = now
            field[3, c, z] = coef[z] * now
            term = now * curl_in[2, c, z]
            dot = term if dot is None else dot + term
        weight[z] = coef[z] * dot
    local_part(3, curl_in.at[1])
    send(3, *LINES)
    pl.when(~odd)(functools.partial(send, 3, *PLANES))
    wait_exchange(plane_sent.at[2], 0, ny)
    pl.when(~odd & (i < n_x - 1))(functools.partial(signal, pair_sem, i + 1, k))

    @pl.when(odd)
    def _():
        pl.semaphore_wait(pair_sem, 1)
        send(3, *PLANES)

    loads[5].wait()

    wait_exchange(recv_sem.at[2], 1, ny)
    change = finish(2, None)
    sums = [jnp.zeros((nx, 128), jnp.float32)] * NI
    for z in range(nz):
        dot = None
        for c in range(3):
            term = outer[c, z] * (coef[z] * change[z][c])
            dot = term if dot is None else dot + term
        both = weight[z] + coef[z] * dot
        which = own[z]
        for t in range(0, ny, 128):
            part, index = both[:, t : t + 128], which[:, t : t + 128]
            for j in range(NI):
                sums[j] = sums[j] + jnp.where(index == j, part, 0.0)
    lane = lax.broadcasted_iota(jnp.int32, (1, 128), 1)
    row = jnp.zeros((1, 128), jnp.float32)
    for j in range(NI):
        column = jnp.sum(sums[j], axis=0, keepdims=True)
        row = jnp.where(lane == j, jnp.sum(column, axis=1, keepdims=True), row)
    mine[0] = row
    gathered[me] = row

    while len(told) <= len(hops):
        tell()

    def share_sum(step, carry):
        other = jnp.where(step < me, step, step + 1)
        pltpu.make_async_remote_copy(
            src_ref=mine.at[0], dst_ref=gathered.at[me], send_sem=sum_send, recv_sem=sum_recv,
            device_id=(other // n_z, lax.rem(other, n_z)), device_id_type=MESH,
        ).start()
        return carry

    lax.fori_loop(0, total - 1, share_sum, 0)

    wait_exchange(recv_sem.at[3], 1, ny)
    change = finish(3, ko_ref)
    for z in range(nz):
        for c in range(3):
            go_ref[c, z] = inner[1, c, z] - COURANT * change[z][c]
    everyone = gathered.at[0 : total - 1]
    pltpu.make_async_copy(everyone, everyone, sum_recv).wait()
    pltpu.make_async_copy(everyone, everyone, sum_send).wait()
    grad_ref[...] = jnp.sum(gathered[...], axis=0)[:, :NI] / norm
    wait_exchange(send_sem, 4, 2 * ny)
    if len(widths) > 1:
        pl.when(~odd)(functools.partial(wait_exchange, plane_sent.at[1], 0, widths[1]))


def store(g_ref, h_ref, grad_ref, g_hbm, h_hbm, grad_hbm, sem):
    pltpu.make_async_copy(grad_ref, grad_hbm, sem.at[2]).start()
    for z in range(g_ref.shape[1]):
        pltpu.make_async_copy(g_ref.at[:, z], g_hbm.at[:, :, z, :], sem.at[0]).start()
        pltpu.make_async_copy(h_ref.at[:, z], h_hbm.at[:, :, z, :], sem.at[1]).start()
    for n, ref in enumerate((g_ref, h_ref, grad_ref)):
        pltpu.make_async_copy(ref, ref, sem.at[n]).wait()


def solution(mesh):
    n_x, n_z = mesh.shape["xy"], mesh.shape["gz"]

    def body(e_check, h_check, adj_e, adj_h, material, owner, permittivity):
        _, nx, nz, ny = e_check.shape
        cells = nx * n_x * nz * n_z * ny
        norm = np.sqrt(np.float32(cells / NI))
        dims = (n_x, n_z, nx, nz, ny, permittivity.shape[0], norm)
        f32 = jnp.float32
        hbm_spec = pl.BlockSpec(memory_space=pltpu.HBM)
        vmem_spec = pl.BlockSpec(memory_space=pltpu.VMEM)
        block = (3, nz, nx, ny)
        g, h, grad = pl.pallas_call(
            functools.partial(kernel, dims),
            out_shape=(
                pltpu.VMEM(block, f32), pltpu.VMEM(block, f32), pltpu.VMEM((1, NI), f32),
            ),
            in_specs=[hbm_spec] * 7,
            out_specs=(vmem_spec,) * 3,
            scratch_shapes=[
                pltpu.SMEM(permittivity.shape, f32),
                pltpu.VMEM((4,) + block, f32),
                pltpu.VMEM((2,) + block, f32),
                pltpu.VMEM((4,) + block, f32),
                pltpu.VMEM((3,) + block, f32),
                pltpu.VMEM(block, f32),
                pltpu.VMEM((nz, nx, ny), jnp.int32),
                pltpu.VMEM((nz, nx, ny), jnp.int32),
                pltpu.VMEM((nz, nx, ny), f32),
                pltpu.VMEM((nz, nx, ny), f32),
                pltpu.VMEM((4, 2, nz, ny), f32),
                pltpu.VMEM((4, 2 * nz, ny), f32),
                pltpu.VMEM((4, 1, ny), f32),
                pltpu.VMEM((4, 1, ny), f32),
                pltpu.VMEM((4, 2, nz, ny), f32),
                pltpu.VMEM((4, 2, nx, ny), f32),
                pltpu.VMEM((4, 2 * nz, ny), f32),
                pltpu.VMEM((4, 2, nx, ny), f32),
                pltpu.VMEM((4, 1, ny), f32),
                pltpu.VMEM((4, 1, ny), f32),
                pltpu.VMEM((1, 1, 128), f32),
                pltpu.VMEM((n_x * n_z, 1, 128), f32),
                pltpu.VMEM((8 * (1 + 2 * nz + 2 * nx) * ny // 128, 1, 128), f32),
                pltpu.SemaphoreType.DMA((7,)),
                pltpu.SemaphoreType.DMA,
                pltpu.SemaphoreType.DMA((3,)),
                pltpu.SemaphoreType.DMA((5,)),
                pltpu.SemaphoreType.DMA,
                pltpu.SemaphoreType.DMA,
                pltpu.SemaphoreType.REGULAR((max(1, (n_x - 1).bit_length()),)),
                pltpu.SemaphoreType.REGULAR,
            ],
            compiler_params=pltpu.CompilerParams(
                collective_id=0, has_side_effects=True
            ),
            name="yee_adjoint",
        )(e_check, h_check, adj_e, adj_h, material, owner, permittivity)
        g, h, grad = pl.pallas_call(
            store,
            out_shape=(
                jax.ShapeDtypeStruct(e_check.shape, f32),
                jax.ShapeDtypeStruct(e_check.shape, f32),
                jax.ShapeDtypeStruct((1, NI), f32),
            ),
            in_specs=[vmem_spec] * 3,
            out_specs=(hbm_spec,) * 3,
            scratch_shapes=[pltpu.SemaphoreType.DMA((3,))],
            compiler_params=pltpu.CompilerParams(vmem_limit_bytes=2**20),
            name="store_outputs",
        )(g, h, grad)
        return g, h, grad.reshape(NI)

    split = P(None, "xy", "gz", None)
    return jax.shard_map(
        body,
        mesh=mesh,
        in_specs=(split,) * 4 + (P("xy", "gz", None),) * 2 + (P(),),
        out_specs=(split, split, P()),
        check_vma=False,
    )
```

```python
import functools
import itertools

import jax
import jax.numpy as jnp
import numpy as np
from jax import lax
from jax.experimental import pallas as pl
from jax.experimental.pallas import tpu as pltpu
from jax.sharding import PartitionSpec as P

NI = 8
COURANT = 0.5
MESH = pl.DeviceIdType.MESH
LINES, PLANES = (0, 1, 2, 3), (4, 5)
SCALES = (-COURANT, 1.0)


def kernel(
    dims, e_hbm, h_hbm, g_hbm, k_hbm, mat_hbm, own_hbm, perm_hbm,
    go_ref, ko_ref, grad_ref,
    perm, field, inner, partial, curl_in, outer, mat, own, coef, weight,
    send_xf, send_xl, send_d5, send_d6,
    got_xf, got_zf, got_xl, got_zl, got_d5, got_d6,
    mine, gathered, tally,
    pair_zf, pair_zl, pair_give, pair_weight, pair_own,
    load_sem, send_sem, plane_sent, recv_sem, sum_send, sum_recv,
    line_sem, pair_sem, pair_sent, pair_got,
):
    n_x, n_z, nx, nz, ny, kinds, norm = dims
    total = n_x * n_z
    i = lax.axis_index("xy")
    k = lax.axis_index("gz")
    me = i * n_z + k
    odd = lax.rem(i, 2) == 1

    def load(src, dst, slot):
        for z in range(nz):
            src_z = src.at[:, :, z, :] if len(src.shape) == 4 else src.at[:, z, :]
            dst_z = dst.at[:, z] if len(src.shape) == 4 else dst.at[z]
            pltpu.make_async_copy(src_z, dst_z, load_sem.at[slot]).start()
        return pltpu.make_async_copy(dst, dst, load_sem.at[slot])

    barrier = pltpu.get_barrier_semaphore()

    def signal(sem, x, z):
        pl.semaphore_signal(sem, inc=1, device_id=(x, z), device_id_type=MESH)

    def greet(sem, partners):
        count = 0
        for cond, x, z in partners:
            pl.when(cond)(functools.partial(signal, sem, x, z))
            count = count + cond.astype(jnp.int32)
        return count

    def greet_line(sem, hop):
        return greet(sem, ((i >= hop, i - hop, k), (i < n_x - hop, i + hop, k)))

    loads = [load(e_hbm, field.at[0], 0), load(h_hbm, inner.at[0], 1)]
    greeted = greet_line(barrier, 1) + greet(
        barrier,
        (
            ((i > 0) & (k < n_z - 1), i - 1, k + 1),
            ((i < n_x - 1) & (k > 0), i + 1, k - 1),
        ),
    )
    for step in range(1, n_z):
        signal(barrier, i, lax.rem(k + step, n_z))
    greeted = greeted + n_z - 1

    perm_load = pltpu.make_async_copy(perm_hbm, perm, load_sem.at[6])
    perm_load.start()
    loads.append(load(mat_hbm, mat, 2))
    loads.append(load(g_hbm, outer, 3))
    loads.append(load(k_hbm, inner.at[1], 4))
    loads.append(load(own_hbm, own, 5))

    rows = lax.broadcasted_iota(jnp.int32, (nx, ny), 0)
    lanes = lax.broadcasted_iota(jnp.int32, (nx, ny), 1)

    def first_row(v):
        return rows[:, : v.shape[1]] == 0

    def last_row(v):
        return rows[:, : v.shape[1]] == nx - 1

    def dy(v, whole):
        width = v.shape[1]
        later = pltpu.roll(v, width - 1, 1)
        return jnp.where(lanes[:, :width] == width - 1, 0.0, later) - v if whole else later - v

    def dx(v):
        return jnp.where(last_row(v), 0.0, pltpu.roll(v, nx - 1, 0)) - v

    def by(v, whole):
        earlier = pltpu.roll(v, 1, 1)
        return v - (jnp.where(lanes[:, : v.shape[1]] == 0, 0.0, earlier) if whole else earlier)

    def bx(v, row):
        return v - jnp.where(first_row(v), row, pltpu.roll(v, 1, 0))

    def local_part(q, mag, low=0, high=ny):
        scale = SCALES[q % 2]
        end = min(high + 128, ny)
        inside, keep = pl.ds(low, end - low), pl.ds(low, high - low)
        width = high - low

        def put(ref, index, v):
            ref[index + (keep,)] = v[:, :width]

        for z in range(nz):
            fx, fy, fz = (field[q, c, z, :, inside] for c in range(3))
            if z < nz - 1:
                up_x, up_y = (field[q, c, z + 1, :, inside] for c in range(2))
                up_x, up_y = up_x - fx, up_y - fy
            else:
                up_x, up_y = -fx, -fy
            whole = end == high
            lx = mag[0, z, :, inside] + scale * (dy(fz, whole) - up_y)
            ly = mag[1, z, :, inside] + scale * (up_x - dx(fz))
            lz = mag[2, z, :, inside] + scale * (dx(fy) - dy(fx, whole))
            for c, v in enumerate((lx, ly, lz)):
                put(partial, (q, c, z, slice(None)), v)
            if q:
                put(send_xf, (q, 0, slice(z, z + 1)), fy[0:1])
                put(send_xf, (q, 1, slice(z, z + 1)), fz[0:1])
            put(send_xl, (q, slice(z, z + 1)), ly[nx - 1 : nx])
            put(send_xl, (q, slice(nz + z, nz + z + 1)), lz[nx - 1 : nx])
            if q and z == 0:
                put(send_d5, (q, slice(None)), fx[nx - 1 : nx])
            if q and z == nz - 1:
                put(send_d6, (q, slice(None)), fz[0:1])

    spans = [((0, ny),)] * 4
    if ny % 1024 == 0:
        cuts = [ny // 8 * n for n in (4,)]
        spans[0] = tuple(zip([0] + cuts, cuts + [ny]))
        ahead = [n - 128 for n in cuts]
        spans[2] = tuple(zip([0] + ahead, ahead + [ny]))
    widths = [high - low for low, high in spans[0]]

    def messages(q):
        below_x, above_x = i > 0, i < n_x - 1
        below_z, above_z = k > 0, k < n_z - 1
        sources = (
            (
                e_hbm.at[0, nx - 1 : nx, 0], e_hbm.at[2, 0:1, nz - 1],
                e_hbm.at[1:3, 0], e_hbm.at[0:2, :, 0],
            )
            if q == 0
            else (send_d5.at[q], send_d6.at[q], send_xf.at[q], field.at[q, 0:2, 0])
        )
        table = [
            (sources[0], got_d5.at[q], (i + 1, k - 1), above_x & below_z),
            (sources[1], got_d6.at[q], (i - 1, k + 1), below_x & above_z),
            (sources[2], got_xf.at[q], (i - 1, k), below_x),
            (send_xl.at[q], got_xl.at[q], (i + 1, k), above_x),
        ]
        top = partial.at[q, 0:2, nz - 1]
        for low, high in spans[q]:
            keep = pl.ds(low, high - low)
            planes = [
                (sources[3], got_zf.at[q], (i, k - 1), below_z),
                (top, got_zl.at[q], (i, k + 1), above_z),
            ]
            if q == 2:
                planes = [(*row[:3], row[3] & odd) for row in planes]
                planes.append((sources[3], pair_zf, (i + 1, k - 1), below_z & ~odd))
                planes.append((top, pair_zl, (i + 1, k + 1), above_z & ~odd))
            for src, got, target, sends in planes:
                table.append((src.at[:, :, keep], got.at[:, :, keep], target, sends))
        return table

    def send(q, *chosen):
        table = messages(q)
        for m in chosen:
            src, dst, target, sends = table[m]
            sent, late = send_sem, max(m // 2 - 2, 0) if q == 0 else 0
            if m >= 4 and q % 2 == 0:
                sent = plane_sent.at[q + min(late, 1)]
            copy = pltpu.make_async_remote_copy(
                src_ref=src, dst_ref=dst, device_id=target, device_id_type=MESH,
                send_sem=sent, recv_sem=recv_sem.at[3 + late if late else q],
            )
            pl.when(sends)(copy.start)

    sides = []
    for below_x, above_x, below_z, above_z in itertools.product((False, True), repeat=4):
        if below_x + above_x > n_x - 1 or below_z + above_z > n_z - 1:
            continue
        if (n_x > 1 and not below_x + above_x) or (n_z > 1 and not below_z + above_z):
            continue
        here = ((i > 0) == below_x) & ((i < n_x - 1) == above_x)
        here = here & ((k > 0) == below_z) & ((k < n_z - 1) == above_z)
        length = (above_x & below_z) + (below_x & above_z) + 2 * nz * (below_x + above_x)
        sides.append((here, length, nx * below_z, nx * above_z))

    def wait_exchange(sem, lines, *widths, pair=False):
        for here, length, below, above in sides:
            plane = 3 * below + 4 * above if pair else 2 * (below + above)
            count = (lines * length * ny + plane * sum(widths)) // 128
            if count:
                span = tally.at[0:count]
                pl.when(here)(pltpu.make_async_copy(span, span, sem).wait)

    def finish(q, put, low=0, high=ny):
        scale = SCALES[q % 2]
        start = max(low - 128, 0)
        inside = pl.ds(start, high - start)
        not_first_x, not_last_x = i > 0, i < n_x - 1
        not_first_z, not_last_z = k > 0, k < n_z - 1

        def only(cond, v):
            return jnp.where(cond, v, 0.0)

        def f(c, z, part=slice(None)):
            return field[q, c, z, part, inside]

        bottom_x, bottom_y = got_zl[q, 0, :, inside], got_zl[q, 1, :, inside]
        top_x, top_y = got_zf[q, 0, :, inside], got_zf[q, 1, :, inside]
        if q == 2:
            bottom_x, bottom_y, top_x, top_y = (
                only(odd, v) for v in (bottom_x, bottom_y, top_x, top_y)
            )
        below_x = only(not_first_z, bottom_x - scale * f(1, 0))
        below_y = bottom_y + scale * f(0, 0)
        diagonal = only(not_last_x, scale * got_d6[q, :, inside])
        below_y = only(not_first_z, below_y - jnp.where(last_row(below_y), diagonal, 0.0))
        result = []
        for z in range(nz):
            mx, my, mz = (partial[q, c, z, :, inside] for c in range(3))
            edge_y = got_xl[q, z : z + 1, inside] - scale * f(2, z, slice(0, 1))
            edge_z = got_xl[q, nz + z : nz + z + 1, inside] + scale * f(1, z, slice(0, 1))
            if z == nz - 1:
                mx = mx - only(not_last_z, scale * top_y)
                my = my + only(not_last_z, scale * top_x)
                edge_y = edge_y + only(not_last_z, scale * got_d5[q, :, inside])
            edge_y, edge_z = only(not_first_x, edge_y), only(not_first_x, edge_z)
            next_y = only(not_last_x, scale * got_xf[q, 0, z : z + 1, inside])
            next_z = only(not_last_x, scale * got_xf[q, 1, z : z + 1, inside])
            my = my - jnp.where(last_row(my), next_z, 0.0)
            mz = mz + jnp.where(last_row(mz), next_y, 0.0)
            curl = (
                by(mz, start == 0) - (my - below_y),
                (mx - below_x) - bx(mz, edge_z),
                bx(my, edge_y) - by(mx, start == 0),
            )
            if put is not None:
                for c, v in enumerate((mx, my, mz)):
                    put[c, z, :, pl.ds(low, high - low)] = v[:, low - start :]
            result.append([v[:, low - start :] for v in curl])
            below_x, below_y = mx, my
        return result

    def open_exchange(*chosen):
        pl.semaphore_wait(barrier, greeted)
        send(0, *chosen)

    downs = [4 + 2 * n for n in range(len(widths))]
    ups = [n + 1 for n in downs]
    both = [n for pair in zip(ups, downs) for n in pair]
    pl.when(k == n_z - 1)(functools.partial(open_exchange, 0, 1, *downs, 2))
    for slot in (0, 1):
        loads[slot].wait()
    local_part(0, inner.at[0])
    pl.when(k < n_z - 1)(functools.partial(open_exchange, 0, 1, *both, 2))
    send(0, 3)
    hops = [1 << turn for turn in range((n_x - 1).bit_length())]
    told = [greet_line(line_sem.at[0], 1)]

    def tell():
        turn = len(told)
        if turn <= len(hops):
            pl.semaphore_wait(line_sem.at[turn - 1], told[-1])
            told.append(greet_line(line_sem.at[turn], hops[turn]) if turn < len(hops) else 0)

    perm_load.wait()
    for slot in (2, 3, 4):
        loads[slot].wait()
    for z in range(nz):
        kind = mat[z]
        eps = jnp.full((nx, ny), perm[0], jnp.float32)
        for number in range(1, kinds):
            eps = jnp.where(kind == number, perm[number], eps)
        coef[z] = COURANT / eps
        for c in range(3):
            field[1, c, z] = coef[z] * outer[c, z]
    local_part(1, inner.at[1])
    send(1, *LINES)
    loads[5].wait()

    @pl.when(~odd)
    def _():
        for c in range(3):
            pair_give[c] = coef[nz - 1] * field[1, c, nz - 1]
        for c in range(2):
            pair_give[3 + c] = coef[0] * field[1, c, 0]
        for src, dst, wanted in (
            (pair_give.at[0:3], pair_weight.at[0:3], k < n_z - 1),
            (own.at[nz - 1], pair_own.at[0], k < n_z - 1),
            (pair_give.at[3:5], pair_weight.at[3:5], k > 0),
            (own.at[0], pair_own.at[1], k > 0),
        ):
            copy = pltpu.make_async_remote_copy(
                src_ref=src, dst_ref=dst, device_id=(i + 1, k), device_id_type=MESH,
                send_sem=pair_sent, recv_sem=pair_got,
            )
            pl.when(wanted)(copy.start)

    wait_exchange(plane_sent.at[0], 0, widths[0])
    if len(widths) > 1:
        pl.when(odd)(functools.partial(wait_exchange, plane_sent.at[1], 0, *widths[1:]))
    send(1, *PLANES)
    tell()
    tell()

    for n, (low, high) in enumerate(spans[0]):
        wait_exchange(recv_sem.at[3 + n if n else 0], int(n == 0), high - low)
        change = finish(0, curl_in.at[0], low, high)
        keep = pl.ds(low, high - low)
        for z in range(nz):
            for c in range(3):
                moved = coef[z, :, keep] * change[z][c]
                curl_in[2, c, z, :, keep] = moved
                field[2, c, z, :, keep] = field[0, c, z, :, keep] + moved
        local_part(2, curl_in.at[0], *spans[2][n])
        if n == len(widths) - 1:
            send(2, 0, 1)
        send(2, *range(4 + 4 * n, 8 + 4 * n))
    send(2, 2, 3)
    tell()

    wait_exchange(recv_sem.at[1], 1, ny)
    change = finish(1, curl_in.at[1])
    for z in range(nz):
        dot = None
        for c in range(3):
            now = outer[c, z] - COURANT * change[z][c]
            inner[1, c, z] = now
            field[3, c, z] = coef[z] * now
            term = now * curl_in[2, c, z]
            dot = term if dot is None else dot + term
        weight[z] = coef[z] * dot
    local_part(3, curl_in.at[1])
    send(3, *LINES)
    pl.when(~odd)(functools.partial(send, 3, *PLANES))
    wait_exchange(plane_sent.at[2], 0, ny)
    pl.when(~odd & (i < n_x - 1))(functools.partial(signal, pair_sem, i + 1, k))

    @pl.when(odd)
    def _():
        pl.semaphore_wait(pair_sem, 1)
        send(3, *PLANES)

    @pl.when(odd)
    def _():
        wait_exchange(pair_got, 0, ny, pair=True)
        wait_exchange(recv_sem.at[2], 1, 2 * ny)

    pl.when(~odd)(functools.partial(wait_exchange, recv_sem.at[2], 1))
    change = finish(2, None)
    sums = [jnp.zeros((nx, 128), jnp.float32)] * NI
    planes = []
    for z in range(nz):
        dot = None
        for c in range(3):
            term = outer[c, z] * (coef[z] * change[z][c])
            dot = term if dot is None else dot + term
        planes.append((weight[z] + coef[z] * dot, own[z]))
    push_x, push_y = -SCALES[0] * pair_zf[1], SCALES[0] * pair_zf[0]
    turn = bx(push_y, 0.0) - by(push_x, True)
    above = pair_weight[1] * push_x - pair_weight[0] * push_y + pair_weight[2] * turn
    below = pair_weight[3] * pair_zl[1] - pair_weight[4] * pair_zl[0]
    planes.append((jnp.where(odd & (k < n_z - 1), above, 0.0), pair_own[0]))
    planes.append((jnp.where(odd & (k > 0), below, 0.0), pair_own[1]))
    for both, which in planes:
        for t in range(0, ny, 128):
            part, index = both[:, t : t + 128], which[:, t : t + 128]
            for j in range(NI):
                sums[j] = sums[j] + jnp.where(index == j, part, 0.0)
    lane = lax.broadcasted_iota(jnp.int32, (1, 128), 1)
    row = jnp.zeros((1, 128), jnp.float32)
    for j in range(NI):
        column = jnp.sum(sums[j], axis=0, keepdims=True)
        row = jnp.where(lane == j, jnp.sum(column, axis=1, keepdims=True), row)
    mine[0] = row
    gathered[me] = row

    while len(told) <= len(hops):
        tell()

    def share_sum(step, carry):
        other = jnp.where(step < me, step, step + 1)
        pltpu.make_async_remote_copy(
            src_ref=mine.at[0], dst_ref=gathered.at[me], send_sem=sum_send, recv_sem=sum_recv,
            device_id=(other // n_z, lax.rem(other, n_z)), device_id_type=MESH,
        ).start()
        return carry

    lax.fori_loop(0, total - 1, share_sum, 0)

    wait_exchange(recv_sem.at[3], 1, ny)
    change = finish(3, ko_ref)
    for z in range(nz):
        for c in range(3):
            go_ref[c, z] = inner[1, c, z] - COURANT * change[z][c]
    everyone = gathered.at[0 : total - 1]
    pltpu.make_async_copy(everyone, everyone, sum_recv).wait()
    pltpu.make_async_copy(everyone, everyone, sum_send).wait()
    grad_ref[...] = jnp.sum(gathered[...], axis=0)[:, :NI] / norm
    wait_exchange(send_sem, 4, 2 * ny)
    pl.when(~odd)(functools.partial(wait_exchange, pair_sent, 0, ny, pair=True))
    if len(widths) > 1:
        pl.when(~odd)(functools.partial(wait_exchange, plane_sent.at[1], 0, *widths[1:]))


def store(g_ref, h_ref, grad_ref, g_hbm, h_hbm, grad_hbm, sem):
    pltpu.make_async_copy(grad_ref, grad_hbm, sem.at[2]).start()
    for z in range(g_ref.shape[1]):
        pltpu.make_async_copy(g_ref.at[:, z], g_hbm.at[:, :, z, :], sem.at[0]).start()
        pltpu.make_async_copy(h_ref.at[:, z], h_hbm.at[:, :, z, :], sem.at[1]).start()
    for n, ref in enumerate((g_ref, h_ref, grad_ref)):
        pltpu.make_async_copy(ref, ref, sem.at[n]).wait()


def solution(mesh):
    n_x, n_z = mesh.shape["xy"], mesh.shape["gz"]

    def body(e_check, h_check, adj_e, adj_h, material, owner, permittivity):
        _, nx, nz, ny = e_check.shape
        cells = nx * n_x * nz * n_z * ny
        norm = np.sqrt(np.float32(cells / NI))
        dims = (n_x, n_z, nx, nz, ny, permittivity.shape[0], norm)
        f32 = jnp.float32
        hbm_spec = pl.BlockSpec(memory_space=pltpu.HBM)
        vmem_spec = pl.BlockSpec(memory_space=pltpu.VMEM)
        block = (3, nz, nx, ny)
        g, h, grad = pl.pallas_call(
            functools.partial(kernel, dims),
            out_shape=(
                pltpu.VMEM(block, f32), pltpu.VMEM(block, f32), pltpu.VMEM((1, NI), f32),
            ),
            in_specs=[hbm_spec] * 7,
            out_specs=(vmem_spec,) * 3,
            scratch_shapes=[
                pltpu.SMEM(permittivity.shape, f32),
                pltpu.VMEM((4,) + block, f32),
                pltpu.VMEM((2,) + block, f32),
                pltpu.VMEM((4,) + block, f32),
                pltpu.VMEM((3,) + block, f32),
                pltpu.VMEM(block, f32),
                pltpu.VMEM((nz, nx, ny), jnp.int32),
                pltpu.VMEM((nz, nx, ny), jnp.int32),
                pltpu.VMEM((nz, nx, ny), f32),
                pltpu.VMEM((nz, nx, ny), f32),
                pltpu.VMEM((4, 2, nz, ny), f32),
                pltpu.VMEM((4, 2 * nz, ny), f32),
                pltpu.VMEM((4, 1, ny), f32),
                pltpu.VMEM((4, 1, ny), f32),
                pltpu.VMEM((4, 2, nz, ny), f32),
                pltpu.VMEM((4, 2, nx, ny), f32),
                pltpu.VMEM((4, 2 * nz, ny), f32),
                pltpu.VMEM((4, 2, nx, ny), f32),
                pltpu.VMEM((4, 1, ny), f32),
                pltpu.VMEM((4, 1, ny), f32),
                pltpu.VMEM((1, 1, 128), f32),
                pltpu.VMEM((n_x * n_z, 1, 128), f32),
                pltpu.VMEM((8 * (1 + 2 * nz + 2 * nx) * ny // 128, 1, 128), f32),
                pltpu.VMEM((2, nx, ny), f32),
                pltpu.VMEM((2, nx, ny), f32),
                pltpu.VMEM((5, nx, ny), f32),
                pltpu.VMEM((5, nx, ny), f32),
                pltpu.VMEM((2, nx, ny), jnp.int32),
                pltpu.SemaphoreType.DMA((7,)),
                pltpu.SemaphoreType.DMA,
                pltpu.SemaphoreType.DMA((3,)),
                pltpu.SemaphoreType.DMA((5,)),
                pltpu.SemaphoreType.DMA,
                pltpu.SemaphoreType.DMA,
                pltpu.SemaphoreType.REGULAR((max(1, (n_x - 1).bit_length()),)),
                pltpu.SemaphoreType.REGULAR,
                pltpu.SemaphoreType.DMA,
                pltpu.SemaphoreType.DMA,
            ],
            compiler_params=pltpu.CompilerParams(
                collective_id=0, has_side_effects=True
            ),
            name="yee_adjoint",
        )(e_check, h_check, adj_e, adj_h, material, owner, permittivity)
        g, h, grad = pl.pallas_call(
            store,
            out_shape=(
                jax.ShapeDtypeStruct(e_check.shape, f32),
                jax.ShapeDtypeStruct(e_check.shape, f32),
                jax.ShapeDtypeStruct((1, NI), f32),
            ),
            in_specs=[vmem_spec] * 3,
            out_specs=(hbm_spec,) * 3,
            scratch_shapes=[pltpu.SemaphoreType.DMA((3,))],
            compiler_params=pltpu.CompilerParams(vmem_limit_bytes=2**20),
            name="store_outputs",
        )(g, h, grad)
        return g, h, grad.reshape(NI)

    split = P(None, "xy", "gz", None)
    return jax.shard_map(
        body,
        mesh=mesh,
        in_specs=(split,) * 4 + (P("xy", "gz", None),) * 2 + (P(),),
        out_specs=(split, split, P()),
        check_vma=False,
    )
```

```python
import functools
import itertools

import jax
import jax.numpy as jnp
import numpy as np
from jax import lax
from jax.experimental import pallas as pl
from jax.experimental.pallas import tpu as pltpu
from jax.sharding import PartitionSpec as P

NI = 8
COURANT = 0.5
MESH = pl.DeviceIdType.MESH
LINES, PLANES = (0, 1, 2, 3), (4, 5)
SCALES = (-COURANT, 1.0)


def kernel(
    dims, e_hbm, h_hbm, g_hbm, k_hbm, mat_hbm, own_hbm, perm_hbm,
    go_ref, ko_ref, grad_ref,
    perm, field, inner, partial, curl_in, outer, mat, own, coef, weight,
    send_xf, send_xl, send_d5, send_d6,
    got_xf, got_zf, got_xl, got_zl, got_d5, got_d6,
    mine, gathered, tally,
    pair_zf, pair_zl, pair_give, pair_weight, pair_own, portion,
    load_sem, send_sem, plane_sent, recv_sem, sum_recv,
    line_sem, pair_sem,
):
    n_x, n_z, nx, nz, ny, kinds, norm = dims
    total = n_x * n_z
    i = lax.axis_index("xy")
    k = lax.axis_index("gz")
    me = i * n_z + k
    odd = lax.rem(i, 2) == 1

    def load(src, dst, slot):
        for z in range(nz):
            src_z = src.at[:, :, z, :] if len(src.shape) == 4 else src.at[:, z, :]
            dst_z = dst.at[:, z] if len(dst.shape) == 4 else dst.at[z]
            pltpu.make_async_copy(src_z, dst_z, load_sem.at[slot]).start()

    def wait_blocks(sem, count):
        span = tally.at[0:count]
        pltpu.make_async_copy(span, span, sem).wait()

    cell_blocks = nx * nz * ny // 128

    barrier = pltpu.get_barrier_semaphore()

    def signal(sem, x, z):
        pl.semaphore_signal(sem, inc=1, device_id=(x, z), device_id_type=MESH)

    def greet(sem, partners):
        count = 0
        for cond, x, z in partners:
            pl.when(cond)(functools.partial(signal, sem, x, z))
            count = count + cond.astype(jnp.int32)
        return count

    def greet_line(sem, hop):
        return greet(sem, ((i >= hop, i - hop, k), (i < n_x - hop, i + hop, k)))

    load(e_hbm, field.at[0], 0)
    load(h_hbm, inner.at[0], 0)
    greeted = greet_line(barrier, 1) + greet(
        barrier,
        (
            ((i > 0) & (k < n_z - 1), i - 1, k + 1),
            ((i < n_x - 1) & (k > 0), i + 1, k - 1),
        ),
    )
    for step in range(1, n_z):
        signal(barrier, i, lax.rem(k + step, n_z))
    greeted = greeted + n_z - 1

    perm_load = pltpu.make_async_copy(perm_hbm, perm, load_sem.at[2])
    perm_load.start()
    load(mat_hbm, mat, 1)
    load(g_hbm, outer, 1)
    load(k_hbm, inner.at[1], 1)
    load(own_hbm, own, 1)

    rows = lax.broadcasted_iota(jnp.int32, (nx, ny), 0)
    lanes = lax.broadcasted_iota(jnp.int32, (nx, ny), 1)

    def first_row(v):
        return rows[:, : v.shape[1]] == 0

    def last_row(v):
        return rows[:, : v.shape[1]] == nx - 1

    def dy(v, whole):
        width = v.shape[1]
        later = pltpu.roll(v, width - 1, 1)
        return jnp.where(lanes[:, :width] == width - 1, 0.0, later) - v if whole else later - v

    def dx(v):
        return jnp.where(last_row(v), 0.0, pltpu.roll(v, nx - 1, 0)) - v

    def by(v, whole):
        earlier = pltpu.roll(v, 1, 1)
        return v - (jnp.where(lanes[:, : v.shape[1]] == 0, 0.0, earlier) if whole else earlier)

    def bx(v, row):
        return v - jnp.where(first_row(v), row, pltpu.roll(v, 1, 0))

    def local_part(q, mag, low=0, high=ny):
        scale = SCALES[q % 2]
        end = min(high + 128, ny)
        inside, keep = pl.ds(low, end - low), pl.ds(low, high - low)
        width = high - low

        def put(ref, index, v):
            ref[index + (keep,)] = v[:, :width]

        for z in range(nz):
            fx, fy, fz = (field[q, c, z, :, inside] for c in range(3))
            if z < nz - 1:
                up_x, up_y = (field[q, c, z + 1, :, inside] for c in range(2))
                up_x, up_y = up_x - fx, up_y - fy
            else:
                up_x, up_y = -fx, -fy
            whole = end == high
            lx = mag[0, z, :, inside] + scale * (dy(fz, whole) - up_y)
            ly = mag[1, z, :, inside] + scale * (up_x - dx(fz))
            lz = mag[2, z, :, inside] + scale * (dx(fy) - dy(fx, whole))
            for c, v in enumerate((lx, ly, lz)):
                put(partial, (q, c, z, slice(None)), v)
            if q:
                put(send_xf, (q, 0, slice(z, z + 1)), fy[0:1])
                put(send_xf, (q, 1, slice(z, z + 1)), fz[0:1])
            put(send_xl, (q, slice(z, z + 1)), ly[nx - 1 : nx])
            put(send_xl, (q, slice(nz + z, nz + z + 1)), lz[nx - 1 : nx])
            if q and z == 0:
                put(send_d5, (q, slice(None)), fx[nx - 1 : nx])
            if q and z == nz - 1:
                put(send_d6, (q, slice(None)), fz[0:1])

    spans = [((0, ny),)] * 4
    if ny % 1024 == 0:
        cuts = [ny // 8 * n for n in (4,)]
        spans[0] = tuple(zip([0] + cuts, cuts + [ny]))
        ahead = [n - 128 for n in cuts]
        spans[2] = tuple(zip([0] + ahead, ahead + [ny]))
    widths = [high - low for low, high in spans[0]]

    def messages(q):
        below_x, above_x = i > 0, i < n_x - 1
        below_z, above_z = k > 0, k < n_z - 1
        sources = (
            (
                e_hbm.at[0, nx - 1 : nx, 0], e_hbm.at[2, 0:1, nz - 1],
                e_hbm.at[1:3, 0], e_hbm.at[0:2, :, 0],
            )
            if q == 0
            else (send_d5.at[q], send_d6.at[q], send_xf.at[q], field.at[q, 0:2, 0])
        )
        table = [
            (sources[0], got_d5.at[q], (i + 1, k - 1), above_x & below_z),
            (sources[1], got_d6.at[q], (i - 1, k + 1), below_x & above_z),
            (sources[2], got_xf.at[q], (i - 1, k), below_x),
            (send_xl.at[q], got_xl.at[q], (i + 1, k), above_x),
        ]
        top = partial.at[q, 0:2, nz - 1]
        for low, high in spans[q]:
            keep = pl.ds(low, high - low)
            planes = [
                (sources[3], got_zf.at[q], (i, k - 1), below_z),
                (top, got_zl.at[q], (i, k + 1), above_z),
            ]
            if q == 2:
                planes = [(*row[:3], row[3] & odd) for row in planes]
                planes.append((sources[3], pair_zf, (i + 1, k - 1), below_z & ~odd))
                planes.append((top, pair_zl, (i + 1, k + 1), above_z & ~odd))
            for src, got, target, sends in planes:
                table.append((src.at[:, :, keep], got.at[:, :, keep], target, sends))
        return table

    def send(q, *chosen):
        table = messages(q)
        for m in chosen:
            src, dst, target, sends = table[m]
            sent, late = send_sem, max(m // 2 - 2, 0) if q == 0 else 0
            if m >= 4 and q % 2 == 0:
                sent = plane_sent.at[q + min(late, 1)]
            copy = pltpu.make_async_remote_copy(
                src_ref=src, dst_ref=dst, device_id=target, device_id_type=MESH,
                send_sem=sent, recv_sem=recv_sem.at[3 + late if late else q],
            )
            pl.when(sends)(copy.start)

    sides = []
    for below_x, above_x, below_z, above_z in itertools.product((False, True), repeat=4):
        if below_x + above_x > n_x - 1 or below_z + above_z > n_z - 1:
            continue
        if (n_x > 1 and not below_x + above_x) or (n_z > 1 and not below_z + above_z):
            continue
        here = ((i > 0) == below_x) & ((i < n_x - 1) == above_x)
        here = here & ((k > 0) == below_z) & ((k < n_z - 1) == above_z)
        length = (above_x & below_z) + (below_x & above_z) + 2 * nz * (below_x + above_x)
        sides.append((here, length, nx * below_z, nx * above_z))

    def wait_exchange(sem, lines, *widths, pairs=0, extra=0):
        for here, length, below, above in sides:
            count = lines * length * ny + 2 * (below + above) * sum(widths)
            count = (count + pairs * (3 * below + 4 * above) * ny) // 128 + extra
            if count:
                span = tally.at[0:count]
                pl.when(here)(pltpu.make_async_copy(span, span, sem).wait)

    def finish(q, put, low=0, high=ny):
        scale = SCALES[q % 2]
        start = max(low - 128, 0)
        inside = pl.ds(start, high - start)
        not_first_x, not_last_x = i > 0, i < n_x - 1
        not_first_z, not_last_z = k > 0, k < n_z - 1

        def only(cond, v):
            return jnp.where(cond, v, 0.0)

        def f(c, z, part=slice(None)):
            return field[q, c, z, part, inside]

        bottom_x, bottom_y = got_zl[q, 0, :, inside], got_zl[q, 1, :, inside]
        top_x, top_y = got_zf[q, 0, :, inside], got_zf[q, 1, :, inside]
        if q == 2:
            bottom_x, bottom_y, top_x, top_y = (
                only(odd, v) for v in (bottom_x, bottom_y, top_x, top_y)
            )
        below_x = only(not_first_z, bottom_x - scale * f(1, 0))
        below_y = bottom_y + scale * f(0, 0)
        diagonal = only(not_last_x, scale * got_d6[q, :, inside])
        below_y = only(not_first_z, below_y - jnp.where(last_row(below_y), diagonal, 0.0))
        result = []
        for z in range(nz):
            mx, my, mz = (partial[q, c, z, :, inside] for c in range(3))
            edge_y = got_xl[q, z : z + 1, inside] - scale * f(2, z, slice(0, 1))
            edge_z = got_xl[q, nz + z : nz + z + 1, inside] + scale * f(1, z, slice(0, 1))
            if z == nz - 1:
                mx = mx - only(not_last_z, scale * top_y)
                my = my + only(not_last_z, scale * top_x)
                edge_y = edge_y + only(not_last_z, scale * got_d5[q, :, inside])
            edge_y, edge_z = only(not_first_x, edge_y), only(not_first_x, edge_z)
            next_y = only(not_last_x, scale * got_xf[q, 0, z : z + 1, inside])
            next_z = only(not_last_x, scale * got_xf[q, 1, z : z + 1, inside])
            my = my - jnp.where(last_row(my), next_z, 0.0)
            mz = mz + jnp.where(last_row(mz), next_y, 0.0)
            curl = (
                by(mz, start == 0) - (my - below_y),
                (mx - below_x) - bx(mz, edge_z),
                bx(my, edge_y) - by(mx, start == 0),
            )
            if put is not None:
                for c, v in enumerate((mx, my, mz)):
                    put[c, z, :, pl.ds(low, high - low)] = v[:, low - start :]
            result.append([v[:, low - start :] for v in curl])
            below_x, below_y = mx, my
        return result

    def open_exchange(*chosen):
        pl.semaphore_wait(barrier, greeted)
        send(0, *chosen)

    downs = [4 + 2 * n for n in range(len(widths))]
    ups = [n + 1 for n in downs]
    both = [n for pair in zip(ups, downs) for n in pair]
    pl.when(k == n_z - 1)(functools.partial(open_exchange, 0, 1, *downs, 2))
    wait_blocks(load_sem.at[0], 6 * cell_blocks)
    local_part(0, inner.at[0])
    pl.when(k < n_z - 1)(functools.partial(open_exchange, 0, 1, *both, 2))
    send(0, 3)
    hops = [1 << turn for turn in range((n_x - 1).bit_length())]
    told = [greet_line(line_sem.at[0], 1)]

    def tell():
        turn = len(told)
        if turn <= len(hops):
            pl.semaphore_wait(line_sem.at[turn - 1], told[-1])
            told.append(greet_line(line_sem.at[turn], hops[turn]) if turn < len(hops) else 0)

    perm_load.wait()
    wait_blocks(load_sem.at[1], 8 * cell_blocks)
    for z in range(nz):
        kind = mat[z]
        eps = jnp.full((nx, ny), perm[0], jnp.float32)
        for number in range(1, kinds):
            eps = jnp.where(kind == number, perm[number], eps)
        coef[z] = COURANT / eps
        for c in range(3):
            field[1, c, z] = coef[z] * outer[c, z]
    local_part(1, inner.at[1])
    send(1, *LINES)
    @pl.when(~odd)
    def _():
        for c in range(3):
            pair_give[c] = coef[nz - 1] * field[1, c, nz - 1]
        for c in range(2):
            pair_give[3 + c] = coef[0] * field[1, c, 0]
        for src, dst, wanted in (
            (pair_give.at[0:3], pair_weight.at[0:3], k < n_z - 1),
            (own.at[nz - 1], pair_own.at[0], k < n_z - 1),
            (pair_give.at[3:5], pair_weight.at[3:5], k > 0),
            (own.at[0], pair_own.at[1], k > 0),
        ):
            copy = pltpu.make_async_remote_copy(
                src_ref=src, dst_ref=dst, device_id=(i + 1, k), device_id_type=MESH,
                send_sem=send_sem, recv_sem=recv_sem.at[2],
            )
            pl.when(wanted)(copy.start)

    wait_exchange(plane_sent.at[0], 0, widths[0])
    if len(widths) > 1:
        pl.when(odd)(functools.partial(wait_exchange, plane_sent.at[1], 0, *widths[1:]))
    send(1, *PLANES)
    tell()
    tell()

    for n, (low, high) in enumerate(spans[0]):
        wait_exchange(recv_sem.at[3 + n if n else 0], int(n == 0), high - low)
        change = finish(0, curl_in.at[0], low, high)
        keep = pl.ds(low, high - low)
        for z in range(nz):
            for c in range(3):
                moved = coef[z, :, keep] * change[z][c]
                curl_in[2, c, z, :, keep] = moved
                field[2, c, z, :, keep] = field[0, c, z, :, keep] + moved
        local_part(2, curl_in.at[0], *spans[2][n])
        if n == len(widths) - 1:
            send(2, 0, 1)
        send(2, *range(4 + 4 * n, 8 + 4 * n))
    send(2, 2, 3)
    tell()

    wait_exchange(recv_sem.at[1], 1, ny)
    change = finish(1, curl_in.at[1])
    for z in range(nz):
        dot = None
        for c in range(3):
            now = outer[c, z] - COURANT * change[z][c]
            inner[1, c, z] = now
            field[3, c, z] = coef[z] * now
            term = now * curl_in[2, c, z]
            dot = term if dot is None else dot + term
        weight[z] = coef[z] * dot
    local_part(3, curl_in.at[1])
    send(3, *LINES)
    pl.when(~odd)(functools.partial(send, 3, *PLANES))
    pl.when(odd)(functools.partial(wait_exchange, recv_sem.at[2], 1, 2 * ny, pairs=1))
    pl.when(~odd)(functools.partial(wait_exchange, recv_sem.at[2], 1))
    change = finish(2, None)
    sums = [jnp.zeros((nx, 128), jnp.float32)] * NI
    planes = []
    for z in range(nz):
        dot = None
        for c in range(3):
            term = outer[c, z] * (coef[z] * change[z][c])
            dot = term if dot is None else dot + term
        planes.append((weight[z] + coef[z] * dot, own[z]))
    for both, which in planes:
        for t in range(0, ny, 128):
            part, index = both[:, t : t + 128], which[:, t : t + 128]
            for j in range(NI):
                sums[j] = sums[j] + jnp.where(index == j, part, 0.0)
    for j in range(NI):
        portion[j] = sums[j]

    def include(both, which):
        for j in range(NI):
            one = portion[j]
            for t in range(0, ny, 128):
                one = one + jnp.where(which[:, t : t + 128] == j, both[:, t : t + 128], 0.0)
            portion[j] = one

    @pl.when(odd & (k < n_z - 1))
    def _():
        push_x, push_y = -SCALES[0] * pair_zf[1], SCALES[0] * pair_zf[0]
        turn = bx(push_y, 0.0) - by(push_x, True)
        above = pair_weight[1] * push_x - pair_weight[0] * push_y + pair_weight[2] * turn
        include(above, pair_own[0])

    @pl.when(odd & (k > 0))
    def _():
        below = pair_weight[3] * pair_zl[1] - pair_weight[4] * pair_zl[0]
        include(below, pair_own[1])

    lane = lax.broadcasted_iota(jnp.int32, (NI, 128), 1)
    number = lax.broadcasted_iota(jnp.int32, (NI, 128), 0)
    table = jnp.zeros((NI, 128), jnp.float32)
    for j in range(NI):
        table = jnp.where(number == j, jnp.sum(portion[j], axis=0, keepdims=True), table)
    table = jnp.where(lane == number, jnp.sum(table, axis=1, keepdims=True), 0.0)
    row = jnp.sum(table, axis=0, keepdims=True)
    mine[0] = row
    gathered[me] = row

    while len(told) <= len(hops):
        tell()

    def share_sum(step, carry):
        other = jnp.where(step < me, step, step + 1)
        pltpu.make_async_remote_copy(
            src_ref=mine.at[0], dst_ref=gathered.at[me], send_sem=send_sem, recv_sem=sum_recv,
            device_id=(other // n_z, lax.rem(other, n_z)), device_id_type=MESH,
        ).start()
        return carry

    lax.fori_loop(0, total - 1, share_sum, 0)

    wait_exchange(plane_sent.at[2], 0, ny)
    pl.when(~odd & (i < n_x - 1))(functools.partial(signal, pair_sem, i + 1, k))

    @pl.when(odd)
    def _():
        pl.semaphore_wait(pair_sem, 1)
        send(3, *PLANES)

    wait_exchange(recv_sem.at[3], 1, ny)
    change = finish(3, ko_ref)
    for z in range(nz):
        for c in range(3):
            go_ref[c, z] = inner[1, c, z] - COURANT * change[z][c]
    for parity, pairs in ((odd, 0), (~odd, 1)):
        pl.when(parity)(
            functools.partial(
                wait_exchange, send_sem, 4, 2 * ny, pairs=pairs, extra=total - 1
            )
        )
    if len(widths) > 1:
        pl.when(~odd)(functools.partial(wait_exchange, plane_sent.at[1], 0, *widths[1:]))
    everyone = gathered.at[0 : total - 1]
    pltpu.make_async_copy(everyone, everyone, sum_recv).wait()
    grad_ref[...] = jnp.sum(gathered[...], axis=0)[:, :NI] / norm


def store(g_ref, h_ref, grad_ref, g_hbm, h_hbm, grad_hbm, sem):
    pltpu.make_async_copy(grad_ref, grad_hbm, sem.at[2]).start()
    for z in range(g_ref.shape[1]):
        pltpu.make_async_copy(g_ref.at[:, z], g_hbm.at[:, :, z, :], sem.at[0]).start()
        pltpu.make_async_copy(h_ref.at[:, z], h_hbm.at[:, :, z, :], sem.at[1]).start()
    for n, ref in enumerate((g_ref, h_ref, grad_ref)):
        pltpu.make_async_copy(ref, ref, sem.at[n]).wait()


def solution(mesh):
    n_x, n_z = mesh.shape["xy"], mesh.shape["gz"]

    def body(e_check, h_check, adj_e, adj_h, material, owner, permittivity):
        _, nx, nz, ny = e_check.shape
        cells = nx * n_x * nz * n_z * ny
        norm = np.sqrt(np.float32(cells / NI))
        dims = (n_x, n_z, nx, nz, ny, permittivity.shape[0], norm)
        f32 = jnp.float32
        hbm_spec = pl.BlockSpec(memory_space=pltpu.HBM)
        vmem_spec = pl.BlockSpec(memory_space=pltpu.VMEM)
        block = (3, nz, nx, ny)
        g, h, grad = pl.pallas_call(
            functools.partial(kernel, dims),
            out_shape=(
                pltpu.VMEM(block, f32), pltpu.VMEM(block, f32), pltpu.VMEM((1, NI), f32),
            ),
            in_specs=[hbm_spec] * 7,
            out_specs=(vmem_spec,) * 3,
            scratch_shapes=[
                pltpu.SMEM(permittivity.shape, f32),
                pltpu.VMEM((4,) + block, f32),
                pltpu.VMEM((2,) + block, f32),
                pltpu.VMEM((4,) + block, f32),
                pltpu.VMEM((3,) + block, f32),
                pltpu.VMEM(block, f32),
                pltpu.VMEM((nz, nx, ny), jnp.int32),
                pltpu.VMEM((nz, nx, ny), jnp.int32),
                pltpu.VMEM((nz, nx, ny), f32),
                pltpu.VMEM((nz, nx, ny), f32),
                pltpu.VMEM((4, 2, nz, ny), f32),
                pltpu.VMEM((4, 2 * nz, ny), f32),
                pltpu.VMEM((4, 1, ny), f32),
                pltpu.VMEM((4, 1, ny), f32),
                pltpu.VMEM((4, 2, nz, ny), f32),
                pltpu.VMEM((4, 2, nx, ny), f32),
                pltpu.VMEM((4, 2 * nz, ny), f32),
                pltpu.VMEM((4, 2, nx, ny), f32),
                pltpu.VMEM((4, 1, ny), f32),
                pltpu.VMEM((4, 1, ny), f32),
                pltpu.VMEM((1, 1, 128), f32),
                pltpu.VMEM((n_x * n_z, 1, 128), f32),
                pltpu.VMEM((16 * (1 + 2 * nz + 2 * nx) * ny // 128 + n_x * n_z, 1, 128), f32),
                pltpu.VMEM((2, nx, ny), f32),
                pltpu.VMEM((2, nx, ny), f32),
                pltpu.VMEM((5, nx, ny), f32),
                pltpu.VMEM((5, nx, ny), f32),
                pltpu.VMEM((2, nx, ny), jnp.int32),
                pltpu.VMEM((NI, nx, 128), f32),
                pltpu.SemaphoreType.DMA((3,)),
                pltpu.SemaphoreType.DMA,
                pltpu.SemaphoreType.DMA((3,)),
                pltpu.SemaphoreType.DMA((5,)),
                pltpu.SemaphoreType.DMA,
                pltpu.SemaphoreType.REGULAR((max(1, (n_x - 1).bit_length()),)),
                pltpu.SemaphoreType.REGULAR,
            ],
            compiler_params=pltpu.CompilerParams(
                collective_id=0, has_side_effects=True
            ),
            name="yee_adjoint",
        )(e_check, h_check, adj_e, adj_h, material, owner, permittivity)
        g, h, grad = pl.pallas_call(
            store,
            out_shape=(
                jax.ShapeDtypeStruct(e_check.shape, f32),
                jax.ShapeDtypeStruct(e_check.shape, f32),
                jax.ShapeDtypeStruct((1, NI), f32),
            ),
            in_specs=[vmem_spec] * 3,
            out_specs=(hbm_spec,) * 3,
            scratch_shapes=[pltpu.SemaphoreType.DMA((3,))],
            compiler_params=pltpu.CompilerParams(vmem_limit_bytes=2**20),
            name="store_outputs",
        )(g, h, grad)
        return g, h, grad.reshape(NI)

    split = P(None, "xy", "gz", None)
    return jax.shard_map(
        body,
        mesh=mesh,
        in_specs=(split,) * 4 + (P("xy", "gz", None),) * 2 + (P(),),
        out_specs=(split, split, P()),
        check_vma=False,
    )
```

```python
import functools
import itertools

import jax
import jax.numpy as jnp
import numpy as np
from jax import lax
from jax.experimental import pallas as pl
from jax.experimental.pallas import tpu as pltpu
from jax.sharding import PartitionSpec as P

NI = 8
COURANT = 0.5
MESH = pl.DeviceIdType.MESH
LINES, PLANES = (0, 1, 2, 3), (4, 5)
SCALES = (-COURANT, 1.0)


def kernel(
    dims, e_hbm, h_hbm, g_hbm, k_hbm, mat_hbm, own_hbm, perm_hbm,
    go_ref, ko_ref, grad_ref,
    perm, field, inner, partial, curl_in, outer, mat, own, coef, weight,
    send_xf, send_xl, send_d5, send_d6,
    got_xf, got_zf, got_xl, got_zl, got_d5, got_d6,
    mine, gathered, tally,
    pair_zf, pair_zl, pair_give, pair_weight, pair_own, portion,
    load_sem, send_sem, plane_sent, recv_sem, sum_recv,
    line_sem, pair_sem,
):
    n_x, n_z, nx, nz, ny, kinds, norm = dims
    total = n_x * n_z
    i = lax.axis_index("xy")
    k = lax.axis_index("gz")
    me = i * n_z + k
    odd = lax.rem(i, 2) == 1

    def load(src, dst, slot):
        for z in range(nz):
            src_z = src.at[:, :, z, :] if len(src.shape) == 4 else src.at[:, z, :]
            dst_z = dst.at[:, z] if len(dst.shape) == 4 else dst.at[z]
            pltpu.make_async_copy(src_z, dst_z, load_sem.at[slot]).start()

    def wait_blocks(sem, count):
        span = tally.at[0:count]
        pltpu.make_async_copy(span, span, sem).wait()

    cell_blocks = nx * nz * ny // 128

    barrier = pltpu.get_barrier_semaphore()

    def signal(sem, x, z):
        pl.semaphore_signal(sem, inc=1, device_id=(x, z), device_id_type=MESH)

    def greet(sem, partners):
        count = 0
        for cond, x, z in partners:
            pl.when(cond)(functools.partial(signal, sem, x, z))
            count = count + cond.astype(jnp.int32)
        return count

    def greet_line(sem, hop):
        return greet(sem, ((i >= hop, i - hop, k), (i < n_x - hop, i + hop, k)))

    pltpu.make_async_copy(e_hbm.at[0:2, :, 0], field.at[0, 0:2, 0], load_sem.at[3]).start()
    pltpu.make_async_copy(e_hbm.at[2, :, 0], field.at[0, 2, 0], load_sem.at[0]).start()
    for z in range(1, nz):
        pltpu.make_async_copy(e_hbm.at[:, :, z], field.at[0, :, z], load_sem.at[0]).start()
    load(h_hbm, inner.at[0], 0)
    greeted = greet_line(barrier, 1) + greet(
        barrier,
        (
            ((i > 0) & (k < n_z - 1), i - 1, k + 1),
            ((i < n_x - 1) & (k > 0), i + 1, k - 1),
        ),
    )
    for step in range(1, n_z):
        signal(barrier, i, lax.rem(k + step, n_z))
    greeted = greeted + n_z - 1

    perm_load = pltpu.make_async_copy(perm_hbm, perm, load_sem.at[2])
    perm_load.start()
    load(mat_hbm, mat, 1)
    load(g_hbm, outer, 1)
    load(k_hbm, inner.at[1], 1)
    load(own_hbm, own, 1)

    rows = lax.broadcasted_iota(jnp.int32, (nx, ny), 0)
    lanes = lax.broadcasted_iota(jnp.int32, (nx, ny), 1)

    def first_row(v):
        return rows[:, : v.shape[1]] == 0

    def last_row(v):
        return rows[:, : v.shape[1]] == nx - 1

    def dy(v, whole):
        width = v.shape[1]
        later = pltpu.roll(v, width - 1, 1)
        return jnp.where(lanes[:, :width] == width - 1, 0.0, later) - v if whole else later - v

    def dx(v):
        return jnp.where(last_row(v), 0.0, pltpu.roll(v, nx - 1, 0)) - v

    def by(v, whole):
        earlier = pltpu.roll(v, 1, 1)
        return v - (jnp.where(lanes[:, : v.shape[1]] == 0, 0.0, earlier) if whole else earlier)

    def bx(v, row):
        return v - jnp.where(first_row(v), row, pltpu.roll(v, 1, 0))

    def local_part(q, mag, low=0, high=ny):
        scale = SCALES[q % 2]
        end = min(high + 128, ny)
        inside, keep = pl.ds(low, end - low), pl.ds(low, high - low)
        width = high - low

        def put(ref, index, v):
            ref[index + (keep,)] = v[:, :width]

        for z in range(nz):
            fx, fy, fz = (field[q, c, z, :, inside] for c in range(3))
            if z < nz - 1:
                up_x, up_y = (field[q, c, z + 1, :, inside] for c in range(2))
                up_x, up_y = up_x - fx, up_y - fy
            else:
                up_x, up_y = -fx, -fy
            whole = end == high
            lx = mag[0, z, :, inside] + scale * (dy(fz, whole) - up_y)
            ly = mag[1, z, :, inside] + scale * (up_x - dx(fz))
            lz = mag[2, z, :, inside] + scale * (dx(fy) - dy(fx, whole))
            for c, v in enumerate((lx, ly, lz)):
                put(partial, (q, c, z, slice(None)), v)
            if q:
                put(send_xf, (q, 0, slice(z, z + 1)), fy[0:1])
                put(send_xf, (q, 1, slice(z, z + 1)), fz[0:1])
            put(send_xl, (q, slice(z, z + 1)), ly[nx - 1 : nx])
            put(send_xl, (q, slice(nz + z, nz + z + 1)), lz[nx - 1 : nx])
            if q and z == 0:
                put(send_d5, (q, slice(None)), fx[nx - 1 : nx])
            if q and z == nz - 1:
                put(send_d6, (q, slice(None)), fz[0:1])

    spans = [((0, ny),)] * 4
    if ny % 1024 == 0:
        cuts = [ny // 8 * n for n in (4,)]
        spans[0] = tuple(zip([0] + cuts, cuts + [ny]))
        ahead = [n - 128 for n in cuts]
        spans[2] = tuple(zip([0] + ahead, ahead + [ny]))
    widths = [high - low for low, high in spans[0]]

    def messages(q):
        below_x, above_x = i > 0, i < n_x - 1
        below_z, above_z = k > 0, k < n_z - 1
        sources = (
            (
                e_hbm.at[0, nx - 1 : nx, 0], e_hbm.at[2, 0:1, nz - 1],
                e_hbm.at[1:3, 0], field.at[0, 0:2, 0],
            )
            if q == 0
            else (send_d5.at[q], send_d6.at[q], send_xf.at[q], field.at[q, 0:2, 0])
        )
        table = [
            (sources[0], got_d5.at[q], (i + 1, k - 1), above_x & below_z),
            (sources[1], got_d6.at[q], (i - 1, k + 1), below_x & above_z),
            (sources[2], got_xf.at[q], (i - 1, k), below_x),
            (send_xl.at[q], got_xl.at[q], (i + 1, k), above_x),
        ]
        top = partial.at[q, 0:2, nz - 1]
        for low, high in spans[q]:
            keep = pl.ds(low, high - low)
            planes = [
                (sources[3], got_zf.at[q], (i, k - 1), below_z),
                (top, got_zl.at[q], (i, k + 1), above_z),
            ]
            if q == 2:
                planes = [(*row[:3], row[3] & odd) for row in planes]
                planes.append((sources[3], pair_zf, (i + 1, k - 1), below_z & ~odd))
                planes.append((top, pair_zl, (i + 1, k + 1), above_z & ~odd))
            for src, got, target, sends in planes:
                table.append((src.at[:, :, keep], got.at[:, :, keep], target, sends))
        return table

    def send(q, *chosen):
        table = messages(q)
        for m in chosen:
            src, dst, target, sends = table[m]
            sent, late = send_sem, max(m // 2 - 2, 0) if q == 0 else 0
            if m >= 4 and q % 2 == 0:
                sent = plane_sent.at[q + min(late, 1)]
            landing = 3 + late if late else q
            if q == 2 and m >= 4 and m % 4 > 1:
                landing = 5
            copy = pltpu.make_async_remote_copy(
                src_ref=src, dst_ref=dst, device_id=target, device_id_type=MESH,
                send_sem=sent, recv_sem=recv_sem.at[landing],
            )
            pl.when(sends)(copy.start)

    sides = []
    for below_x, above_x, below_z, above_z in itertools.product((False, True), repeat=4):
        if below_x + above_x > n_x - 1 or below_z + above_z > n_z - 1:
            continue
        if (n_x > 1 and not below_x + above_x) or (n_z > 1 and not below_z + above_z):
            continue
        here = ((i > 0) == below_x) & ((i < n_x - 1) == above_x)
        here = here & ((k > 0) == below_z) & ((k < n_z - 1) == above_z)
        length = (above_x & below_z) + (below_x & above_z) + 2 * nz * (below_x + above_x)
        sides.append((here, length, nx * below_z, nx * above_z))

    def wait_exchange(sem, lines, *widths, pairs=0, extra=0):
        for here, length, below, above in sides:
            count = lines * length * ny + 2 * (below + above) * sum(widths)
            count = (count + pairs * (3 * below + 4 * above) * ny) // 128 + extra
            if count:
                span = tally.at[0:count]
                pl.when(here)(pltpu.make_async_copy(span, span, sem).wait)

    def finish(q, put, low=0, high=ny):
        scale = SCALES[q % 2]
        start = max(low - 128, 0)
        inside = pl.ds(start, high - start)
        not_first_x, not_last_x = i > 0, i < n_x - 1
        not_first_z, not_last_z = k > 0, k < n_z - 1

        def only(cond, v):
            return jnp.where(cond, v, 0.0)

        def f(c, z, part=slice(None)):
            return field[q, c, z, part, inside]

        bottom_x, bottom_y = got_zl[q, 0, :, inside], got_zl[q, 1, :, inside]
        top_x, top_y = got_zf[q, 0, :, inside], got_zf[q, 1, :, inside]
        if q == 2:
            bottom_x, bottom_y, top_x, top_y = (
                only(odd, v) for v in (bottom_x, bottom_y, top_x, top_y)
            )
        below_x = only(not_first_z, bottom_x - scale * f(1, 0))
        below_y = bottom_y + scale * f(0, 0)
        diagonal = only(not_last_x, scale * got_d6[q, :, inside])
        below_y = only(not_first_z, below_y - jnp.where(last_row(below_y), diagonal, 0.0))
        result = []
        for z in range(nz):
            mx, my, mz = (partial[q, c, z, :, inside] for c in range(3))
            edge_y = got_xl[q, z : z + 1, inside] - scale * f(2, z, slice(0, 1))
            edge_z = got_xl[q, nz + z : nz + z + 1, inside] + scale * f(1, z, slice(0, 1))
            if z == nz - 1:
                mx = mx - only(not_last_z, scale * top_y)
                my = my + only(not_last_z, scale * top_x)
                edge_y = edge_y + only(not_last_z, scale * got_d5[q, :, inside])
            edge_y, edge_z = only(not_first_x, edge_y), only(not_first_x, edge_z)
            next_y = only(not_last_x, scale * got_xf[q, 0, z : z + 1, inside])
            next_z = only(not_last_x, scale * got_xf[q, 1, z : z + 1, inside])
            my = my - jnp.where(last_row(my), next_z, 0.0)
            mz = mz + jnp.where(last_row(mz), next_y, 0.0)
            curl = (
                by(mz, start == 0) - (my - below_y),
                (mx - below_x) - bx(mz, edge_z),
                bx(my, edge_y) - by(mx, start == 0),
            )
            if put is not None:
                for c, v in enumerate((mx, my, mz)):
                    put[c, z, :, pl.ds(low, high - low)] = v[:, low - start :]
            result.append([v[:, low - start :] for v in curl])
            below_x, below_y = mx, my
        return result

    def open_exchange(*chosen):
        pl.semaphore_wait(barrier, greeted)
        send(0, *chosen)

    downs = [4 + 2 * n for n in range(len(widths))]
    ups = [n + 1 for n in downs]
    both = [n for pair in zip(ups, downs) for n in pair]
    @pl.when(k == n_z - 1)
    def _():
        open_exchange(0, 1)
        wait_blocks(load_sem.at[3], 2 * nx * ny // 128)
        pl.when(~odd)(functools.partial(send, 0, *downs))
        send(0, 2)

    wait_blocks(load_sem.at[0], 6 * cell_blocks - 2 * nx * ny // 128)
    pl.when(k < n_z - 1)(functools.partial(wait_blocks, load_sem.at[3], 2 * nx * ny // 128))
    pl.when(odd & (k == n_z - 1))(functools.partial(send, 0, *downs))
    local_part(0, inner.at[0])
    pl.when(k < n_z - 1)(functools.partial(open_exchange, 0, 1, *both, 2))
    send(0, 3)
    hops = [1 << turn for turn in range((n_x - 1).bit_length())]
    told = [greet_line(line_sem.at[0], 1)]

    def tell():
        turn = len(told)
        if turn <= len(hops):
            pl.semaphore_wait(line_sem.at[turn - 1], told[-1])
            told.append(greet_line(line_sem.at[turn], hops[turn]) if turn < len(hops) else 0)

    perm_load.wait()
    wait_blocks(load_sem.at[1], 8 * cell_blocks)
    for z in range(nz):
        kind = mat[z]
        eps = jnp.full((nx, ny), perm[0], jnp.float32)
        for number in range(1, kinds):
            eps = jnp.where(kind == number, perm[number], eps)
        coef[z] = COURANT / eps
        for c in range(3):
            field[1, c, z] = coef[z] * outer[c, z]
    local_part(1, inner.at[1])
    send(1, *LINES)
    @pl.when(~odd)
    def _():
        for c in range(3):
            pair_give[c] = coef[nz - 1] * field[1, c, nz - 1]
        for c in range(2):
            pair_give[3 + c] = coef[0] * field[1, c, 0]
        for src, dst, wanted in (
            (pair_give.at[0:3], pair_weight.at[0:3], k < n_z - 1),
            (own.at[nz - 1], pair_own.at[0], k < n_z - 1),
            (pair_give.at[3:5], pair_weight.at[3:5], k > 0),
            (own.at[0], pair_own.at[1], k > 0),
        ):
            copy = pltpu.make_async_remote_copy(
                src_ref=src, dst_ref=dst, device_id=(i + 1, k), device_id_type=MESH,
                send_sem=send_sem, recv_sem=recv_sem.at[2],
            )
            pl.when(wanted)(copy.start)

    wait_exchange(plane_sent.at[0], 0, widths[0])
    if len(widths) > 1:
        pl.when(odd)(functools.partial(wait_exchange, plane_sent.at[1], 0, *widths[1:]))
    send(1, *PLANES)
    tell()

    for n, (low, high) in enumerate(spans[0]):
        wait_exchange(recv_sem.at[3 + n if n else 0], int(n == 0), high - low)
        change = finish(0, curl_in.at[0], low, high)
        keep = pl.ds(low, high - low)
        for z in range(nz):
            for c in range(3):
                moved = coef[z, :, keep] * change[z][c]
                curl_in[2, c, z, :, keep] = moved
                field[2, c, z, :, keep] = field[0, c, z, :, keep] + moved
        local_part(2, curl_in.at[0], *spans[2][n])
        if n == len(widths) - 1:
            send(2, 0, 1)
        send(2, *range(4 + 4 * n, 8 + 4 * n))
        if n == 0:
            tell()
    send(2, 2, 3)
    tell()

    wait_exchange(recv_sem.at[1], 1, ny)
    change = finish(1, curl_in.at[1])
    for z in range(nz):
        dot = None
        for c in range(3):
            now = outer[c, z] - COURANT * change[z][c]
            inner[1, c, z] = now
            field[3, c, z] = coef[z] * now
            term = now * curl_in[2, c, z]
            dot = term if dot is None else dot + term
        weight[z] = coef[z] * dot
    local_part(3, curl_in.at[1])
    send(3, *LINES)
    pl.when(~odd)(functools.partial(send, 3, *PLANES))
    pl.when(odd)(functools.partial(wait_exchange, recv_sem.at[2], 1, ny, pairs=1))
    pl.when(~odd)(functools.partial(wait_exchange, recv_sem.at[2], 1))
    change = finish(2, None)
    sums = [jnp.zeros((nx, 128), jnp.float32)] * NI
    planes = []
    for z in range(nz):
        dot = None
        for c in range(3):
            term = outer[c, z] * (coef[z] * change[z][c])
            dot = term if dot is None else dot + term
        planes.append((weight[z] + coef[z] * dot, own[z]))
    for both, which in planes:
        for t in range(0, ny, 128):
            part, index = both[:, t : t + 128], which[:, t : t + 128]
            for j in range(NI):
                sums[j] = sums[j] + jnp.where(index == j, part, 0.0)
    for j in range(NI):
        portion[j] = sums[j]

    def include(both, which):
        for j in range(NI):
            one = portion[j]
            for t in range(0, ny, 128):
                one = one + jnp.where(which[:, t : t + 128] == j, both[:, t : t + 128], 0.0)
            portion[j] = one

    pl.when(odd)(functools.partial(wait_exchange, recv_sem.at[5], 0, ny))

    @pl.when(odd & (k < n_z - 1))
    def _():
        push_x, push_y = -SCALES[0] * pair_zf[1], SCALES[0] * pair_zf[0]
        turn = bx(push_y, 0.0) - by(push_x, True)
        above = pair_weight[1] * push_x - pair_weight[0] * push_y + pair_weight[2] * turn
        include(above, pair_own[0])

    @pl.when(odd & (k > 0))
    def _():
        below = pair_weight[3] * pair_zl[1] - pair_weight[4] * pair_zl[0]
        include(below, pair_own[1])

    lane = lax.broadcasted_iota(jnp.int32, (NI, 128), 1)
    number = lax.broadcasted_iota(jnp.int32, (NI, 128), 0)
    table = jnp.zeros((NI, 128), jnp.float32)
    for j in range(NI):
        table = jnp.where(number == j, jnp.sum(portion[j], axis=0, keepdims=True), table)
    table = jnp.where(lane == number, jnp.sum(table, axis=1, keepdims=True), 0.0)
    row = jnp.sum(table, axis=0, keepdims=True)
    mine[0] = row
    gathered[me] = row

    while len(told) <= len(hops):
        tell()

    def share_sum(step, carry):
        other = jnp.where(step < me, step, step + 1)
        pltpu.make_async_remote_copy(
            src_ref=mine.at[0], dst_ref=gathered.at[me], send_sem=send_sem, recv_sem=sum_recv,
            device_id=(other // n_z, lax.rem(other, n_z)), device_id_type=MESH,
        ).start()
        return carry

    lax.fori_loop(0, total - 1, share_sum, 0)

    wait_exchange(plane_sent.at[2], 0, ny)
    pl.when(~odd & (i < n_x - 1))(functools.partial(signal, pair_sem, i + 1, k))

    @pl.when(odd)
    def _():
        pl.semaphore_wait(pair_sem, 1)
        send(3, *PLANES)

    wait_exchange(recv_sem.at[3], 1, ny)
    change = finish(3, ko_ref)
    for z in range(nz):
        for c in range(3):
            go_ref[c, z] = inner[1, c, z] - COURANT * change[z][c]
    for parity, pairs in ((odd, 0), (~odd, 1)):
        pl.when(parity)(
            functools.partial(
                wait_exchange, send_sem, 4, 2 * ny, pairs=pairs, extra=total - 1
            )
        )
    if len(widths) > 1:
        pl.when(~odd)(functools.partial(wait_exchange, plane_sent.at[1], 0, *widths[1:]))
    everyone = gathered.at[0 : total - 1]
    pltpu.make_async_copy(everyone, everyone, sum_recv).wait()
    grad_ref[...] = jnp.sum(gathered[...], axis=0)[:, :NI] / norm


def store(g_ref, h_ref, grad_ref, g_hbm, h_hbm, grad_hbm, sem):
    pltpu.make_async_copy(grad_ref, grad_hbm, sem.at[2]).start()
    for z in range(g_ref.shape[1]):
        pltpu.make_async_copy(g_ref.at[:, z], g_hbm.at[:, :, z, :], sem.at[0]).start()
        pltpu.make_async_copy(h_ref.at[:, z], h_hbm.at[:, :, z, :], sem.at[1]).start()
    for n, ref in enumerate((g_ref, h_ref, grad_ref)):
        pltpu.make_async_copy(ref, ref, sem.at[n]).wait()


def solution(mesh):
    n_x, n_z = mesh.shape["xy"], mesh.shape["gz"]

    def body(e_check, h_check, adj_e, adj_h, material, owner, permittivity):
        _, nx, nz, ny = e_check.shape
        cells = nx * n_x * nz * n_z * ny
        norm = np.sqrt(np.float32(cells / NI))
        dims = (n_x, n_z, nx, nz, ny, permittivity.shape[0], norm)
        f32 = jnp.float32
        hbm_spec = pl.BlockSpec(memory_space=pltpu.HBM)
        vmem_spec = pl.BlockSpec(memory_space=pltpu.VMEM)
        block = (3, nz, nx, ny)
        g, h, grad = pl.pallas_call(
            functools.partial(kernel, dims),
            out_shape=(
                pltpu.VMEM(block, f32), pltpu.VMEM(block, f32), pltpu.VMEM((1, NI), f32),
            ),
            in_specs=[hbm_spec] * 7,
            out_specs=(vmem_spec,) * 3,
            scratch_shapes=[
                pltpu.SMEM(permittivity.shape, f32),
                pltpu.VMEM((4,) + block, f32),
                pltpu.VMEM((2,) + block, f32),
                pltpu.VMEM((4,) + block, f32),
                pltpu.VMEM((3,) + block, f32),
                pltpu.VMEM(block, f32),
                pltpu.VMEM((nz, nx, ny), jnp.int32),
                pltpu.VMEM((nz, nx, ny), jnp.int32),
                pltpu.VMEM((nz, nx, ny), f32),
                pltpu.VMEM((nz, nx, ny), f32),
                pltpu.VMEM((4, 2, nz, ny), f32),
                pltpu.VMEM((4, 2 * nz, ny), f32),
                pltpu.VMEM((4, 1, ny), f32),
                pltpu.VMEM((4, 1, ny), f32),
                pltpu.VMEM((4, 2, nz, ny), f32),
                pltpu.VMEM((4, 2, nx, ny), f32),
                pltpu.VMEM((4, 2 * nz, ny), f32),
                pltpu.VMEM((4, 2, nx, ny), f32),
                pltpu.VMEM((4, 1, ny), f32),
                pltpu.VMEM((4, 1, ny), f32),
                pltpu.VMEM((1, 1, 128), f32),
                pltpu.VMEM((n_x * n_z, 1, 128), f32),
                pltpu.VMEM((16 * (1 + 2 * nz + 2 * nx) * ny // 128 + n_x * n_z, 1, 128), f32),
                pltpu.VMEM((2, nx, ny), f32),
                pltpu.VMEM((2, nx, ny), f32),
                pltpu.VMEM((5, nx, ny), f32),
                pltpu.VMEM((5, nx, ny), f32),
                pltpu.VMEM((2, nx, ny), jnp.int32),
                pltpu.VMEM((NI, nx, 128), f32),
                pltpu.SemaphoreType.DMA((4,)),
                pltpu.SemaphoreType.DMA,
                pltpu.SemaphoreType.DMA((3,)),
                pltpu.SemaphoreType.DMA((6,)),
                pltpu.SemaphoreType.DMA,
                pltpu.SemaphoreType.REGULAR((max(1, (n_x - 1).bit_length()),)),
                pltpu.SemaphoreType.REGULAR,
            ],
            compiler_params=pltpu.CompilerParams(
                collective_id=0, has_side_effects=True
            ),
            name="yee_adjoint",
        )(e_check, h_check, adj_e, adj_h, material, owner, permittivity)
        g, h, grad = pl.pallas_call(
            store,
            out_shape=(
                jax.ShapeDtypeStruct(e_check.shape, f32),
                jax.ShapeDtypeStruct(e_check.shape, f32),
                jax.ShapeDtypeStruct((1, NI), f32),
            ),
            in_specs=[vmem_spec] * 3,
            out_specs=(hbm_spec,) * 3,
            scratch_shapes=[pltpu.SemaphoreType.DMA((3,))],
            compiler_params=pltpu.CompilerParams(vmem_limit_bytes=2**20),
            name="store_outputs",
        )(g, h, grad)
        return g, h, grad.reshape(NI)

    split = P(None, "xy", "gz", None)
    return jax.shard_map(
        body,
        mesh=mesh,
        in_specs=(split,) * 4 + (P("xy", "gz", None),) * 2 + (P(),),
        out_specs=(split, split, P()),
        check_vma=False,
    )
```

```python
import functools
import itertools

import jax
import jax.numpy as jnp
import numpy as np
from jax import lax
from jax.experimental import pallas as pl
from jax.experimental.pallas import tpu as pltpu
from jax.sharding import PartitionSpec as P

NI = 8
COURANT = 0.5
MESH = pl.DeviceIdType.MESH
LINES, PLANES = (0, 1, 2, 3), (4, 5)
SCALES = (-COURANT, 1.0)


def kernel(
    dims, e_hbm, h_hbm, g_hbm, k_hbm, mat_hbm, own_hbm, perm_hbm,
    go_ref, ko_ref, grad_ref,
    perm, field, inner, partial, curl_in, outer, mat, own, coef, weight,
    send_xf, send_xl, send_d5, send_d6,
    got_xf, got_zf, got_xl, got_zl, got_d5, got_d6,
    mine, gathered, tally,
    pair_zf, pair_zl, pair_give, pair_weight, pair_own, portion,
    load_sem, send_sem, plane_sent, recv_sem, sum_recv,
    line_sem, pair_sem,
):
    n_x, n_z, nx, nz, ny, kinds, norm = dims
    total = n_x * n_z
    i = lax.axis_index("xy")
    k = lax.axis_index("gz")
    me = i * n_z + k
    odd = lax.rem(i, 2) == 1

    def load(src, dst, slot):
        for z in range(nz):
            src_z = src.at[:, :, z, :] if len(src.shape) == 4 else src.at[:, z, :]
            dst_z = dst.at[:, z] if len(dst.shape) == 4 else dst.at[z]
            pltpu.make_async_copy(src_z, dst_z, load_sem.at[slot]).start()

    def wait_blocks(sem, count):
        span = tally.at[0:count]
        pltpu.make_async_copy(span, span, sem).wait()

    cell_blocks = nx * nz * ny // 128

    barrier = pltpu.get_barrier_semaphore()

    def signal(sem, x, z):
        pl.semaphore_signal(sem, inc=1, device_id=(x, z), device_id_type=MESH)

    def greet(sem, partners):
        count = 0
        for cond, x, z in partners:
            pl.when(cond)(functools.partial(signal, sem, x, z))
            count = count + cond.astype(jnp.int32)
        return count

    def greet_line(sem, hop):
        return greet(sem, ((i >= hop, i - hop, k), (i < n_x - hop, i + hop, k)))

    load(e_hbm, field.at[0], 0)
    load(h_hbm, inner.at[0], 0)
    greeted = greet_line(barrier, 1) + greet(
        barrier,
        (
            ((i > 0) & (k < n_z - 1), i - 1, k + 1),
            ((i < n_x - 1) & (k > 0), i + 1, k - 1),
        ),
    )
    for step in range(1, n_z):
        signal(barrier, i, lax.rem(k + step, n_z))
    greeted = greeted + n_z - 1

    perm_load = pltpu.make_async_copy(perm_hbm, perm, load_sem.at[2])
    perm_load.start()
    load(mat_hbm, mat, 1)
    load(g_hbm, outer, 1)
    load(k_hbm, inner.at[1], 1)
    load(own_hbm, own, 1)

    rows = lax.broadcasted_iota(jnp.int32, (nx, ny), 0)
    lanes = lax.broadcasted_iota(jnp.int32, (nx, ny), 1)

    def first_row(v):
        return rows[:, : v.shape[1]] == 0

    def last_row(v):
        return rows[:, : v.shape[1]] == nx - 1

    def dy(v, whole):
        width = v.shape[1]
        later = pltpu.roll(v, width - 1, 1)
        return jnp.where(lanes[:, :width] == width - 1, 0.0, later) - v if whole else later - v

    def dx(v):
        return jnp.where(last_row(v), 0.0, pltpu.roll(v, nx - 1, 0)) - v

    def by(v, whole):
        earlier = pltpu.roll(v, 1, 1)
        return v - (jnp.where(lanes[:, : v.shape[1]] == 0, 0.0, earlier) if whole else earlier)

    def bx(v, row):
        return v - jnp.where(first_row(v), row, pltpu.roll(v, 1, 0))

    def local_part(q, mag, low=0, high=ny):
        scale = SCALES[q % 2]
        end = min(high + 128, ny)
        inside, keep = pl.ds(low, end - low), pl.ds(low, high - low)
        width = high - low

        def put(ref, index, v):
            ref[index + (keep,)] = v[:, :width]

        for z in range(nz):
            fx, fy, fz = (field[q, c, z, :, inside] for c in range(3))
            if z < nz - 1:
                up_x, up_y = (field[q, c, z + 1, :, inside] for c in range(2))
                up_x, up_y = up_x - fx, up_y - fy
            else:
                up_x, up_y = -fx, -fy
            whole = end == high
            lx = mag[0, z, :, inside] + scale * (dy(fz, whole) - up_y)
            ly = mag[1, z, :, inside] + scale * (up_x - dx(fz))
            lz = mag[2, z, :, inside] + scale * (dx(fy) - dy(fx, whole))
            for c, v in enumerate((lx, ly, lz)):
                put(partial, (q, c, z, slice(None)), v)
            if q:
                put(send_xf, (q, 0, slice(z, z + 1)), fy[0:1])
                put(send_xf, (q, 1, slice(z, z + 1)), fz[0:1])
            put(send_xl, (q, slice(z, z + 1)), ly[nx - 1 : nx])
            put(send_xl, (q, slice(nz + z, nz + z + 1)), lz[nx - 1 : nx])
            if q and z == 0:
                put(send_d5, (q, slice(None)), fx[nx - 1 : nx])
            if q and z == nz - 1:
                put(send_d6, (q, slice(None)), fz[0:1])

    spans = [((0, ny),)] * 4
    if ny % 1024 == 0:
        cuts = [ny // 8 * n for n in (4,)]
        spans[0] = tuple(zip([0] + cuts, cuts + [ny]))
        ahead = [n - 128 for n in cuts]
        spans[2] = tuple(zip([0] + ahead, ahead + [ny]))
    widths = [high - low for low, high in spans[0]]

    def messages(q):
        below_x, above_x = i > 0, i < n_x - 1
        below_z, above_z = k > 0, k < n_z - 1
        sources = (
            (
                e_hbm.at[0, nx - 1 : nx, 0], e_hbm.at[2, 0:1, nz - 1],
                e_hbm.at[1:3, 0], e_hbm.at[0:2, :, 0],
            )
            if q == 0
            else (send_d5.at[q], send_d6.at[q], send_xf.at[q], field.at[q, 0:2, 0])
        )
        table = [
            (sources[0], got_d5.at[q], (i + 1, k - 1), above_x & below_z),
            (sources[1], got_d6.at[q], (i - 1, k + 1), below_x & above_z),
            (sources[2], got_xf.at[q], (i - 1, k), below_x),
            (send_xl.at[q], got_xl.at[q], (i + 1, k), above_x),
        ]
        top = partial.at[q, 0:2, nz - 1]
        for low, high in spans[q]:
            keep = pl.ds(low, high - low)
            planes = [
                (sources[3], got_zf.at[q], (i, k - 1), below_z),
                (top, got_zl.at[q], (i, k + 1), above_z),
            ]
            if q == 2:
                planes = [(*row[:3], row[3] & odd) for row in planes]
                planes.append((sources[3], pair_zf, (i + 1, k - 1), below_z & ~odd))
                planes.append((top, pair_zl, (i + 1, k + 1), above_z & ~odd))
            for src, got, target, sends in planes:
                table.append((src.at[:, :, keep], got.at[:, :, keep], target, sends))
        return table

    def send(q, *chosen):
        table = messages(q)
        for m in chosen:
            src, dst, target, sends = table[m]
            sent, late = send_sem, max(m // 2 - 2, 0) if q == 0 else 0
            if m >= 4 and q % 2 == 0:
                sent = plane_sent.at[q + min(late, 1)]
            landing = 3 + late if late else q
            if q == 2 and m >= 4 and m % 4 > 1:
                landing = 5
            copy = pltpu.make_async_remote_copy(
                src_ref=src, dst_ref=dst, device_id=target, device_id_type=MESH,
                send_sem=sent, recv_sem=recv_sem.at[landing],
            )
            pl.when(sends)(copy.start)

    sides = []
    for below_x, above_x, below_z, above_z in itertools.product((False, True), repeat=4):
        if below_x + above_x > n_x - 1 or below_z + above_z > n_z - 1:
            continue
        if (n_x > 1 and not below_x + above_x) or (n_z > 1 and not below_z + above_z):
            continue
        here = ((i > 0) == below_x) & ((i < n_x - 1) == above_x)
        here = here & ((k > 0) == below_z) & ((k < n_z - 1) == above_z)
        length = (above_x & below_z) + (below_x & above_z) + 2 * nz * (below_x + above_x)
        sides.append((here, length, nx * below_z, nx * above_z))

    def wait_exchange(sem, lines, *widths, pairs=0, extra=0):
        for here, length, below, above in sides:
            count = lines * length * ny + 2 * (below + above) * sum(widths)
            count = (count + pairs * (3 * below + 4 * above) * ny) // 128 + extra
            if count:
                span = tally.at[0:count]
                pl.when(here)(pltpu.make_async_copy(span, span, sem).wait)

    def finish(q, put, low=0, high=ny):
        scale = SCALES[q % 2]
        start = max(low - 128, 0)
        inside = pl.ds(start, high - start)
        not_first_x, not_last_x = i > 0, i < n_x - 1
        not_first_z, not_last_z = k > 0, k < n_z - 1

        def only(cond, v):
            return jnp.where(cond, v, 0.0)

        def f(c, z, part=slice(None)):
            return field[q, c, z, part, inside]

        bottom_x, bottom_y = got_zl[q, 0, :, inside], got_zl[q, 1, :, inside]
        top_x, top_y = got_zf[q, 0, :, inside], got_zf[q, 1, :, inside]
        if q == 2:
            bottom_x, bottom_y, top_x, top_y = (
                only(odd, v) for v in (bottom_x, bottom_y, top_x, top_y)
            )
        below_x = only(not_first_z, bottom_x - scale * f(1, 0))
        below_y = bottom_y + scale * f(0, 0)
        diagonal = only(not_last_x, scale * got_d6[q, :, inside])
        below_y = only(not_first_z, below_y - jnp.where(last_row(below_y), diagonal, 0.0))
        result = []
        for z in range(nz):
            mx, my, mz = (partial[q, c, z, :, inside] for c in range(3))
            edge_y = got_xl[q, z : z + 1, inside] - scale * f(2, z, slice(0, 1))
            edge_z = got_xl[q, nz + z : nz + z + 1, inside] + scale * f(1, z, slice(0, 1))
            if z == nz - 1:
                mx = mx - only(not_last_z, scale * top_y)
                my = my + only(not_last_z, scale * top_x)
                edge_y = edge_y + only(not_last_z, scale * got_d5[q, :, inside])
            edge_y, edge_z = only(not_first_x, edge_y), only(not_first_x, edge_z)
            next_y = only(not_last_x, scale * got_xf[q, 0, z : z + 1, inside])
            next_z = only(not_last_x, scale * got_xf[q, 1, z : z + 1, inside])
            my = my - jnp.where(last_row(my), next_z, 0.0)
            mz = mz + jnp.where(last_row(mz), next_y, 0.0)
            curl = (
                by(mz, start == 0) - (my - below_y),
                (mx - below_x) - bx(mz, edge_z),
                bx(my, edge_y) - by(mx, start == 0),
            )
            if put is not None:
                for c, v in enumerate((mx, my, mz)):
                    put[c, z, :, pl.ds(low, high - low)] = v[:, low - start :]
            result.append([v[:, low - start :] for v in curl])
            below_x, below_y = mx, my
        return result

    def open_exchange(*chosen):
        pl.semaphore_wait(barrier, greeted)
        send(0, *chosen)

    downs = [4 + 2 * n for n in range(len(widths))]
    ups = [n + 1 for n in downs]
    both = [n for pair in zip(ups, downs) for n in pair]
    @pl.when(k == n_z - 1)
    def _():
        open_exchange(0, 1)
        pl.when(~odd)(functools.partial(send, 0, *downs))
        send(0, 2)

    wait_blocks(load_sem.at[0], 6 * cell_blocks)
    pl.when(odd & (k == n_z - 1))(functools.partial(send, 0, *downs))
    local_part(0, inner.at[0])
    pl.when(k < n_z - 1)(functools.partial(open_exchange, 0, 1, *both, 2))
    send(0, 3)
    hops = [1 << turn for turn in range((n_x - 1).bit_length())]
    told = [greet_line(line_sem.at[0], 1)]

    def tell():
        turn = len(told)
        if turn <= len(hops):
            pl.semaphore_wait(line_sem.at[turn - 1], told[-1])
            told.append(greet_line(line_sem.at[turn], hops[turn]) if turn < len(hops) else 0)

    perm_load.wait()
    wait_blocks(load_sem.at[1], 8 * cell_blocks)
    for z in range(nz):
        kind = mat[z]
        eps = jnp.full((nx, ny), perm[0], jnp.float32)
        for number in range(1, kinds):
            eps = jnp.where(kind == number, perm[number], eps)
        coef[z] = COURANT / eps
        for c in range(3):
            field[1, c, z] = coef[z] * outer[c, z]
    local_part(1, inner.at[1])
    send(1, *LINES)
    @pl.when(~odd)
    def _():
        for c in range(3):
            pair_give[c] = coef[nz - 1] * field[1, c, nz - 1]
        for c in range(2):
            pair_give[3 + c] = coef[0] * field[1, c, 0]
        for src, dst, wanted in (
            (pair_give.at[0:3], pair_weight.at[0:3], k < n_z - 1),
            (own.at[nz - 1], pair_own.at[0], k < n_z - 1),
            (pair_give.at[3:5], pair_weight.at[3:5], k > 0),
            (own.at[0], pair_own.at[1], k > 0),
        ):
            copy = pltpu.make_async_remote_copy(
                src_ref=src, dst_ref=dst, device_id=(i + 1, k), device_id_type=MESH,
                send_sem=send_sem, recv_sem=recv_sem.at[2],
            )
            pl.when(wanted)(copy.start)

    wait_exchange(plane_sent.at[0], 0, widths[0])
    if len(widths) > 1:
        pl.when(odd)(functools.partial(wait_exchange, plane_sent.at[1], 0, *widths[1:]))
    send(1, *PLANES)
    tell()

    for n, (low, high) in enumerate(spans[0]):
        wait_exchange(recv_sem.at[3 + n if n else 0], int(n == 0), high - low)
        change = finish(0, curl_in.at[0], low, high)
        keep = pl.ds(low, high - low)
        for z in range(nz):
            for c in range(3):
                moved = coef[z, :, keep] * change[z][c]
                curl_in[2, c, z, :, keep] = moved
                field[2, c, z, :, keep] = field[0, c, z, :, keep] + moved
        local_part(2, curl_in.at[0], *spans[2][n])
        if n == len(widths) - 1:
            send(2, 0, 1)
        send(2, *range(4 + 4 * n, 8 + 4 * n))
        if n == 0:
            tell()
    send(2, 2, 3)
    tell()

    wait_exchange(recv_sem.at[1], 1, ny)
    change = finish(1, curl_in.at[1])
    for z in range(nz):
        dot = None
        for c in range(3):
            now = outer[c, z] - COURANT * change[z][c]
            inner[1, c, z] = now
            field[3, c, z] = coef[z] * now
            term = now * curl_in[2, c, z]
            dot = term if dot is None else dot + term
        weight[z] = coef[z] * dot
    local_part(3, curl_in.at[1])
    send(3, *LINES)
    pl.when(~odd)(functools.partial(send, 3, *PLANES))
    pl.when(odd)(functools.partial(wait_exchange, recv_sem.at[2], 1, ny, pairs=1))
    pl.when(~odd)(functools.partial(wait_exchange, recv_sem.at[2], 1))
    change = finish(2, None)
    sums = [jnp.zeros((nx, 128), jnp.float32)] * NI
    planes = []
    for z in range(nz):
        dot = None
        for c in range(3):
            term = outer[c, z] * (coef[z] * change[z][c])
            dot = term if dot is None else dot + term
        planes.append((weight[z] + coef[z] * dot, own[z]))
    for both, which in planes:
        for t in range(0, ny, 128):
            part, index = both[:, t : t + 128], which[:, t : t + 128]
            for j in range(NI):
                sums[j] = sums[j] + jnp.where(index == j, part, 0.0)
    for j in range(NI):
        portion[j] = sums[j]

    def include(both, which):
        for j in range(NI):
            one = portion[j]
            for t in range(0, ny, 128):
                one = one + jnp.where(which[:, t : t + 128] == j, both[:, t : t + 128], 0.0)
            portion[j] = one

    pl.when(odd)(functools.partial(wait_exchange, recv_sem.at[5], 0, ny))

    @pl.when(odd & (k < n_z - 1))
    def _():
        push_x, push_y = -SCALES[0] * pair_zf[1], SCALES[0] * pair_zf[0]
        turn = bx(push_y, 0.0) - by(push_x, True)
        above = pair_weight[1] * push_x - pair_weight[0] * push_y + pair_weight[2] * turn
        include(above, pair_own[0])

    @pl.when(odd & (k > 0))
    def _():
        below = pair_weight[3] * pair_zl[1] - pair_weight[4] * pair_zl[0]
        include(below, pair_own[1])

    lane = lax.broadcasted_iota(jnp.int32, (NI, 128), 1)
    number = lax.broadcasted_iota(jnp.int32, (NI, 128), 0)
    table = jnp.zeros((NI, 128), jnp.float32)
    for j in range(NI):
        table = jnp.where(number == j, jnp.sum(portion[j], axis=0, keepdims=True), table)
    table = jnp.where(lane == number, jnp.sum(table, axis=1, keepdims=True), 0.0)
    row = jnp.sum(table, axis=0, keepdims=True)
    mine[0] = row
    gathered[me] = row

    while len(told) <= len(hops):
        tell()

    def share_sum(step, carry):
        other = jnp.where(step < me, step, step + 1)
        pltpu.make_async_remote_copy(
            src_ref=mine.at[0], dst_ref=gathered.at[me], send_sem=send_sem, recv_sem=sum_recv,
            device_id=(other // n_z, lax.rem(other, n_z)), device_id_type=MESH,
        ).start()
        return carry

    lax.fori_loop(0, total - 1, share_sum, 0)

    wait_exchange(plane_sent.at[2], 0, ny)
    pl.when(~odd & (i < n_x - 1))(functools.partial(signal, pair_sem, i + 1, k))

    @pl.when(odd)
    def _():
        pl.semaphore_wait(pair_sem, 1)
        send(3, *PLANES)

    wait_exchange(recv_sem.at[3], 1, ny)
    change = finish(3, ko_ref)
    for z in range(nz):
        for c in range(3):
            go_ref[c, z] = inner[1, c, z] - COURANT * change[z][c]
    for parity, pairs in ((odd, 0), (~odd, 1)):
        pl.when(parity)(
            functools.partial(
                wait_exchange, send_sem, 4, 2 * ny, pairs=pairs, extra=total - 1
            )
        )
    if len(widths) > 1:
        pl.when(~odd)(functools.partial(wait_exchange, plane_sent.at[1], 0, *widths[1:]))
    everyone = gathered.at[0 : total - 1]
    pltpu.make_async_copy(everyone, everyone, sum_recv).wait()
    grad_ref[...] = jnp.sum(gathered[...], axis=0)[:, :NI] / norm


def store(g_ref, h_ref, grad_ref, g_hbm, h_hbm, grad_hbm, sem):
    pltpu.make_async_copy(grad_ref, grad_hbm, sem.at[2]).start()
    for z in range(g_ref.shape[1]):
        pltpu.make_async_copy(g_ref.at[:, z], g_hbm.at[:, :, z, :], sem.at[0]).start()
        pltpu.make_async_copy(h_ref.at[:, z], h_hbm.at[:, :, z, :], sem.at[1]).start()
    for n, ref in enumerate((g_ref, h_ref, grad_ref)):
        pltpu.make_async_copy(ref, ref, sem.at[n]).wait()


def solution(mesh):
    n_x, n_z = mesh.shape["xy"], mesh.shape["gz"]

    def body(e_check, h_check, adj_e, adj_h, material, owner, permittivity):
        _, nx, nz, ny = e_check.shape
        cells = nx * n_x * nz * n_z * ny
        norm = np.sqrt(np.float32(cells / NI))
        dims = (n_x, n_z, nx, nz, ny, permittivity.shape[0], norm)
        f32 = jnp.float32
        hbm_spec = pl.BlockSpec(memory_space=pltpu.HBM)
        vmem_spec = pl.BlockSpec(memory_space=pltpu.VMEM)
        block = (3, nz, nx, ny)
        g, h, grad = pl.pallas_call(
            functools.partial(kernel, dims),
            out_shape=(
                pltpu.VMEM(block, f32), pltpu.VMEM(block, f32), pltpu.VMEM((1, NI), f32),
            ),
            in_specs=[hbm_spec] * 7,
            out_specs=(vmem_spec,) * 3,
            scratch_shapes=[
                pltpu.SMEM(permittivity.shape, f32),
                pltpu.VMEM((4,) + block, f32),
                pltpu.VMEM((2,) + block, f32),
                pltpu.VMEM((4,) + block, f32),
                pltpu.VMEM((3,) + block, f32),
                pltpu.VMEM(block, f32),
                pltpu.VMEM((nz, nx, ny), jnp.int32),
                pltpu.VMEM((nz, nx, ny), jnp.int32),
                pltpu.VMEM((nz, nx, ny), f32),
                pltpu.VMEM((nz, nx, ny), f32),
                pltpu.VMEM((4, 2, nz, ny), f32),
                pltpu.VMEM((4, 2 * nz, ny), f32),
                pltpu.VMEM((4, 1, ny), f32),
                pltpu.VMEM((4, 1, ny), f32),
                pltpu.VMEM((4, 2, nz, ny), f32),
                pltpu.VMEM((4, 2, nx, ny), f32),
                pltpu.VMEM((4, 2 * nz, ny), f32),
                pltpu.VMEM((4, 2, nx, ny), f32),
                pltpu.VMEM((4, 1, ny), f32),
                pltpu.VMEM((4, 1, ny), f32),
                pltpu.VMEM((1, 1, 128), f32),
                pltpu.VMEM((n_x * n_z, 1, 128), f32),
                pltpu.VMEM((16 * (1 + 2 * nz + 2 * nx) * ny // 128 + n_x * n_z, 1, 128), f32),
                pltpu.VMEM((2, nx, ny), f32),
                pltpu.VMEM((2, nx, ny), f32),
                pltpu.VMEM((5, nx, ny), f32),
                pltpu.VMEM((5, nx, ny), f32),
                pltpu.VMEM((2, nx, ny), jnp.int32),
                pltpu.VMEM((NI, nx, 128), f32),
                pltpu.SemaphoreType.DMA((3,)),
                pltpu.SemaphoreType.DMA,
                pltpu.SemaphoreType.DMA((3,)),
                pltpu.SemaphoreType.DMA((6,)),
                pltpu.SemaphoreType.DMA,
                pltpu.SemaphoreType.REGULAR((max(1, (n_x - 1).bit_length()),)),
                pltpu.SemaphoreType.REGULAR,
            ],
            compiler_params=pltpu.CompilerParams(
                collective_id=0, has_side_effects=True
            ),
            name="yee_adjoint",
        )(e_check, h_check, adj_e, adj_h, material, owner, permittivity)
        g, h, grad = pl.pallas_call(
            store,
            out_shape=(
                jax.ShapeDtypeStruct(e_check.shape, f32),
                jax.ShapeDtypeStruct(e_check.shape, f32),
                jax.ShapeDtypeStruct((1, NI), f32),
            ),
            in_specs=[vmem_spec] * 3,
            out_specs=(hbm_spec,) * 3,
            scratch_shapes=[pltpu.SemaphoreType.DMA((3,))],
            compiler_params=pltpu.CompilerParams(vmem_limit_bytes=2**20),
            name="store_outputs",
        )(g, h, grad)
        return g, h, grad.reshape(NI)

    split = P(None, "xy", "gz", None)
    return jax.shard_map(
        body,
        mesh=mesh,
        in_specs=(split,) * 4 + (P("xy", "gz", None),) * 2 + (P(),),
        out_specs=(split, split, P()),
        check_vma=False,
    )
```

```python
import functools
import itertools

import jax
import jax.numpy as jnp
import numpy as np
from jax import lax
from jax.experimental import pallas as pl
from jax.experimental.pallas import tpu as pltpu
from jax.sharding import PartitionSpec as P

NI = 8
COURANT = 0.5
MESH = pl.DeviceIdType.MESH
LINES, PLANES = (0, 1, 2, 3), (4, 5)
SCALES = (-COURANT, 1.0)


def kernel(
    dims, e_hbm, h_hbm, g_hbm, k_hbm, mat_hbm, own_hbm, perm_hbm,
    go_ref, ko_ref, grad_ref,
    perm, field, inner, partial, curl_in, outer, mat, own, coef, weight,
    send_xf, send_xl, send_d5, send_d6,
    got_xf, got_zf, got_xl, got_zl, got_d5, got_d6,
    mine, gathered, tally,
    pair_zf, pair_zl, pair_give, pair_weight, pair_own, portion,
    load_sem, send_sem, plane_sent, recv_sem, sum_recv,
    line_sem, pair_sem,
):
    n_x, n_z, nx, nz, ny, kinds, norm = dims
    total = n_x * n_z
    i = lax.axis_index("xy")
    k = lax.axis_index("gz")
    me = i * n_z + k
    odd = lax.rem(i, 2) == 1

    def load(src, dst, slot):
        for z in range(nz):
            src_z = src.at[:, :, z, :] if len(src.shape) == 4 else src.at[:, z, :]
            dst_z = dst.at[:, z] if len(dst.shape) == 4 else dst.at[z]
            pltpu.make_async_copy(src_z, dst_z, load_sem.at[slot]).start()

    def wait_blocks(sem, count):
        span = tally.at[0:count]
        pltpu.make_async_copy(span, span, sem).wait()

    cell_blocks = nx * nz * ny // 128

    barrier = pltpu.get_barrier_semaphore()

    def signal(sem, x, z):
        pl.semaphore_signal(sem, inc=1, device_id=(x, z), device_id_type=MESH)

    def greet(sem, partners):
        count = 0
        for cond, x, z in partners:
            pl.when(cond)(functools.partial(signal, sem, x, z))
            count = count + cond.astype(jnp.int32)
        return count

    def greet_line(sem, hop):
        return greet(sem, ((i >= hop, i - hop, k), (i < n_x - hop, i + hop, k)))

    for step in range(1, n_z):
        signal(barrier, i, lax.rem(k + step, n_z))
    greeted = greet_line(barrier, 1) + greet(
        barrier,
        (
            ((i > 0) & (k < n_z - 1), i - 1, k + 1),
            ((i < n_x - 1) & (k > 0), i + 1, k - 1),
        ),
    )
    greeted = greeted + n_z - 1
    load(e_hbm, field.at[0], 0)
    load(h_hbm, inner.at[0], 0)

    perm_load = pltpu.make_async_copy(perm_hbm, perm, load_sem.at[2])
    perm_load.start()
    load(mat_hbm, mat, 1)
    load(g_hbm, outer, 1)
    load(k_hbm, inner.at[1], 1)
    load(own_hbm, own, 1)

    rows = lax.broadcasted_iota(jnp.int32, (nx, ny), 0)
    lanes = lax.broadcasted_iota(jnp.int32, (nx, ny), 1)

    def first_row(v):
        return rows[:, : v.shape[1]] == 0

    def last_row(v):
        return rows[:, : v.shape[1]] == nx - 1

    def dy(v, whole):
        width = v.shape[1]
        later = pltpu.roll(v, width - 1, 1)
        return jnp.where(lanes[:, :width] == width - 1, 0.0, later) - v if whole else later - v

    def dx(v):
        return jnp.where(last_row(v), 0.0, pltpu.roll(v, nx - 1, 0)) - v

    def by(v, whole):
        earlier = pltpu.roll(v, 1, 1)
        return v - (jnp.where(lanes[:, : v.shape[1]] == 0, 0.0, earlier) if whole else earlier)

    def bx(v, row):
        return v - jnp.where(first_row(v), row, pltpu.roll(v, 1, 0))

    def local_part(q, mag, low=0, high=ny):
        scale = SCALES[q % 2]
        end = min(high + 128, ny)
        inside, keep = pl.ds(low, end - low), pl.ds(low, high - low)
        width = high - low

        def put(ref, index, v):
            ref[index + (keep,)] = v[:, :width]

        for z in range(nz):
            fx, fy, fz = (field[q, c, z, :, inside] for c in range(3))
            if z < nz - 1:
                up_x, up_y = (field[q, c, z + 1, :, inside] for c in range(2))
                up_x, up_y = up_x - fx, up_y - fy
            else:
                up_x, up_y = -fx, -fy
            whole = end == high
            lx = mag[0, z, :, inside] + scale * (dy(fz, whole) - up_y)
            ly = mag[1, z, :, inside] + scale * (up_x - dx(fz))
            lz = mag[2, z, :, inside] + scale * (dx(fy) - dy(fx, whole))
            for c, v in enumerate((lx, ly, lz)):
                put(partial, (q, c, z, slice(None)), v)
            if q:
                put(send_xf, (q, 0, slice(z, z + 1)), fy[0:1])
                put(send_xf, (q, 1, slice(z, z + 1)), fz[0:1])
            put(send_xl, (q, slice(z, z + 1)), ly[nx - 1 : nx])
            put(send_xl, (q, slice(nz + z, nz + z + 1)), lz[nx - 1 : nx])
            if q and z == 0:
                put(send_d5, (q, slice(None)), fx[nx - 1 : nx])
            if q and z == nz - 1:
                put(send_d6, (q, slice(None)), fz[0:1])

    spans = [((0, ny),)] * 4
    if ny % 1024 == 0:
        cuts = [ny // 8 * n for n in (4,)]
        spans[0] = tuple(zip([0] + cuts, cuts + [ny]))
        ahead = [n - 128 for n in cuts]
        spans[2] = tuple(zip([0] + ahead, ahead + [ny]))
    widths = [high - low for low, high in spans[0]]

    def messages(q):
        below_x, above_x = i > 0, i < n_x - 1
        below_z, above_z = k > 0, k < n_z - 1
        sources = (
            (
                e_hbm.at[0, nx - 1 : nx, 0], e_hbm.at[2, 0:1, nz - 1],
                e_hbm.at[1:3, 0], e_hbm.at[0:2, :, 0],
            )
            if q == 0
            else (send_d5.at[q], send_d6.at[q], send_xf.at[q], field.at[q, 0:2, 0])
        )
        table = [
            (sources[0], got_d5.at[q], (i + 1, k - 1), above_x & below_z),
            (sources[1], got_d6.at[q], (i - 1, k + 1), below_x & above_z),
            (sources[2], got_xf.at[q], (i - 1, k), below_x),
            (send_xl.at[q], got_xl.at[q], (i + 1, k), above_x),
        ]
        top = partial.at[q, 0:2, nz - 1]
        for low, high in spans[q]:
            keep = pl.ds(low, high - low)
            planes = [
                (sources[3], got_zf.at[q], (i, k - 1), below_z),
                (top, got_zl.at[q], (i, k + 1), above_z),
            ]
            if q == 2:
                planes = [(*row[:3], row[3] & odd) for row in planes]
                planes.append((sources[3], pair_zf, (i + 1, k - 1), below_z & ~odd))
                planes.append((top, pair_zl, (i + 1, k + 1), above_z & ~odd))
            for src, got, target, sends in planes:
                table.append((src.at[:, :, keep], got.at[:, :, keep], target, sends))
        return table

    def send(q, *chosen):
        table = messages(q)
        for m in chosen:
            src, dst, target, sends = table[m]
            sent, late = send_sem, max(m // 2 - 2, 0) if q == 0 else 0
            if m >= 4 and q % 2 == 0:
                sent = plane_sent.at[q + min(late, 1)]
            landing = 3 + late if late else q
            if q == 2 and m >= 4 and m % 4 > 1:
                landing = 5
            copy = pltpu.make_async_remote_copy(
                src_ref=src, dst_ref=dst, device_id=target, device_id_type=MESH,
                send_sem=sent, recv_sem=recv_sem.at[landing],
            )
            pl.when(sends)(copy.start)

    sides = []
    for below_x, above_x, below_z, above_z in itertools.product((False, True), repeat=4):
        if below_x + above_x > n_x - 1 or below_z + above_z > n_z - 1:
            continue
        if (n_x > 1 and not below_x + above_x) or (n_z > 1 and not below_z + above_z):
            continue
        here = ((i > 0) == below_x) & ((i < n_x - 1) == above_x)
        here = here & ((k > 0) == below_z) & ((k < n_z - 1) == above_z)
        length = (above_x & below_z) + (below_x & above_z) + 2 * nz * (below_x + above_x)
        sides.append((here, length, nx * below_z, nx * above_z))

    def wait_exchange(sem, lines, *widths, pairs=0, extra=0):
        for here, length, below, above in sides:
            count = lines * length * ny + 2 * (below + above) * sum(widths)
            count = (count + pairs * (3 * below + 4 * above) * ny) // 128 + extra
            if count:
                span = tally.at[0:count]
                pl.when(here)(pltpu.make_async_copy(span, span, sem).wait)

    def finish(q, put, low=0, high=ny):
        scale = SCALES[q % 2]
        start = max(low - 128, 0)
        inside = pl.ds(start, high - start)
        not_first_x, not_last_x = i > 0, i < n_x - 1
        not_first_z, not_last_z = k > 0, k < n_z - 1

        def only(cond, v):
            return jnp.where(cond, v, 0.0)

        def f(c, z, part=slice(None)):
            return field[q, c, z, part, inside]

        bottom_x, bottom_y = got_zl[q, 0, :, inside], got_zl[q, 1, :, inside]
        top_x, top_y = got_zf[q, 0, :, inside], got_zf[q, 1, :, inside]
        if q == 2:
            bottom_x, bottom_y, top_x, top_y = (
                only(odd, v) for v in (bottom_x, bottom_y, top_x, top_y)
            )
        below_x = only(not_first_z, bottom_x - scale * f(1, 0))
        below_y = bottom_y + scale * f(0, 0)
        diagonal = only(not_last_x, scale * got_d6[q, :, inside])
        below_y = only(not_first_z, below_y - jnp.where(last_row(below_y), diagonal, 0.0))
        result = []
        for z in range(nz):
            mx, my, mz = (partial[q, c, z, :, inside] for c in range(3))
            edge_y = got_xl[q, z : z + 1, inside] - scale * f(2, z, slice(0, 1))
            edge_z = got_xl[q, nz + z : nz + z + 1, inside] + scale * f(1, z, slice(0, 1))
            if z == nz - 1:
                mx = mx - only(not_last_z, scale * top_y)
                my = my + only(not_last_z, scale * top_x)
                edge_y = edge_y + only(not_last_z, scale * got_d5[q, :, inside])
            edge_y, edge_z = only(not_first_x, edge_y), only(not_first_x, edge_z)
            next_y = only(not_last_x, scale * got_xf[q, 0, z : z + 1, inside])
            next_z = only(not_last_x, scale * got_xf[q, 1, z : z + 1, inside])
            my = my - jnp.where(last_row(my), next_z, 0.0)
            mz = mz + jnp.where(last_row(mz), next_y, 0.0)
            curl = (
                by(mz, start == 0) - (my - below_y),
                (mx - below_x) - bx(mz, edge_z),
                bx(my, edge_y) - by(mx, start == 0),
            )
            if put is not None:
                for c, v in enumerate((mx, my, mz)):
                    put[c, z, :, pl.ds(low, high - low)] = v[:, low - start :]
            result.append([v[:, low - start :] for v in curl])
            below_x, below_y = mx, my
        return result

    def open_exchange(*chosen):
        pl.semaphore_wait(barrier, greeted)
        send(0, *chosen)

    downs = [4 + 2 * n for n in range(len(widths))]
    ups = [n + 1 for n in downs]
    both = [n for pair in zip(ups, downs) for n in pair]
    @pl.when(k == n_z - 1)
    def _():
        open_exchange(0, 1)
        pl.when(~odd)(functools.partial(send, 0, *downs))
        send(0, 2)

    wait_blocks(load_sem.at[0], 6 * cell_blocks)
    pl.when(odd & (k == n_z - 1))(functools.partial(send, 0, *downs))
    local_part(0, inner.at[0])
    pl.when(k < n_z - 1)(functools.partial(open_exchange, 0, 1, *both, 2))
    send(0, 3)
    hops = [1 << turn for turn in range((n_x - 1).bit_length())]
    told = [greet_line(line_sem.at[0], 1)]

    def tell():
        turn = len(told)
        if turn <= len(hops):
            pl.semaphore_wait(line_sem.at[turn - 1], told[-1])
            told.append(greet_line(line_sem.at[turn], hops[turn]) if turn < len(hops) else 0)

    perm_load.wait()
    wait_blocks(load_sem.at[1], 8 * cell_blocks)
    for z in range(nz):
        kind = mat[z]
        eps = jnp.full((nx, ny), perm[0], jnp.float32)
        for number in range(1, kinds):
            eps = jnp.where(kind == number, perm[number], eps)
        coef[z] = COURANT / eps
        for c in range(3):
            field[1, c, z] = coef[z] * outer[c, z]
    local_part(1, inner.at[1])
    send(1, *LINES)
    @pl.when(~odd)
    def _():
        for c in range(3):
            pair_give[c] = coef[nz - 1] * field[1, c, nz - 1]
        for c in range(2):
            pair_give[3 + c] = coef[0] * field[1, c, 0]
        for src, dst, wanted in (
            (pair_give.at[0:3], pair_weight.at[0:3], k < n_z - 1),
            (own.at[nz - 1], pair_own.at[0], k < n_z - 1),
            (pair_give.at[3:5], pair_weight.at[3:5], k > 0),
            (own.at[0], pair_own.at[1], k > 0),
        ):
            copy = pltpu.make_async_remote_copy(
                src_ref=src, dst_ref=dst, device_id=(i + 1, k), device_id_type=MESH,
                send_sem=send_sem, recv_sem=recv_sem.at[2],
            )
            pl.when(wanted)(copy.start)

    wait_exchange(plane_sent.at[0], 0, widths[0])
    if len(widths) > 1:
        pl.when(odd)(functools.partial(wait_exchange, plane_sent.at[1], 0, *widths[1:]))
    send(1, *PLANES)
    tell()

    for n, (low, high) in enumerate(spans[0]):
        wait_exchange(recv_sem.at[3 + n if n else 0], int(n == 0), high - low)
        change = finish(0, curl_in.at[0], low, high)
        keep = pl.ds(low, high - low)
        for z in range(nz):
            for c in range(3):
                moved = coef[z, :, keep] * change[z][c]
                curl_in[2, c, z, :, keep] = moved
                field[2, c, z, :, keep] = field[0, c, z, :, keep] + moved
        local_part(2, curl_in.at[0], *spans[2][n])
        if n == len(widths) - 1:
            send(2, 0, 1)
        send(2, *range(4 + 4 * n, 8 + 4 * n))
        if n == 0:
            tell()
    send(2, 2, 3)
    tell()

    wait_exchange(recv_sem.at[1], 1, ny)
    change = finish(1, curl_in.at[1])
    for z in range(nz):
        dot = None
        for c in range(3):
            now = outer[c, z] - COURANT * change[z][c]
            inner[1, c, z] = now
            field[3, c, z] = coef[z] * now
            term = now * curl_in[2, c, z]
            dot = term if dot is None else dot + term
        weight[z] = coef[z] * dot
    local_part(3, curl_in.at[1])
    send(3, *LINES)
    pl.when(~odd)(functools.partial(send, 3, *PLANES))
    pl.when(odd)(functools.partial(wait_exchange, recv_sem.at[2], 1, ny, pairs=1))
    pl.when(~odd)(functools.partial(wait_exchange, recv_sem.at[2], 1))
    change = finish(2, None)
    sums = [jnp.zeros((nx, 128), jnp.float32)] * NI
    planes = []
    for z in range(nz):
        dot = None
        for c in range(3):
            term = outer[c, z] * (coef[z] * change[z][c])
            dot = term if dot is None else dot + term
        planes.append((weight[z] + coef[z] * dot, own[z]))
    for both, which in planes:
        for t in range(0, ny, 128):
            part, index = both[:, t : t + 128], which[:, t : t + 128]
            for j in range(NI):
                sums[j] = sums[j] + jnp.where(index == j, part, 0.0)
    for j in range(NI):
        portion[j] = sums[j]

    def include(both, which):
        for j in range(NI):
            one = portion[j]
            for t in range(0, ny, 128):
                one = one + jnp.where(which[:, t : t + 128] == j, both[:, t : t + 128], 0.0)
            portion[j] = one

    pl.when(odd)(functools.partial(wait_exchange, recv_sem.at[5], 0, ny))

    @pl.when(odd & (k < n_z - 1))
    def _():
        push_x, push_y = -SCALES[0] * pair_zf[1], SCALES[0] * pair_zf[0]
        turn = bx(push_y, 0.0) - by(push_x, True)
        above = pair_weight[1] * push_x - pair_weight[0] * push_y + pair_weight[2] * turn
        include(above, pair_own[0])

    @pl.when(odd & (k > 0))
    def _():
        below = pair_weight[3] * pair_zl[1] - pair_weight[4] * pair_zl[0]
        include(below, pair_own[1])

    lane = lax.broadcasted_iota(jnp.int32, (NI, 128), 1)
    number = lax.broadcasted_iota(jnp.int32, (NI, 128), 0)
    table = jnp.zeros((NI, 128), jnp.float32)
    for j in range(NI):
        table = jnp.where(number == j, jnp.sum(portion[j], axis=0, keepdims=True), table)
    table = jnp.where(lane == number, jnp.sum(table, axis=1, keepdims=True), 0.0)
    row = jnp.sum(table, axis=0, keepdims=True)
    mine[0] = row
    gathered[me] = row

    while len(told) <= len(hops):
        tell()

    def share_sum(step, carry):
        other = jnp.where(step < me, step, step + 1)
        pltpu.make_async_remote_copy(
            src_ref=mine.at[0], dst_ref=gathered.at[me], send_sem=send_sem, recv_sem=sum_recv,
            device_id=(other // n_z, lax.rem(other, n_z)), device_id_type=MESH,
        ).start()
        return carry

    lax.fori_loop(0, total - 1, share_sum, 0)

    wait_exchange(plane_sent.at[2], 0, ny)
    pl.when(~odd & (i < n_x - 1))(functools.partial(signal, pair_sem, i + 1, k))

    @pl.when(odd)
    def _():
        pl.semaphore_wait(pair_sem, 1)
        send(3, *PLANES)

    wait_exchange(recv_sem.at[3], 1, ny)
    change = finish(3, ko_ref)
    for z in range(nz):
        for c in range(3):
            go_ref[c, z] = inner[1, c, z] - COURANT * change[z][c]
    for parity, pairs in ((odd, 0), (~odd, 1)):
        pl.when(parity)(
            functools.partial(
                wait_exchange, send_sem, 4, 2 * ny, pairs=pairs, extra=total - 1
            )
        )
    if len(widths) > 1:
        pl.when(~odd)(functools.partial(wait_exchange, plane_sent.at[1], 0, *widths[1:]))
    everyone = gathered.at[0 : total - 1]
    pltpu.make_async_copy(everyone, everyone, sum_recv).wait()
    grad_ref[...] = jnp.sum(gathered[...], axis=0)[:, :NI] / norm


def store(g_ref, h_ref, grad_ref, g_hbm, h_hbm, grad_hbm, sem):
    pltpu.make_async_copy(grad_ref, grad_hbm, sem.at[2]).start()
    for z in range(g_ref.shape[1]):
        pltpu.make_async_copy(g_ref.at[:, z], g_hbm.at[:, :, z, :], sem.at[0]).start()
        pltpu.make_async_copy(h_ref.at[:, z], h_hbm.at[:, :, z, :], sem.at[1]).start()
    for n, ref in enumerate((g_ref, h_ref, grad_ref)):
        pltpu.make_async_copy(ref, ref, sem.at[n]).wait()


def solution(mesh):
    n_x, n_z = mesh.shape["xy"], mesh.shape["gz"]

    def body(e_check, h_check, adj_e, adj_h, material, owner, permittivity):
        _, nx, nz, ny = e_check.shape
        cells = nx * n_x * nz * n_z * ny
        norm = np.sqrt(np.float32(cells / NI))
        dims = (n_x, n_z, nx, nz, ny, permittivity.shape[0], norm)
        f32 = jnp.float32
        hbm_spec = pl.BlockSpec(memory_space=pltpu.HBM)
        vmem_spec = pl.BlockSpec(memory_space=pltpu.VMEM)
        block = (3, nz, nx, ny)
        g, h, grad = pl.pallas_call(
            functools.partial(kernel, dims),
            out_shape=(
                pltpu.VMEM(block, f32), pltpu.VMEM(block, f32), pltpu.VMEM((1, NI), f32),
            ),
            in_specs=[hbm_spec] * 7,
            out_specs=(vmem_spec,) * 3,
            scratch_shapes=[
                pltpu.SMEM(permittivity.shape, f32),
                pltpu.VMEM((4,) + block, f32),
                pltpu.VMEM((2,) + block, f32),
                pltpu.VMEM((4,) + block, f32),
                pltpu.VMEM((3,) + block, f32),
                pltpu.VMEM(block, f32),
                pltpu.VMEM((nz, nx, ny), jnp.int32),
                pltpu.VMEM((nz, nx, ny), jnp.int32),
                pltpu.VMEM((nz, nx, ny), f32),
                pltpu.VMEM((nz, nx, ny), f32),
                pltpu.VMEM((4, 2, nz, ny), f32),
                pltpu.VMEM((4, 2 * nz, ny), f32),
                pltpu.VMEM((4, 1, ny), f32),
                pltpu.VMEM((4, 1, ny), f32),
                pltpu.VMEM((4, 2, nz, ny), f32),
                pltpu.VMEM((4, 2, nx, ny), f32),
                pltpu.VMEM((4, 2 * nz, ny), f32),
                pltpu.VMEM((4, 2, nx, ny), f32),
                pltpu.VMEM((4, 1, ny), f32),
                pltpu.VMEM((4, 1, ny), f32),
                pltpu.VMEM((1, 1, 128), f32),
                pltpu.VMEM((n_x * n_z, 1, 128), f32),
                pltpu.VMEM((16 * (1 + 2 * nz + 2 * nx) * ny // 128 + n_x * n_z, 1, 128), f32),
                pltpu.VMEM((2, nx, ny), f32),
                pltpu.VMEM((2, nx, ny), f32),
                pltpu.VMEM((5, nx, ny), f32),
                pltpu.VMEM((5, nx, ny), f32),
                pltpu.VMEM((2, nx, ny), jnp.int32),
                pltpu.VMEM((NI, nx, 128), f32),
                pltpu.SemaphoreType.DMA((3,)),
                pltpu.SemaphoreType.DMA,
                pltpu.SemaphoreType.DMA((3,)),
                pltpu.SemaphoreType.DMA((6,)),
                pltpu.SemaphoreType.DMA,
                pltpu.SemaphoreType.REGULAR((max(1, (n_x - 1).bit_length()),)),
                pltpu.SemaphoreType.REGULAR,
            ],
            compiler_params=pltpu.CompilerParams(
                collective_id=0, has_side_effects=True
            ),
            name="yee_adjoint",
        )(e_check, h_check, adj_e, adj_h, material, owner, permittivity)
        g, h, grad = pl.pallas_call(
            store,
            out_shape=(
                jax.ShapeDtypeStruct(e_check.shape, f32),
                jax.ShapeDtypeStruct(e_check.shape, f32),
                jax.ShapeDtypeStruct((1, NI), f32),
            ),
            in_specs=[vmem_spec] * 3,
            out_specs=(hbm_spec,) * 3,
            scratch_shapes=[pltpu.SemaphoreType.DMA((3,))],
            compiler_params=pltpu.CompilerParams(vmem_limit_bytes=2**20),
            name="store_outputs",
        )(g, h, grad)
        return g, h, grad.reshape(NI)

    split = P(None, "xy", "gz", None)
    return jax.shard_map(
        body,
        mesh=mesh,
        in_specs=(split,) * 4 + (P("xy", "gz", None),) * 2 + (P(),),
        out_specs=(split, split, P()),
        check_vma=False,
    )
```
